128 devices in a mesh: dp: 1, tp: 16 (over z, y), sp: 8 (over x, core).
Axes of the slice: x: 4, y: 4, z: 4, core: 2. Of those that a mesh axis runs over, the one named last changes fastest.
Arguments:
- x_tokens: bfloat16 [8192, 4096], P(('dp', 'sp'), 'tp')
- doc_ids: int32 [8192], P(('dp', 'sp'))
- w_qkv: bfloat16 [4096, 12288], P('sp', 'tp')
- w_out: bfloat16 [4096, 4096], P('sp', 'tp')
Outputs:
- output: bfloat16 [8192, 4096], P(('dp', 'sp', 'tp'))
All inputs are finite; a program needn't handle non-finite values.
Results may differ from the reference program's by a relative error of at most 0.00246272.
Values are sent between devices in bfloat16 or wider.
A program may use at most 1 GiB of HBM per device.

```python
import jax
import jax.numpy as jnp
from jax import lax

SEQ_LEN = 8192
HIDDEN = 4096
NUM_HEADS = 32
HEAD_DIM = 128
QUERY_BLOCK = 512
NUM_PIECES = 32
NUM_CUTS = 3

NUM_QBLOCKS = SEQ_LEN // QUERY_BLOCK
PIECE_LEN = SEQ_LEN // NUM_PIECES
SOFTMAX_SCALE = HEAD_DIM ** -0.5


def draw_segments(seg_key):
    cut_points = jax.random.randint(seg_key, (NUM_CUTS,), 1, SEQ_LEN)
    positions = jnp.arange(SEQ_LEN, dtype=jnp.int32)
    return jnp.sum((positions[:, None] >= cut_points[None, :]).astype(jnp.int32), axis=1).astype(jnp.int32)


def setup_inputs(seed: int = 0, part: int = 0) -> dict:
    base_key = jax.random.key(seed)
    part_key = jax.random.fold_in(base_key, part)
    noise_key, piece_key, seg_key = jax.random.split(part_key, 3)
    wqkv_key, wout_key = jax.random.split(jax.random.key(seed + 1), 2)
    x_noise = jax.random.normal(noise_key, (NUM_PIECES, PIECE_LEN, HIDDEN), jnp.float32)
    pieces = jax.random.normal(piece_key, (NUM_PIECES, 1, HIDDEN), jnp.float32)
    x_val = 0.6 * x_noise + 0.8 * pieces
    x_tokens = x_val.reshape(SEQ_LEN, HIDDEN).astype(jnp.bfloat16)
    w_qkv = (jax.random.normal(wqkv_key, (HIDDEN, 3 * HIDDEN), jnp.float32) * HIDDEN ** -0.5).astype(jnp.bfloat16)
    w_out = (jax.random.normal(wout_key, (HIDDEN, HIDDEN), jnp.float32) * (2.0 * HIDDEN ** -0.5)).astype(jnp.bfloat16)
    return {"x_tokens": x_tokens, "doc_ids": draw_segments(seg_key), "w_qkv": w_qkv, "w_out": w_out}


def reference(x_tokens, doc_ids, w_qkv, w_out):
    qkv_all = jnp.dot(x_tokens, w_qkv, preferred_element_type=jnp.float32).astype(jnp.bfloat16)
    per_head = qkv_all.reshape(SEQ_LEN, NUM_HEADS, 3, HEAD_DIM).transpose(1, 2, 0, 3).astype(jnp.float32)
    doc_blocks = doc_ids.reshape(NUM_QBLOCKS, QUERY_BLOCK)

    def head_attention(head_qkv):
        key_head = head_qkv[1]
        value_head = head_qkv[2]
        query_blocks = head_qkv[0].reshape(NUM_QBLOCKS, QUERY_BLOCK, HEAD_DIM)

        def block_attention(block):
            query_blk, doc_blk = block
            scores = jnp.dot(query_blk, key_head.T, preferred_element_type=jnp.float32) * SOFTMAX_SCALE
            same_doc = doc_blk[:, None] == doc_ids[None, :]
            scores = jnp.where(same_doc, scores, -jnp.inf)
            weights = jax.nn.softmax(scores, axis=-1).astype(jnp.bfloat16).astype(jnp.float32)
            return jnp.dot(weights, value_head, preferred_element_type=jnp.float32)

        context = lax.map(block_attention, (query_blocks, doc_blocks))
        return context.reshape(SEQ_LEN, HEAD_DIM).astype(jnp.bfloat16)

    context_all = lax.map(head_attention, per_head)
    context_all = context_all.transpose(1, 0, 2).reshape(SEQ_LEN, HIDDEN)
    return jnp.dot(context_all, w_out, preferred_element_type=jnp.float32).astype(jnp.bfloat16)
```

```python
import functools

import jax
import jax.numpy as jnp
from jax import lax
from jax.experimental import pallas as pl
from jax.experimental.pallas import tpu as pltpu
from jax.sharding import PartitionSpec as P

HEAD_DIM = 128
EXP2_SCALE = HEAD_DIM ** -0.5 * 1.4426950408889634
FLOOR = -3.0e38


def attention_kernel(qb, kb, sub, q_ref, kv_ref, segq_ref, segk_ref, segall_ref, o_ref, acc_ref, m_ref, l_ref):
    segq_row = segq_ref[0]
    lo = jnp.min(segq_row)
    hi = jnp.max(segq_row)
    seg_all = segall_ref[...]
    first = jnp.sum(jnp.where(seg_all < lo, 1.0, 0.0)).astype(jnp.int32)
    last = jnp.sum(jnp.where(seg_all <= hi, 1.0, 0.0)).astype(jnp.int32)
    one_doc = lo == hi

    acc_ref[...] = jnp.zeros_like(acc_ref)
    l_ref[...] = jnp.zeros_like(l_ref)
    m_ref[...] = jnp.full_like(m_ref, FLOOR)

    def block(j, masked):
        start = pl.multiple_of(j * kb, kb)
        k = kv_ref[pl.ds(start, kb), :HEAD_DIM]
        v = kv_ref[pl.ds(start, kb), HEAD_DIM:]
        if masked:
            segk_row = segk_ref[j]
        for i in range(qb // sub):
            rows = slice(i * sub, (i + 1) * sub)
            s = lax.dot_general(q_ref[rows, :], k, (((1,), (1,)), ((), ())), preferred_element_type=jnp.float32)
            t = s * EXP2_SCALE
            if masked:
                segq_col = jnp.broadcast_to(segq_row[:, rows], (HEAD_DIM, sub)).T
                t = jnp.where(segq_col[:, :1] == segk_row, t, -jnp.inf)
            m_prev = m_ref[rows, :1]
            m_new = jnp.maximum(m_prev, jnp.max(t, axis=1, keepdims=True))
            p = jnp.exp2(t - m_new)
            alpha = jnp.exp2(m_prev - m_new)
            l_new = l_ref[rows, :1] * alpha + jnp.sum(p, axis=1, keepdims=True)
            pv = jnp.dot(p.astype(jnp.bfloat16), v, preferred_element_type=jnp.float32)
            acc_ref[rows, :] = acc_ref[rows, :] * alpha + pv
            m_ref[rows, :] = jnp.broadcast_to(m_new, (sub, HEAD_DIM))
            l_ref[rows, :] = jnp.broadcast_to(l_new, (sub, HEAD_DIM))

    def step(j, carry):
        whole = one_doc & (j * kb >= first) & ((j + 1) * kb <= last)

        @pl.when(whole)
        def _():
            block(j, False)

        @pl.when(jnp.logical_not(whole))
        def _():
            block(j, True)

        return carry

    lax.fori_loop(first // kb, (last + kb - 1) // kb, step, 0)
    o_ref[...] = (acc_ref[...] / l_ref[...]).astype(o_ref.dtype)


def attention(q, kv, seg_q, seg_all, qb=512, kb=512, sub=256):
    rows, keys = q.shape[0], kv.shape[0]
    heads = q.shape[1] // HEAD_DIM
    return pl.pallas_call(
        functools.partial(attention_kernel, qb, kb, sub),
        grid=(heads, rows // qb),
        out_shape=jax.ShapeDtypeStruct(q.shape, jnp.bfloat16),
        in_specs=[
            pl.BlockSpec((qb, HEAD_DIM), lambda h, i: (i, h)),
            pl.BlockSpec((keys, 2 * HEAD_DIM), lambda h, i: (0, h)),
            pl.BlockSpec((1, 1, qb), lambda h, i: (i, 0, 0)),
            pl.BlockSpec((keys // kb, 1, kb), lambda h, i: (0, 0, 0)),
            pl.BlockSpec((keys // HEAD_DIM, HEAD_DIM), lambda h, i: (0, 0)),
        ],
        out_specs=pl.BlockSpec((qb, HEAD_DIM), lambda h, i: (i, h)),
        scratch_shapes=[
            pltpu.VMEM((qb, HEAD_DIM), jnp.float32),
            pltpu.VMEM((qb, HEAD_DIM), jnp.float32),
            pltpu.VMEM((qb, HEAD_DIM), jnp.float32),
        ],
        compiler_params=pltpu.CompilerParams(vmem_limit_bytes=48 * 1024 * 1024),
        name="attention",
    )(q, kv, seg_q.reshape(rows // qb, 1, qb), seg_all.reshape(keys // kb, 1, kb), seg_all.reshape(keys // HEAD_DIM, HEAD_DIM))


def solution(mesh):
    def device_block(x_block, doc_block, wqkv_block, wout_block):
        x_rows = lax.all_gather(x_block, "tp", axis=1, tiled=True)
        wqkv_cols = lax.all_gather(wqkv_block, "sp", axis=0, tiled=True)
        qkv_local = jnp.dot(x_rows, wqkv_cols, preferred_element_type=jnp.float32).astype(jnp.bfloat16)
        row_count = x_rows.shape[0]
        head_count = wqkv_cols.shape[1] // (3 * HEAD_DIM)
        qkv_local = qkv_local.reshape(row_count, head_count, 3 * HEAD_DIM)
        query_loc = qkv_local[:, :, :HEAD_DIM].reshape(row_count, head_count * HEAD_DIM)
        kv_loc = qkv_local[:, :, HEAD_DIM:].reshape(row_count, head_count * 2 * HEAD_DIM)
        kv_all = lax.all_gather(kv_loc, "sp", axis=0, tiled=True)
        doc_all = lax.all_gather(doc_block, "sp", axis=0, tiled=True)
        context = attention(query_loc, kv_all, doc_block, doc_all)
        ctx_rows = lax.all_gather(context, "tp", axis=1, tiled=True)
        wout_cols = lax.all_gather(wout_block, "sp", axis=0, tiled=True)
        y_block = jnp.dot(ctx_rows, wout_cols, preferred_element_type=jnp.float32).astype(jnp.bfloat16)
        return lax.all_to_all(y_block, "tp", 0, 1, tiled=True)

    return jax.shard_map(
        device_block,
        mesh=mesh,
        in_specs=(P(("dp", "sp"), "tp"), P(("dp", "sp")), P("sp", "tp"), P("sp", "tp")),
        out_specs=P(("dp", "sp", "tp"), None),
        check_vma=False,
    )
```

```python
import functools

import jax
import jax.numpy as jnp
from jax import lax
from jax.experimental import pallas as pl
from jax.experimental.pallas import tpu as pltpu
from jax.sharding import PartitionSpec as P

HEAD_DIM = 128
EXP2_SCALE = HEAD_DIM ** -0.5 * 1.4426950408889634
FLOOR = -3.0e38


def attention_kernel(qb, kb, sub, q_ref, kv_ref, segq_ref, segk_ref, segall_ref, o_ref, acc_ref, m_ref, l_ref):
    segq_row = segq_ref[0]
    lo = jnp.min(segq_row)
    hi = jnp.max(segq_row)
    seg_all = segall_ref[...]
    first = jnp.sum(jnp.where(seg_all < lo, 1.0, 0.0)).astype(jnp.int32)
    last = jnp.sum(jnp.where(seg_all <= hi, 1.0, 0.0)).astype(jnp.int32)
    one_doc = lo == hi

    acc_ref[...] = jnp.zeros_like(acc_ref)
    l_ref[...] = jnp.zeros_like(l_ref)
    m_ref[...] = jnp.full_like(m_ref, FLOOR)

    def block(j, masked):
        start = pl.multiple_of(j * kb, kb)
        k = kv_ref[pl.ds(start, kb), :HEAD_DIM]
        v = kv_ref[pl.ds(start, kb), HEAD_DIM:]
        if masked:
            segk_row = segk_ref[j]
        for i in range(qb // sub):
            rows = slice(i * sub, (i + 1) * sub)
            s = lax.dot_general(q_ref[rows, :], k, (((1,), (1,)), ((), ())), preferred_element_type=jnp.float32)
            t = s * EXP2_SCALE
            if masked:
                segq_col = jnp.broadcast_to(segq_row[:, rows], (HEAD_DIM, sub)).T
                t = jnp.where(segq_col[:, :1] == segk_row, t, -jnp.inf)
            m_prev = m_ref[rows, :1]
            m_new = jnp.maximum(m_prev, jnp.max(t, axis=1, keepdims=True))
            p = jnp.exp2(t - m_new)
            alpha = jnp.exp2(m_prev - m_new)
            l_new = l_ref[rows, :1] * alpha + jnp.sum(p, axis=1, keepdims=True)
            pv = jnp.dot(p.astype(jnp.bfloat16), v, preferred_element_type=jnp.float32)
            acc_ref[rows, :] = acc_ref[rows, :] * alpha + pv
            m_ref[rows, :] = jnp.broadcast_to(m_new, (sub, HEAD_DIM))
            l_ref[rows, :] = jnp.broadcast_to(l_new, (sub, HEAD_DIM))

    def step(j, carry):
        whole = one_doc & (j * kb >= first) & ((j + 1) * kb <= last)

        @pl.when(whole)
        def _():
            block(j, False)

        @pl.when(jnp.logical_not(whole))
        def _():
            block(j, True)

        return carry

    lax.fori_loop(first // kb, (last + kb - 1) // kb, step, 0)
    o_ref[...] = (acc_ref[...] / l_ref[...]).astype(o_ref.dtype)


def attention(q, kv, seg_q, seg_all, qb=512, kb=512, sub=256):
    rows, keys = q.shape[0], kv.shape[0]
    heads = q.shape[1] // HEAD_DIM
    return pl.pallas_call(
        functools.partial(attention_kernel, qb, kb, sub),
        grid=(heads, rows // qb),
        out_shape=jax.ShapeDtypeStruct(q.shape, jnp.bfloat16),
        in_specs=[
            pl.BlockSpec((qb, HEAD_DIM), lambda h, i: (i, h)),
            pl.BlockSpec((keys, 2 * HEAD_DIM), lambda h, i: (0, h)),
            pl.BlockSpec((1, 1, qb), lambda h, i: (i, 0, 0)),
            pl.BlockSpec((keys // kb, 1, kb), lambda h, i: (0, 0, 0)),
            pl.BlockSpec((keys // HEAD_DIM, HEAD_DIM), lambda h, i: (0, 0)),
        ],
        out_specs=pl.BlockSpec((qb, HEAD_DIM), lambda h, i: (i, h)),
        scratch_shapes=[
            pltpu.VMEM((qb, HEAD_DIM), jnp.float32),
            pltpu.VMEM((qb, HEAD_DIM), jnp.float32),
            pltpu.VMEM((qb, HEAD_DIM), jnp.float32),
        ],
        compiler_params=pltpu.CompilerParams(vmem_limit_bytes=48 * 1024 * 1024),
        name="attention",
    )(q, kv, seg_q.reshape(rows // qb, 1, qb), seg_all.reshape(keys // kb, 1, kb), seg_all.reshape(keys // HEAD_DIM, HEAD_DIM))


SIDE = 4
CHUNKS = 4
MESH = pl.DeviceIdType.MESH


def remote(src, dst, send_sem, recv_sem, tp, sp):
    return pltpu.make_async_remote_copy(
        src_ref=src, dst_ref=dst, send_sem=send_sem, recv_sem=recv_sem,
        device_id={"tp": tp, "sp": sp}, device_id_type=MESH)


def arrived(ref, sem, tp, sp):
    remote(ref, ref, sem, sem, tp, sp).wait_recv()


def barrier_with(peers):
    barrier = pltpu.get_barrier_semaphore()
    for tp, sp in peers:
        pl.semaphore_signal(barrier, inc=1, device_id={"tp": tp, "sp": sp}, device_id_type=MESH)
    pl.semaphore_wait(barrier, len(peers))


class Gather2D:
    def __init__(self, coords, place, own, held, send_sem, recv_sem):
        self.coords, self.place, self.own, self.held = coords, place, own, held
        self.send_sem, self.recv_sem = send_sem, recv_sem
        self.sent = {}

    def at(self, h, j1, j2):
        u, v = self.coords
        j1, j2 = (j1, j2) if h == 0 else (j2, j1)
        return lax.rem(u + j1, SIDE), lax.rem(v + j2, SIDE)

    def send(self, r, h, piece, to):
        src_at, dst_at = self.at(h, *piece), self.at(h, *to)
        src = self.own(r, h) if piece == (0, 0) else self.held(r, h, *src_at)
        k = self.sent.get((r, h), 0)
        self.sent[r, h] = k + 1
        copy = remote(src, self.held(r, h, *src_at), self.send_sem.at[r, h, k],
                      self.recv_sem.at[r, h, src_at[0] * SIDE + src_at[1]], *self.place(*dst_at))
        copy.start()

    def wait(self, r, h, piece):
        src_at = self.at(h, *piece)
        arrived(self.held(r, h, *src_at), self.recv_sem.at[r, h, src_at[0] * SIDE + src_at[1]], *self.place(*self.coords))

    def start(self, r):
        for h in (0, 1):
            for to in ((1, 0), (3, 0), (0, 1), (0, 3)):
                self.send(r, h, (0, 0), to)

    def spread(self, r, h, j1):
        for j2 in (1, 3):
            self.send(r, h, (j1, 0), (0, j2))

    def near(self, r):
        for j1 in (3, 1):
            for h in (0, 1):
                self.wait(r, h, (j1, 0))
                if j1 == (3 if (r + h) % 2 == 0 else 1):
                    self.send(r, h, (j1, 0), (4 - j1, 0))
                self.spread(r, h, j1)

    def pass_on(self, r, j1):
        for h in (0, 1):
            for j2 in (3, 1):
                self.wait(r, h, (j1, j2))
                if j2 == (3 if (r + h + (j1 + 1) // 2) % 2 == 0 else 1):
                    self.send(r, h, (j1, j2), (0, 4 - j2))

    def far(self, r):
        self.pass_on(r, 0)
        for h in (0, 1):
            self.wait(r, h, (2, 0))
            self.spread(r, h, 2)

    def last(self, r):
        for j1 in (3, 1, 2):
            self.pass_on(r, j1)
        for j1 in (0, 3, 1, 2):
            for h in (0, 1):
                self.wait(r, h, (j1, 2))

    def drain(self, r):
        for h in (0, 1):
            for k in range(self.sent[r, h]):
                ref = self.own(r, h)
                remote(ref, ref, self.send_sem.at[r, h, k], self.recv_sem.at[r, h, 0], *self.place(*self.coords)).wait_send()


def qkv_kernel(x_ref, w_ref, seg_ref, q_ref, kv_ref, segall_ref,
               x_all, w_all, qkv, xs, xr, ws, wr, ss, sr, ks, kr):
    tp, sp = lax.axis_index("tp"), lax.axis_index("sp")
    z, y = tp // SIDE, lax.rem(tp, SIDE)
    x, core = sp // 2, lax.rem(sp, 2)
    rows, width = x_ref.shape
    depth = w_ref.shape[0]
    chunk = rows // CHUNKS
    half = width // 2

    def sp_at(dx, other=0):
        return lax.rem(x + dx, SIDE) * 2 + lax.rem(core + other, 2)

    mate = sp_at(0, 1)
    group = x // 2
    ally = (x + 1 - 2 * lax.rem(x, 2)) * 2 + core
    cross = (SIDE - 1 - x) * 2 + core

    peers = [(lax.rem(z + d, SIDE) * SIDE + y, sp) for d in (1, 3)]
    peers += [(z * SIDE + lax.rem(y + d, SIDE), sp) for d in (1, 3)]
    peers += [(tp, lax.rem(sp + d, 2 * SIDE)) for d in range(1, 2 * SIDE)]
    barrier_with(peers)

    grid = Gather2D(
        (z, y), lambda u, v: (u * SIDE + v, sp),
        lambda r, h: x_ref.at[pl.ds(r * chunk, chunk), pl.ds(h * half, half)],
        lambda r, h, u, v: x_all.at[pl.ds(r * chunk, chunk), pl.ds(pl.multiple_of((u * SIDE + v) * width + h * half, half), half)],
        xs, xr)

    def w_at(owner, p):
        return w_all.at[pl.ds(pl.multiple_of(owner * depth + p * (depth // 2), depth // 2), depth // 2), :]

    w_sends = []

    def w_send(owner, p, to, src=None):
        k = len(w_sends)
        copy = remote(w_at(owner, p) if src is None else src, w_at(owner, p), ws.at[k], wr.at[owner, p], tp, to)
        copy.start()
        w_sends.append(copy)

    def w_wait(owner, p):
        arrived(w_at(owner, p), wr.at[owner, p], tp, sp)

    def w_own(p):
        src = w_ref.at[pl.ds(p * (depth // 2), depth // 2), :]
        for to in (sp_at(1), sp_at(3), mate):
            w_send(sp, p, to, src)

    def w_near(p):
        for d in (3, 1):
            w_wait(sp_at(d), p)
            if d == (3 if p == 0 else 1):
                w_send(sp_at(d), p, sp_at(4 - d))
            w_send(sp_at(d), p, mate)

    def w_far():
        for p in (0, 1):
            w_wait(sp_at(2), p)
            w_send(sp_at(2), p, mate)

    def w_mate():
        for p in (0, 1):
            for d in (0, 1, 3, 2):
                w_wait(sp_at(d, 1), p)

    grid.start(0)
    w_own(0)
    w_own(1)
    seg_copies = []
    for d in range(1, 2 * SIDE):
        copy = remote(seg_ref, segall_ref.at[sp], ss.at[d], sr.at[sp], tp, lax.rem(sp + d, 2 * SIDE))
        copy.start()
        seg_copies.append(copy)
    segall_ref[sp] = seg_ref[...]
    x_all[:, pl.ds(pl.multiple_of(tp * width, width), width)] = x_ref[...]
    w_all[pl.ds(pl.multiple_of(sp * depth, depth), depth), :] = w_ref[...]

    def kv_at(owner, r):
        return kv_ref.at[pl.ds(pl.multiple_of(owner * rows + r * chunk, chunk), chunk), :]

    kv_sends = []

    def kv_send(src, dst, recv, to):
        k = len(kv_sends)
        copy = remote(src, dst, ks.at[k], recv, tp, to)
        copy.start()
        kv_sends.append(copy)

    def project(r):
        here = slice(r * chunk, (r + 1) * chunk)
        for n in range(3):
            part = slice(n * 256, (n + 1) * 256)
            out = jnp.dot(x_all[here, :], w_all[:, part], preferred_element_type=jnp.float32).astype(jnp.bfloat16)
            for m in range(2):
                col = n * 2 + m
                qkv[col // 3, here, (col % 3) * HEAD_DIM:(col % 3 + 1) * HEAD_DIM] = out[:, m * HEAD_DIM:(m + 1) * HEAD_DIM]
        q_ref[here, :] = qkv[group, here, :HEAD_DIM]
        kv_ref[pl.ds(pl.multiple_of(sp * rows + r * chunk, chunk), chunk), :] = qkv[group, here, HEAD_DIM:]
        span = pl.ds(r * chunk, chunk)
        kv_send(qkv.at[1 - group, span, pl.ds(HEAD_DIM, 2 * HEAD_DIM)], kv_at(sp, r), kr.at[sp, r], cross)
        kv_send(qkv.at[1 - group, span, pl.ds(0, HEAD_DIM)], q_ref.at[pl.ds(rows + r * chunk, chunk), :], kr.at[2 * SIDE, r], cross)
        kv_send(qkv.at[group, span, pl.ds(HEAD_DIM, 2 * HEAD_DIM)], kv_at(sp, r), kr.at[sp, r], ally)
        kv_send(qkv.at[group, span, pl.ds(HEAD_DIM, 2 * HEAD_DIM)], kv_at(sp, r), kr.at[sp, r], mate)

    ally_cross = lax.rem(x + 2, SIDE) * 2 + core

    def kv_wait(owner, r):
        arrived(kv_at(owner, r), kr.at[owner, r], tp, sp)

    def kv_cross(r):
        kv_wait(cross, r)
        kv_send(kv_at(cross, r), kv_at(cross, r), kr.at[cross, r], ally)
        kv_send(kv_at(cross, r), kv_at(cross, r), kr.at[cross, r], mate)

    def kv_ally(r):
        for owner in (ally, ally_cross):
            kv_wait(owner, r)
            kv_send(kv_at(owner, r), kv_at(owner, r), kr.at[owner, r], mate)

    def kv_mate(r):
        arrived(q_ref.at[pl.ds(rows + r * chunk, chunk), :], kr.at[2 * SIDE, r], tp, sp)
        for d in range(SIDE):
            kv_wait(sp_at(d, 1), r)

    grid.near(0)
    grid.start(1)
    grid.far(0)
    grid.last(0)
    w_near(0)
    grid.near(1)
    grid.start(2)
    grid.far(1)
    grid.last(1)
    w_near(1)
    grid.near(2)
    grid.start(3)
    w_far()
    w_mate()
    project(0)
    grid.far(2)
    project(1)
    grid.last(2)
    kv_cross(0)
    grid.near(3)
    project(2)
    kv_cross(1)
    kv_ally(0)
    grid.far(3)
    kv_ally(1)
    kv_cross(2)
    grid.last(3)
    project(3)
    kv_ally(2)
    kv_cross(3)
    kv_ally(3)
    for r in range(CHUNKS):
        kv_mate(r)
    for d in range(1, 2 * SIDE):
        arrived(segall_ref.at[lax.rem(sp + d, 2 * SIDE)], sr.at[lax.rem(sp + d, 2 * SIDE)], tp, sp)
    for r in range(CHUNKS):
        grid.drain(r)
    for copy in w_sends + seg_copies + kv_sends:
        copy.wait_send()


def qkv_exchange(x_block, wqkv_block, seg_block):
    rows, width = x_block.shape
    depth, cols = wqkv_block.shape
    sps, tps = 2 * SIDE, SIDE * SIDE
    seg_tile = seg_block.reshape(rows // HEAD_DIM, HEAD_DIM)
    vmem = pl.BlockSpec(memory_space=pltpu.VMEM)
    dma = pltpu.SemaphoreType.DMA
    return pl.pallas_call(
        qkv_kernel,
        out_shape=(
            jax.ShapeDtypeStruct((2 * rows, HEAD_DIM), jnp.bfloat16),
            jax.ShapeDtypeStruct((sps * rows, 2 * HEAD_DIM), jnp.bfloat16),
            jax.ShapeDtypeStruct((sps,) + seg_tile.shape, jnp.int32),
        ),
        in_specs=[vmem] * 3,
        out_specs=(vmem,) * 3,
        scratch_shapes=[
            pltpu.VMEM((rows, tps * width), jnp.bfloat16),
            pltpu.VMEM((sps * depth, cols), jnp.bfloat16),
            pltpu.VMEM((2, rows, 3 * HEAD_DIM), jnp.bfloat16),
            dma((CHUNKS, 2, 15)), dma((CHUNKS, 2, tps)),
            dma((14,)), dma((sps, 2)),
            dma((sps,)), dma((sps,)),
            dma((8 * CHUNKS,)), dma((sps + 1, CHUNKS)),
        ],
        compiler_params=pltpu.CompilerParams(collective_id=0, has_side_effects=True, vmem_limit_bytes=56 * 1024 * 1024),
        name="qkv_exchange",
    )(x_block, wqkv_block, seg_tile)


def solution(mesh):
    def device_block(x_block, doc_block, wqkv_block, wout_block):
        rows = x_block.shape[0]
        q, kv, seg_all = qkv_exchange(x_block, wqkv_block, doc_block)
        seg_all = seg_all.reshape(-1)
        sp = lax.axis_index("sp")
        cross = (SIDE - 1 - sp // 2) * 2 + sp % 2
        seg_q = jnp.concatenate([doc_block, lax.dynamic_slice(seg_all, (cross * rows,), (rows,))])
        context = attention(q, kv, seg_q, seg_all)
        swap = [(i, (SIDE - 1 - i // 2) * 2 + i % 2) for i in range(2 * SIDE)]
        other = lax.ppermute(context[rows:], "sp", swap)
        low = sp < SIDE
        context = jnp.concatenate([jnp.where(low, context[:rows], other), jnp.where(low, other, context[:rows])], axis=1)
        ctx_rows = lax.all_gather(context, "tp", axis=1, tiled=True)
        wout_cols = lax.all_gather(wout_block, "sp", axis=0, tiled=True)
        y_block = jnp.dot(ctx_rows, wout_cols, preferred_element_type=jnp.float32).astype(jnp.bfloat16)
        return lax.all_to_all(y_block, "tp", 0, 1, tiled=True)

    return jax.shard_map(
        device_block,
        mesh=mesh,
        in_specs=(P(("dp", "sp"), "tp"), P(("dp", "sp")), P("sp", "tp"), P("sp", "tp")),
        out_specs=P(("dp", "sp", "tp"), None),
        check_vma=False,
    )
```

```python
import functools

import jax
import jax.numpy as jnp
from jax import lax
from jax.experimental import pallas as pl
from jax.experimental.pallas import tpu as pltpu
from jax.sharding import PartitionSpec as P

HEAD_DIM = 128
EXP2_SCALE = HEAD_DIM ** -0.5 * 1.4426950408889634
FLOOR = -3.0e38


def attention_kernel(qb, kb, sub, q_ref, kv_ref, segq_ref, segk_ref, segall_ref, o_ref, acc_ref, m_ref, l_ref):
    segq_row = segq_ref[0]
    lo = jnp.min(segq_row)
    hi = jnp.max(segq_row)
    seg_all = segall_ref[...]
    first = jnp.sum(jnp.where(seg_all < lo, 1.0, 0.0)).astype(jnp.int32)
    last = jnp.sum(jnp.where(seg_all <= hi, 1.0, 0.0)).astype(jnp.int32)
    one_doc = lo == hi

    acc_ref[...] = jnp.zeros_like(acc_ref)
    l_ref[...] = jnp.zeros_like(l_ref)
    m_ref[...] = jnp.full_like(m_ref, FLOOR)

    def block(j, masked):
        start = pl.multiple_of(j * kb, kb)
        k = kv_ref[pl.ds(start, kb), :HEAD_DIM]
        v = kv_ref[pl.ds(start, kb), HEAD_DIM:]
        if masked:
            segk_row = segk_ref[j]
        for i in range(qb // sub):
            rows = slice(i * sub, (i + 1) * sub)
            s = lax.dot_general(q_ref[rows, :], k, (((1,), (1,)), ((), ())), preferred_element_type=jnp.float32)
            t = s * EXP2_SCALE
            if masked:
                segq_col = jnp.broadcast_to(segq_row[:, rows], (HEAD_DIM, sub)).T
                t = jnp.where(segq_col[:, :1] == segk_row, t, -jnp.inf)
            m_prev = m_ref[rows, :1]
            m_new = jnp.maximum(m_prev, jnp.max(t, axis=1, keepdims=True))
            p = jnp.exp2(t - m_new)
            alpha = jnp.exp2(m_prev - m_new)
            l_new = l_ref[rows, :1] * alpha + jnp.sum(p, axis=1, keepdims=True)
            pv = jnp.dot(p.astype(jnp.bfloat16), v, preferred_element_type=jnp.float32)
            acc_ref[rows, :] = acc_ref[rows, :] * alpha + pv
            m_ref[rows, :] = jnp.broadcast_to(m_new, (sub, HEAD_DIM))
            l_ref[rows, :] = jnp.broadcast_to(l_new, (sub, HEAD_DIM))

    def step(j, carry):
        whole = one_doc & (j * kb >= first) & ((j + 1) * kb <= last)

        @pl.when(whole)
        def _():
            block(j, False)

        @pl.when(jnp.logical_not(whole))
        def _():
            block(j, True)

        return carry

    lax.fori_loop(first // kb, (last + kb - 1) // kb, step, 0)
    o_ref[...] = (acc_ref[...] / l_ref[...]).astype(o_ref.dtype)


def attention(q, kv, seg_q, seg_all, qb=512, kb=512, sub=256):
    rows, keys = q.shape[0], kv.shape[0]
    heads = q.shape[1] // HEAD_DIM
    return pl.pallas_call(
        functools.partial(attention_kernel, qb, kb, sub),
        grid=(heads, rows // qb),
        out_shape=jax.ShapeDtypeStruct(q.shape, jnp.bfloat16),
        in_specs=[
            pl.BlockSpec((qb, HEAD_DIM), lambda h, i: (i, h)),
            pl.BlockSpec((keys, 2 * HEAD_DIM), lambda h, i: (0, h)),
            pl.BlockSpec((1, 1, qb), lambda h, i: (i, 0, 0)),
            pl.BlockSpec((keys // kb, 1, kb), lambda h, i: (0, 0, 0)),
            pl.BlockSpec((keys // HEAD_DIM, HEAD_DIM), lambda h, i: (0, 0)),
        ],
        out_specs=pl.BlockSpec((qb, HEAD_DIM), lambda h, i: (i, h)),
        scratch_shapes=[
            pltpu.VMEM((qb, HEAD_DIM), jnp.float32),
            pltpu.VMEM((qb, HEAD_DIM), jnp.float32),
            pltpu.VMEM((qb, HEAD_DIM), jnp.float32),
        ],
        compiler_params=pltpu.CompilerParams(vmem_limit_bytes=48 * 1024 * 1024),
        name="attention",
    )(q, kv, seg_q.reshape(rows // qb, 1, qb), seg_all.reshape(keys // kb, 1, kb), seg_all.reshape(keys // HEAD_DIM, HEAD_DIM))


SIDE = 4
CHUNKS = 4
MESH = pl.DeviceIdType.MESH


def remote(src, dst, send_sem, recv_sem, tp, sp):
    return pltpu.make_async_remote_copy(
        src_ref=src, dst_ref=dst, send_sem=send_sem, recv_sem=recv_sem,
        device_id={"tp": tp, "sp": sp}, device_id_type=MESH)


def arrived(ref, sem, tp, sp):
    remote(ref, ref, sem, sem, tp, sp).wait_recv()


def barrier_with(peers):
    barrier = pltpu.get_barrier_semaphore()
    for tp, sp in peers:
        pl.semaphore_signal(barrier, inc=1, device_id={"tp": tp, "sp": sp}, device_id_type=MESH)
    pl.semaphore_wait(barrier, len(peers))


class Gather2D:
    def __init__(self, coords, place, own, held, send_sem, recv_sem):
        self.coords, self.place, self.own, self.held = coords, place, own, held
        self.send_sem, self.recv_sem = send_sem, recv_sem
        self.sent = {}

    def at(self, h, j1, j2):
        u, v = self.coords
        j1, j2 = (j1, j2) if h == 0 else (j2, j1)
        return lax.rem(u + j1, SIDE), lax.rem(v + j2, SIDE)

    def send(self, r, h, piece, to):
        src_at, dst_at = self.at(h, *piece), self.at(h, *to)
        src = self.own(r, h) if piece == (0, 0) else self.held(r, h, *src_at)
        k = self.sent.get((r, h), 0)
        self.sent[r, h] = k + 1
        copy = remote(src, self.held(r, h, *src_at), self.send_sem.at[r, h, k],
                      self.recv_sem.at[r, h, src_at[0] * SIDE + src_at[1]], *self.place(*dst_at))
        copy.start()

    def wait(self, r, h, piece):
        src_at = self.at(h, *piece)
        arrived(self.held(r, h, *src_at), self.recv_sem.at[r, h, src_at[0] * SIDE + src_at[1]], *self.place(*self.coords))

    def start(self, r):
        for h in (0, 1):
            for to in ((1, 0), (3, 0), (0, 1), (0, 3)):
                self.send(r, h, (0, 0), to)

    def spread(self, r, h, j1):
        for j2 in (1, 3):
            self.send(r, h, (j1, 0), (0, j2))

    def near(self, r):
        for j1 in (3, 1):
            for h in (0, 1):
                self.wait(r, h, (j1, 0))
                if j1 == (3 if (r + h) % 2 == 0 else 1):
                    self.send(r, h, (j1, 0), (4 - j1, 0))
                self.spread(r, h, j1)

    def pass_on(self, r, j1):
        for h in (0, 1):
            for j2 in (3, 1):
                self.wait(r, h, (j1, j2))
                if j2 == (3 if (r + h + (j1 + 1) // 2) % 2 == 0 else 1):
                    self.send(r, h, (j1, j2), (0, 4 - j2))

    def far(self, r):
        self.pass_on(r, 0)
        for h in (0, 1):
            self.wait(r, h, (2, 0))
            self.spread(r, h, 2)

    def last(self, r):
        for j1 in (3, 1, 2):
            self.pass_on(r, j1)
        for j1 in (0, 3, 1, 2):
            for h in (0, 1):
                self.wait(r, h, (j1, 2))

    def drain(self, r):
        for h in (0, 1):
            for k in range(self.sent[r, h]):
                ref = self.own(r, h)
                remote(ref, ref, self.send_sem.at[r, h, k], self.recv_sem.at[r, h, 0], *self.place(*self.coords)).wait_send()


def qkv_kernel(x_ref, w_ref, seg_ref, q_ref, kv_ref, segall_ref,
               x_all, w_all, qkv, xs, xr, ws, wr, ss, sr, ks, kr):
    tp, sp = lax.axis_index("tp"), lax.axis_index("sp")
    z, y = tp // SIDE, lax.rem(tp, SIDE)
    x, core = sp // 2, lax.rem(sp, 2)
    rows, width = x_ref.shape
    depth = w_ref.shape[0]
    chunk = rows // CHUNKS
    half = width // 2

    def sp_at(dx, other=0):
        return lax.rem(x + dx, SIDE) * 2 + lax.rem(core + other, 2)

    mate = sp_at(0, 1)
    group = x // 2
    ally = (x + 1 - 2 * lax.rem(x, 2)) * 2 + core
    cross = (SIDE - 1 - x) * 2 + core

    peers = [(lax.rem(z + d, SIDE) * SIDE + y, sp) for d in (1, 3)]
    peers += [(z * SIDE + lax.rem(y + d, SIDE), sp) for d in (1, 3)]
    peers += [(tp, lax.rem(sp + d, 2 * SIDE)) for d in range(1, 2 * SIDE)]
    barrier_with(peers)

    grid = Gather2D(
        (z, y), lambda u, v: (u * SIDE + v, sp),
        lambda r, h: x_ref.at[pl.ds(r * chunk, chunk), pl.ds(h * half, half)],
        lambda r, h, u, v: x_all.at[pl.ds(r * chunk, chunk), pl.ds(pl.multiple_of((u * SIDE + v) * width + h * half, half), half)],
        xs, xr)

    def w_at(owner, p):
        return w_all.at[pl.ds(pl.multiple_of(owner * depth + p * (depth // 2), depth // 2), depth // 2), :]

    w_sends = []

    def w_send(owner, p, to, src=None):
        k = len(w_sends)
        copy = remote(w_at(owner, p) if src is None else src, w_at(owner, p), ws.at[k], wr.at[owner, p], tp, to)
        copy.start()
        w_sends.append(copy)

    def w_wait(owner, p):
        arrived(w_at(owner, p), wr.at[owner, p], tp, sp)

    def w_own(p):
        src = w_ref.at[pl.ds(p * (depth // 2), depth // 2), :]
        for to in (sp_at(1), sp_at(3), mate):
            w_send(sp, p, to, src)

    def w_near(p):
        for d in (3, 1):
            w_wait(sp_at(d), p)
            if d == (3 if p == 0 else 1):
                w_send(sp_at(d), p, sp_at(4 - d))
            w_send(sp_at(d), p, mate)

    def w_far():
        for p in (0, 1):
            w_wait(sp_at(2), p)
            w_send(sp_at(2), p, mate)

    def w_mate():
        for p in (0, 1):
            for d in (0, 1, 3, 2):
                w_wait(sp_at(d, 1), p)

    grid.start(0)
    w_own(0)
    w_own(1)
    seg_copies = []
    for d in range(1, 2 * SIDE):
        copy = remote(seg_ref, segall_ref.at[sp], ss.at[d], sr.at[sp], tp, lax.rem(sp + d, 2 * SIDE))
        copy.start()
        seg_copies.append(copy)
    segall_ref[sp] = seg_ref[...]
    x_all[:, pl.ds(pl.multiple_of(tp * width, width), width)] = x_ref[...]
    w_all[pl.ds(pl.multiple_of(sp * depth, depth), depth), :] = w_ref[...]

    def kv_at(owner, r):
        return kv_ref.at[pl.ds(pl.multiple_of(owner * rows + r * chunk, chunk), chunk), :]

    kv_sends = []

    def kv_send(src, dst, recv, to):
        k = len(kv_sends)
        copy = remote(src, dst, ks.at[k], recv, tp, to)
        copy.start()
        kv_sends.append(copy)

    def project(r):
        here = slice(r * chunk, (r + 1) * chunk)
        for n in range(3):
            part = slice(n * 256, (n + 1) * 256)
            out = jnp.dot(x_all[here, :], w_all[:, part], preferred_element_type=jnp.float32).astype(jnp.bfloat16)
            for m in range(2):
                col = n * 2 + m
                qkv[col // 3, here, (col % 3) * HEAD_DIM:(col % 3 + 1) * HEAD_DIM] = out[:, m * HEAD_DIM:(m + 1) * HEAD_DIM]
        q_ref[here, :] = qkv[group, here, :HEAD_DIM]
        kv_ref[pl.ds(pl.multiple_of(sp * rows + r * chunk, chunk), chunk), :] = qkv[group, here, HEAD_DIM:]
        span = pl.ds(r * chunk, chunk)
        kv_send(qkv.at[1 - group, span, pl.ds(HEAD_DIM, 2 * HEAD_DIM)], kv_at(sp, r), kr.at[sp, r], cross)
        kv_send(qkv.at[1 - group, span, pl.ds(0, HEAD_DIM)], q_ref.at[pl.ds(rows + r * chunk, chunk), :], kr.at[2 * SIDE, r], cross)
        kv_send(qkv.at[group, span, pl.ds(HEAD_DIM, 2 * HEAD_DIM)], kv_at(sp, r), kr.at[sp, r], ally)
        kv_send(qkv.at[group, span, pl.ds(HEAD_DIM, 2 * HEAD_DIM)], kv_at(sp, r), kr.at[sp, r], mate)

    ally_cross = lax.rem(x + 2, SIDE) * 2 + core

    def kv_wait(owner, r):
        arrived(kv_at(owner, r), kr.at[owner, r], tp, sp)

    def kv_cross(r):
        kv_wait(cross, r)
        kv_send(kv_at(cross, r), kv_at(cross, r), kr.at[cross, r], ally)
        kv_send(kv_at(cross, r), kv_at(cross, r), kr.at[cross, r], mate)

    def kv_ally(r):
        for owner in (ally, ally_cross):
            kv_wait(owner, r)
            kv_send(kv_at(owner, r), kv_at(owner, r), kr.at[owner, r], mate)

    def kv_mate(r):
        arrived(q_ref.at[pl.ds(rows + r * chunk, chunk), :], kr.at[2 * SIDE, r], tp, sp)
        for d in range(SIDE):
            kv_wait(sp_at(d, 1), r)

    grid.near(0)
    grid.start(1)
    grid.far(0)
    grid.last(0)
    w_near(0)
    grid.near(1)
    grid.start(2)
    grid.far(1)
    grid.last(1)
    w_near(1)
    grid.near(2)
    grid.start(3)
    w_far()
    w_mate()
    project(0)
    grid.far(2)
    project(1)
    grid.last(2)
    kv_cross(0)
    grid.near(3)
    project(2)
    kv_cross(1)
    kv_ally(0)
    grid.far(3)
    kv_ally(1)
    kv_cross(2)
    grid.last(3)
    project(3)
    kv_ally(2)
    kv_cross(3)
    kv_ally(3)
    for r in range(CHUNKS):
        kv_mate(r)
    for d in range(1, 2 * SIDE):
        arrived(segall_ref.at[lax.rem(sp + d, 2 * SIDE)], sr.at[lax.rem(sp + d, 2 * SIDE)], tp, sp)
    for r in range(CHUNKS):
        grid.drain(r)
    for copy in w_sends + seg_copies + kv_sends:
        copy.wait_send()


def qkv_exchange(x_block, wqkv_block, seg_block):
    rows, width = x_block.shape
    depth, cols = wqkv_block.shape
    sps, tps = 2 * SIDE, SIDE * SIDE
    seg_tile = seg_block.reshape(rows // HEAD_DIM, HEAD_DIM)
    vmem = pl.BlockSpec(memory_space=pltpu.VMEM)
    dma = pltpu.SemaphoreType.DMA
    return pl.pallas_call(
        qkv_kernel,
        out_shape=(
            jax.ShapeDtypeStruct((2 * rows, HEAD_DIM), jnp.bfloat16),
            jax.ShapeDtypeStruct((sps * rows, 2 * HEAD_DIM), jnp.bfloat16),
            jax.ShapeDtypeStruct((sps,) + seg_tile.shape, jnp.int32),
        ),
        in_specs=[vmem] * 3,
        out_specs=(vmem,) * 3,
        scratch_shapes=[
            pltpu.VMEM((rows, tps * width), jnp.bfloat16),
            pltpu.VMEM((sps * depth, cols), jnp.bfloat16),
            pltpu.VMEM((2, rows, 3 * HEAD_DIM), jnp.bfloat16),
            dma((CHUNKS, 2, 15)), dma((CHUNKS, 2, tps)),
            dma((14,)), dma((sps, 2)),
            dma((sps,)), dma((sps,)),
            dma((8 * CHUNKS,)), dma((sps + 1, CHUNKS)),
        ],
        compiler_params=pltpu.CompilerParams(collective_id=0, has_side_effects=True, vmem_limit_bytes=56 * 1024 * 1024),
        name="qkv_exchange",
    )(x_block, wqkv_block, seg_tile)


def output_kernel(ctx_ref, w_ref, y_ref, o_all, w_all, part, os, orr, ws, wr, ms, mr, ys, yr):
    tp, sp = lax.axis_index("tp"), lax.axis_index("sp")
    z, y = tp // SIDE, lax.rem(tp, SIDE)
    x, core = sp // 2, lax.rem(sp, 2)
    rows = ctx_ref.shape[0] // 2
    quarter = rows // SIDE
    depth, width = w_ref.shape
    group = x // 2
    cross = (SIDE - 1 - x) * 2 + core
    mate = x * 2 + 1 - core

    def x_at(d):
        return lax.rem(x + d, SIDE) * 2 + core

    def z_at(d):
        return lax.rem(z + d, SIDE)

    def y_at(d):
        return lax.rem(y + d, SIDE)

    peers = [(z_at(d) * SIDE + y, sp) for d in (1, 2, 3)]
    peers += [(z_at(d) * SIDE + y, cross) for d in range(SIDE)]
    peers += [(z * SIDE + y_at(d), sp) for d in (1, 2, 3)]
    peers += [(tp, x_at(1)), (tp, x_at(3)), (tp, mate)]
    barrier_with(peers)

    o_sends = []

    def o_slot(j, yo, b):
        return (z_at(j) * SIDE + yo) * 2 + (group if b == 0 else 1 - group)

    def o_col(slot):
        return o_all.at[:, pl.ds(pl.multiple_of(slot * HEAD_DIM, HEAD_DIM), HEAD_DIM)]

    def o_send(src, slot, to_tp, to_sp):
        copy = remote(src, o_col(slot), os.at[len(o_sends)], orr.at[slot], to_tp, to_sp)
        copy.start()
        o_sends.append(copy)

    def o_wait(slot):
        arrived(o_col(slot), orr.at[slot], tp, sp)

    def ctx_rows(j, b):
        return ctx_ref.at[pl.ds(pl.multiple_of(b * rows + z_at(j) * quarter, quarter), quarter), :]

    def o_along_y(j, b, src):
        slot = o_slot(j, y, b)
        for d in (1, 3):
            o_send(src, slot, z * SIDE + y_at(d), sp)

    mine = (z * SIDE + y) * 2 + group
    order = [(0, 1), (1, 0), (3, 0), (1, 1), (3, 1), (2, 0), (2, 1)]
    for j, b in order:
        o_send(ctx_rows(j, b), mine, z_at(j) * SIDE + y, sp if b == 0 else cross)
    o_along_y(0, 0, ctx_rows(0, 0))
    o_all[:, pl.ds(pl.multiple_of(mine * HEAD_DIM, HEAD_DIM), HEAD_DIM)] = ctx_ref[pl.ds(pl.multiple_of(z * quarter, quarter), quarter), :]

    steps = 2
    chunk = depth // steps
    half = width // 2
    grid = Gather2D(
        (x, z), lambda u, v: (v * SIDE + y, u * 2 + core),
        lambda r, h: w_ref.at[pl.ds(r * chunk, chunk), pl.ds(h * half, half)],
        lambda r, h, u, v: w_all.at[pl.ds(pl.multiple_of((u * 2 + core) * depth + r * chunk, chunk), chunk),
                                    pl.ds(pl.multiple_of(v * width + h * half, half), half)],
        ws, wr)
    w_all[pl.ds(pl.multiple_of(sp * depth, depth), depth), pl.ds(pl.multiple_of(z * width, width), width)] = w_ref[...]

    def o_near(j, b):
        for d in (3, 1):
            slot = o_slot(j, y_at(d), b)
            o_wait(slot)
            if d == (3 if (j + b) % 2 == 0 else 1):
                o_send(o_col(slot), slot, z * SIDE + y_at(4 - d), sp)

    def o_first(j, b):
        o_wait(o_slot(j, y, b))
        o_along_y(j, b, o_col(o_slot(j, y, b)))

    m_sends = []

    def m_at(sx, other, dz, r):
        owner = lax.rem(x + sx, SIDE) * 2 + (1 - core if other else core)
        return w_all.at[pl.ds(pl.multiple_of(owner * depth + r * chunk, chunk), chunk),
                        pl.ds(pl.multiple_of(z_at(dz) * width, width), width)]

    def m_slot(sx, dz):
        return lax.rem(x + sx, SIDE) * SIDE + z_at(dz)

    def w_mate(r):
        for sx in range(SIDE):
            for dz in range(SIDE):
                src = w_ref.at[pl.ds(r * chunk, chunk), :] if (sx, dz) == (0, 0) else m_at(sx, False, dz, r)
                copy = remote(src, m_at(sx, False, dz, r), ms.at[len(m_sends)], mr.at[m_slot(sx, dz), r], tp, mate)
                copy.start()
                m_sends.append(copy)

    grid.start(0)
    for j, b in order[:3]:
        o_first(j, b)
    o_near(0, 0)
    grid.near(0)
    grid.start(1)
    for j, b in order[3:]:
        o_first(j, b)
    for j, b in order[:2]:
        o_near(j, b)
    grid.far(0)
    for j, b in order[2:4]:
        o_near(j, b)
    grid.last(0)
    w_mate(0)
    for j, b in order[4:]:
        o_near(j, b)
    grid.near(1)
    grid.far(1)
    grid.last(1)
    w_mate(1)
    for j, b in [(0, 0)] + order:
        o_wait(o_slot(j, y_at(2), b))
    for r in range(steps):
        for sx in range(SIDE):
            for dz in range(SIDE):
                arrived(m_at(sx, True, dz, r), mr.at[m_slot(sx, dz), r], tp, sp)

    y_sends = []
    strip = quarter // SIDE
    for zz in range(SIDE):
        out = jnp.dot(o_all[...], w_all[:, zz * width:(zz + 1) * width], preferred_element_type=jnp.float32)
        part[zz] = out.astype(jnp.bfloat16)
        cols = pl.ds(pl.multiple_of((zz * SIDE + y) * width, width), width)
        for d in (2, 1, 3):
            copy = remote(part.at[zz, pl.ds(pl.multiple_of(y_at(d) * strip, strip), strip), :], y_ref.at[:, cols],
                          ys.at[len(y_sends)], yr.at[zz, y], z * SIDE + y_at(d), sp)
            copy.start()
            y_sends.append(copy)
        y_ref[:, cols] = part[zz, pl.ds(pl.multiple_of(y * strip, strip), strip), :]
    for zz in range(SIDE):
        for d in (1, 3, 2):
            cols = pl.ds(pl.multiple_of((zz * SIDE + y_at(d)) * width, width), width)
            arrived(y_ref.at[:, cols], yr.at[zz, y_at(d)], tp, sp)
    for r in range(steps):
        grid.drain(r)
    for copy in o_sends + m_sends + y_sends:
        copy.wait_send()


def output_exchange(context, wout_block):
    rows = context.shape[0] // 2
    depth, width = wout_block.shape
    sps, tps = 2 * SIDE, SIDE * SIDE
    quarter = rows // SIDE
    vmem = pl.BlockSpec(memory_space=pltpu.VMEM)
    dma = pltpu.SemaphoreType.DMA
    return pl.pallas_call(
        output_kernel,
        out_shape=jax.ShapeDtypeStruct((quarter // SIDE, tps * width), jnp.bfloat16),
        in_specs=[vmem] * 2,
        out_specs=vmem,
        scratch_shapes=[
            pltpu.VMEM((quarter, tps * 2 * HEAD_DIM), jnp.bfloat16),
            pltpu.VMEM((sps * depth, SIDE * width), jnp.bfloat16),
            pltpu.VMEM((SIDE, quarter, width), jnp.bfloat16),
            dma((31,)), dma((2 * tps,)),
            dma((2, 2, 15)), dma((2, 2, tps)),
            dma((2 * tps,)), dma((tps, 2)),
            dma((3 * SIDE,)), dma((SIDE, SIDE)),
        ],
        compiler_params=pltpu.CompilerParams(collective_id=1, has_side_effects=True, vmem_limit_bytes=56 * 1024 * 1024),
        name="output_exchange",
    )(context, wout_block)


def solution(mesh):
    def device_block(x_block, doc_block, wqkv_block, wout_block):
        rows = x_block.shape[0]
        q, kv, seg_all = qkv_exchange(x_block, wqkv_block, doc_block)
        seg_all = seg_all.reshape(-1)
        sp = lax.axis_index("sp")
        cross = (SIDE - 1 - sp // 2) * 2 + sp % 2
        seg_q = jnp.concatenate([doc_block, lax.dynamic_slice(seg_all, (cross * rows,), (rows,))])
        context = attention(q, kv, seg_q, seg_all)
        return output_exchange(context, wout_block)

    return jax.shard_map(
        device_block,
        mesh=mesh,
        in_specs=(P(("dp", "sp"), "tp"), P(("dp", "sp")), P("sp", "tp"), P("sp", "tp")),
        out_specs=P(("dp", "sp", "tp"), None),
        check_vma=False,
    )
```

```python
import functools

import jax
import jax.numpy as jnp
from jax import lax
from jax.experimental import pallas as pl
from jax.experimental.pallas import tpu as pltpu
from jax.sharding import PartitionSpec as P

HEAD_DIM = 128
EXP2_SCALE = HEAD_DIM ** -0.5 * 1.4426950408889634
FLOOR = -3.0e38
SMALL = 2.0 ** -77


def seg_column(segq_ref, base, rows):
    tiles = [jnp.broadcast_to(segq_ref[pl.ds(base + i, 1), :], (HEAD_DIM, HEAD_DIM)).T for i in range(rows // HEAD_DIM)]
    return jnp.concatenate(tiles, axis=0)


def attention_kernel(qb, kb, sub, q_ref, kv_ref, segq_ref, segall_ref, o_ref, q2_ref, acc_ref, m_ref, l_ref, kmax_ref, segc_ref):
    step_id = pl.program_id(0)
    keys = kv_ref.shape[0]
    qrow = step_id * (qb // HEAD_DIM)

    @pl.when(step_id == 0)
    def _():
        def norms(j, best):
            k = kv_ref[pl.ds(pl.multiple_of(j * 2048, 2048), 2048), :HEAD_DIM].astype(jnp.float32)
            total = jnp.dot((k * k).astype(jnp.bfloat16), jnp.ones((HEAD_DIM, HEAD_DIM), jnp.bfloat16), preferred_element_type=jnp.float32)
            return jnp.maximum(best, jnp.max(total, axis=0, keepdims=True))

        kmax_ref[...] = jnp.broadcast_to(jnp.sqrt(lax.fori_loop(0, keys // 2048, norms, jnp.zeros((1, HEAD_DIM), jnp.float32))), kmax_ref.shape)

    segq = segq_ref[pl.ds(qrow, qb // HEAD_DIM), :]
    lo = jnp.min(segq)
    hi = jnp.max(segq)
    seg_all = segall_ref[...]
    first = jnp.sum(jnp.where(seg_all < lo, 1.0, 0.0)).astype(jnp.int32)
    last = jnp.sum(jnp.where(seg_all <= hi, 1.0, 0.0)).astype(jnp.int32)
    one_doc = lo == hi
    whole_rows = first // HEAD_DIM * HEAD_DIM
    count = (last - whole_rows + kb - 1) // kb
    base = jnp.minimum(whole_rows, keys - count * kb)

    q = q_ref[...]
    qf = q.astype(jnp.float32)
    bound = jnp.sqrt(jnp.sum(qf * qf, axis=1, keepdims=True)) * kmax_ref[:1, :] * (-1.01 / HEAD_DIM)
    q2_ref[:, :HEAD_DIM] = q
    q2_ref[:, HEAD_DIM:] = bound.astype(jnp.bfloat16)
    acc_ref[...] = jnp.zeros_like(acc_ref)
    segc_ref[...] = seg_column(segq_ref, qrow, qb)

    def same_doc(j, rows):
        row = jnp.concatenate([segall_ref[pl.ds(base // HEAD_DIM + j * (kb // HEAD_DIM) + i, 1), :] for i in range(kb // HEAD_DIM)], axis=1)
        return segc_ref[rows, :1] == row

    def pieces(j):
        start = pl.multiple_of(base + j * kb, HEAD_DIM)
        return kv_ref[pl.ds(start, kb), :HEAD_DIM], kv_ref[pl.ds(start, kb), HEAD_DIM:]

    ones = jnp.ones((kb, HEAD_DIM), jnp.bfloat16)

    def block(j, masked):
        k, v = pieces(j)
        k2 = jnp.concatenate([k, ones], axis=1)
        v2 = jnp.concatenate([v, ones], axis=1)
        for i in range(qb // sub):
            rows = slice(i * sub, (i + 1) * sub)
            s = lax.dot_general(q2_ref[rows, :], k2, (((1,), (1,)), ((), ())), preferred_element_type=jnp.float32)
            p = jnp.exp2(s * EXP2_SCALE)
            if masked:
                p = jnp.where(same_doc(j, rows), p, 0.0)
            acc_ref[rows, :] += jnp.dot(p.astype(jnp.bfloat16), v2, preferred_element_type=jnp.float32)

    def online(j, masked):
        k, v = pieces(j)
        for i in range(qb // sub):
            rows = slice(i * sub, (i + 1) * sub)
            s = lax.dot_general(q_ref[rows, :], k, (((1,), (1,)), ((), ())), preferred_element_type=jnp.float32)
            t = jnp.where(same_doc(j, rows), s * EXP2_SCALE, -jnp.inf)
            m_prev = m_ref[rows, :1]
            m_new = jnp.maximum(m_prev, jnp.max(t, axis=1, keepdims=True))
            p = jnp.exp2(t - m_new)
            alpha = jnp.exp2(m_prev - m_new)
            l_new = l_ref[rows, :1] * alpha + jnp.sum(p, axis=1, keepdims=True)
            pv = jnp.dot(p.astype(jnp.bfloat16), v, preferred_element_type=jnp.float32)
            acc_ref[rows, :HEAD_DIM] = acc_ref[rows, :HEAD_DIM] * alpha + pv
            m_ref[rows, :] = jnp.broadcast_to(m_new, (sub, HEAD_DIM))
            l_ref[rows, :] = jnp.broadcast_to(l_new, (sub, HEAD_DIM))

    def step(j, carry):
        whole = one_doc & (base + j * kb >= first) & (base + (j + 1) * kb <= last)

        @pl.when(whole)
        def _():
            block(j, False)

        @pl.when(jnp.logical_not(whole))
        def _():
            block(j, True)

        return carry

    lax.fori_loop(0, count, step, 0)
    total = acc_ref[:, HEAD_DIM:]
    o_ref[...] = (acc_ref[:, :HEAD_DIM] / total).astype(o_ref.dtype)

    @pl.when(jnp.logical_not(jnp.min(total) >= SMALL))
    def _():
        acc_ref[...] = jnp.zeros_like(acc_ref)
        l_ref[...] = jnp.zeros_like(l_ref)
        m_ref[...] = jnp.full_like(m_ref, FLOOR)

        def again(j, carry):
            online(j, True)
            return carry

        lax.fori_loop(0, count, again, 0)
        o_ref[...] = (acc_ref[:, :HEAD_DIM] / l_ref[...]).astype(o_ref.dtype)


def attention(q, kv, seg_q, seg_all, qb=1024, kb=1024, sub=256):
    rows, keys = q.shape[0], kv.shape[0]
    whole = lambda a: pl.BlockSpec(a, lambda i: (0, 0))
    f32 = lambda *shape: pltpu.VMEM(shape, jnp.float32)
    return pl.pallas_call(
        functools.partial(attention_kernel, qb, kb, sub),
        grid=(rows // qb,),
        out_shape=jax.ShapeDtypeStruct(q.shape, jnp.bfloat16),
        in_specs=[
            pl.BlockSpec((qb, HEAD_DIM), lambda i: (i, 0)),
            whole(kv.shape), whole(seg_q.shape), whole(seg_all.shape),
        ],
        out_specs=pl.BlockSpec((qb, HEAD_DIM), lambda i: (i, 0)),
        scratch_shapes=[
            pltpu.VMEM((qb, 2 * HEAD_DIM), jnp.bfloat16),
            f32(qb, 2 * HEAD_DIM), f32(qb, HEAD_DIM), f32(qb, HEAD_DIM), f32(8, HEAD_DIM),
            pltpu.VMEM((qb, HEAD_DIM), jnp.int32),
        ],
        compiler_params=pltpu.CompilerParams(vmem_limit_bytes=24 * 1024 * 1024),
        name="attention",
    )(q, kv, seg_q, seg_all)

SIDE = 4
CHUNKS = 4
MESH = pl.DeviceIdType.MESH


def remote(src, dst, send_sem, recv_sem, tp, sp):
    return pltpu.make_async_remote_copy(
        src_ref=src, dst_ref=dst, send_sem=send_sem, recv_sem=recv_sem,
        device_id={"tp": tp, "sp": sp}, device_id_type=MESH)


def arrived(ref, sem, tp, sp):
    remote(ref, ref, sem, sem, tp, sp).wait_recv()


def barrier_with(peers):
    barrier = pltpu.get_barrier_semaphore()
    for tp, sp in peers:
        pl.semaphore_signal(barrier, inc=1, device_id={"tp": tp, "sp": sp}, device_id_type=MESH)
    pl.semaphore_wait(barrier, len(peers))


class Gather2D:
    def __init__(self, coords, place, own, held, send_sem, recv_sem):
        self.coords, self.place, self.own, self.held = coords, place, own, held
        self.send_sem, self.recv_sem = send_sem, recv_sem
        self.sent = {}

    def at(self, h, j1, j2):
        u, v = self.coords
        j1, j2 = (j1, j2) if h == 0 else (j2, j1)
        return lax.rem(u + j1, SIDE), lax.rem(v + j2, SIDE)

    def send(self, r, h, piece, to):
        src_at, dst_at = self.at(h, *piece), self.at(h, *to)
        src = self.own(r, h) if piece == (0, 0) else self.held(r, h, *src_at)
        k = self.sent.get((r, h), 0)
        self.sent[r, h] = k + 1
        copy = remote(src, self.held(r, h, *src_at), self.send_sem.at[r, h, k],
                      self.recv_sem.at[r, h, src_at[0] * SIDE + src_at[1]], *self.place(*dst_at))
        copy.start()

    def wait(self, r, h, piece):
        src_at = self.at(h, *piece)
        arrived(self.held(r, h, *src_at), self.recv_sem.at[r, h, src_at[0] * SIDE + src_at[1]], *self.place(*self.coords))

    def start(self, r):
        for h in (0, 1):
            for to in ((1, 0), (3, 0), (0, 1), (0, 3)):
                self.send(r, h, (0, 0), to)

    def spread(self, r, h, j1):
        for j2 in (1, 3):
            self.send(r, h, (j1, 0), (0, j2))

    def near(self, r):
        for j1 in (3, 1):
            for h in (0, 1):
                self.wait(r, h, (j1, 0))
                if j1 == (3 if (r + h) % 2 == 0 else 1):
                    self.send(r, h, (j1, 0), (4 - j1, 0))
                self.spread(r, h, j1)

    def pass_on(self, r, j1):
        for h in (0, 1):
            for j2 in (3, 1):
                self.wait(r, h, (j1, j2))
                if j2 == (3 if (r + h + (j1 + 1) // 2) % 2 == 0 else 1):
                    self.send(r, h, (j1, j2), (0, 4 - j2))

    def far(self, r):
        self.pass_on(r, 0)
        for h in (0, 1):
            self.wait(r, h, (2, 0))
            self.spread(r, h, 2)

    def last(self, r):
        for j1 in (3, 1, 2):
            self.pass_on(r, j1)

    def final(self, r):
        for j1 in (0, 3, 1, 2):
            for h in (0, 1):
                self.wait(r, h, (j1, 2))

    def drain(self, r):
        for h in (0, 1):
            for k in range(self.sent[r, h]):
                ref = self.own(r, h)
                remote(ref, ref, self.send_sem.at[r, h, k], self.recv_sem.at[r, h, 0], *self.place(*self.coords)).wait_send()


def qkv_kernel(x_ref, w_ref, seg_ref, q_ref, kv_ref, segall_ref, segq_ref,
               x_all, w_all, qkv, xs, xr, ws, wr, ss, sr, ks, kr):
    tp, sp = lax.axis_index("tp"), lax.axis_index("sp")
    z, y = tp // SIDE, lax.rem(tp, SIDE)
    x, core = sp // 2, lax.rem(sp, 2)
    rows, width = x_ref.shape
    depth = w_ref.shape[0]
    chunk = rows // CHUNKS
    half = width // 2

    def sp_at(dx, other=0):
        return lax.rem(x + dx, SIDE) * 2 + lax.rem(core + other, 2)

    mate = sp_at(0, 1)
    group = x // 2
    ally = (x + 1 - 2 * lax.rem(x, 2)) * 2 + core
    cross = (SIDE - 1 - x) * 2 + core

    peers = [(lax.rem(z + d, SIDE) * SIDE + y, sp) for d in (1, 3)]
    peers += [(z * SIDE + lax.rem(y + d, SIDE), sp) for d in (1, 3)]
    peers += [(tp, lax.rem(sp + d, 2 * SIDE)) for d in range(1, 2 * SIDE)]
    barrier_with(peers)

    grid = Gather2D(
        (z, y), lambda u, v: (u * SIDE + v, sp),
        lambda r, h: x_ref.at[pl.ds(r * chunk, chunk), pl.ds(h * half, half)],
        lambda r, h, u, v: x_all.at[pl.ds(r * chunk, chunk), pl.ds(pl.multiple_of((u * SIDE + v) * width + h * half, half), half)],
        xs, xr)

    def w_at(owner, p):
        return w_all.at[pl.ds(pl.multiple_of(owner * depth + p * (depth // 2), depth // 2), depth // 2), :]

    w_sends = []

    def w_send(owner, p, to, src=None):
        k = len(w_sends)
        copy = remote(w_at(owner, p) if src is None else src, w_at(owner, p), ws.at[k], wr.at[owner, p], tp, to)
        copy.start()
        w_sends.append(copy)

    def w_wait(owner, p):
        arrived(w_at(owner, p), wr.at[owner, p], tp, sp)

    def w_own(p):
        src = w_ref.at[pl.ds(p * (depth // 2), depth // 2), :]
        for to in (sp_at(1), sp_at(3), mate):
            w_send(sp, p, to, src)

    def w_near(p):
        for d in (3, 1):
            w_wait(sp_at(d), p)
            if d == (3 if p == 0 else 1):
                w_send(sp_at(d), p, sp_at(4 - d))
            w_send(sp_at(d), p, mate)

    def w_far():
        for p in (0, 1):
            w_wait(sp_at(2), p)
            w_send(sp_at(2), p, mate)

    def w_mate():
        for p in (0, 1):
            for d in (0, 1, 3, 2):
                w_wait(sp_at(d, 1), p)

    grid.start(0)
    w_own(0)
    seg_copies = []
    for d in range(1, 2 * SIDE):
        copy = remote(seg_ref, segall_ref.at[sp], ss.at[d], sr.at[sp], tp, lax.rem(sp + d, 2 * SIDE))
        copy.start()
        seg_copies.append(copy)
    segall_ref[sp] = seg_ref[...]
    x_all[:, pl.ds(pl.multiple_of(tp * width, width), width)] = x_ref[...]
    w_all[pl.ds(pl.multiple_of(sp * depth, depth), depth), :] = w_ref[...]

    def kv_at(owner, r):
        return kv_ref.at[pl.ds(pl.multiple_of(owner * rows + r * chunk, chunk), chunk), :]

    kv_sends = []

    def kv_send(src, dst, recv, to):
        k = len(kv_sends)
        copy = remote(src, dst, ks.at[k], recv, tp, to)
        copy.start()
        kv_sends.append(copy)

    def project(r):
        here = slice(r * chunk, (r + 1) * chunk)
        for n in range(3):
            part = slice(n * 256, (n + 1) * 256)
            out = jnp.dot(x_all[here, :], w_all[:, part], preferred_element_type=jnp.float32).astype(jnp.bfloat16)
            for m in range(2):
                col = n * 2 + m
                qkv[col // 3, here, (col % 3) * HEAD_DIM:(col % 3 + 1) * HEAD_DIM] = out[:, m * HEAD_DIM:(m + 1) * HEAD_DIM]
        q_ref[here, :] = qkv[group, here, :HEAD_DIM]
        kv_ref[pl.ds(pl.multiple_of(sp * rows + r * chunk, chunk), chunk), :] = qkv[group, here, HEAD_DIM:]
        span = pl.ds(r * chunk, chunk)
        kv_send(qkv.at[1 - group, span, pl.ds(HEAD_DIM, 2 * HEAD_DIM)], kv_at(sp, r), kr.at[sp, r], cross)
        kv_send(qkv.at[1 - group, span, pl.ds(0, HEAD_DIM)], q_ref.at[pl.ds(rows + r * chunk, chunk), :], kr.at[2 * SIDE, r], cross)
        kv_send(qkv.at[group, span, pl.ds(HEAD_DIM, 2 * HEAD_DIM)], kv_at(sp, r), kr.at[sp, r], ally)
        kv_send(qkv.at[group, span, pl.ds(HEAD_DIM, 2 * HEAD_DIM)], kv_at(sp, r), kr.at[sp, r], mate)

    ally_cross = lax.rem(x + 2, SIDE) * 2 + core

    def kv_wait(owner, r):
        arrived(kv_at(owner, r), kr.at[owner, r], tp, sp)

    def kv_cross(r):
        kv_wait(cross, r)
        kv_send(kv_at(cross, r), kv_at(cross, r), kr.at[cross, r], ally)
        kv_send(kv_at(cross, r), kv_at(cross, r), kr.at[cross, r], mate)

    def kv_ally(r):
        for owner in (ally, ally_cross):
            kv_wait(owner, r)
            kv_send(kv_at(owner, r), kv_at(owner, r), kr.at[owner, r], mate)

    def kv_mate(r):
        arrived(q_ref.at[pl.ds(rows + r * chunk, chunk), :], kr.at[2 * SIDE, r], tp, sp)
        for d in range(SIDE):
            kv_wait(sp_at(d, 1), r)

    grid.near(0)
    w_own(1)
    grid.start(1)
    grid.far(0)
    grid.near(1)
    grid.last(0)
    w_near(0)
    grid.start(2)
    grid.far(1)
    grid.near(2)
    w_near(1)
    grid.last(1)
    grid.start(3)
    grid.far(2)
    w_far()
    w_mate()
    grid.final(0)
    project(0)
    grid.near(3)
    grid.final(1)
    project(1)
    grid.last(2)
    kv_cross(0)
    grid.far(3)
    kv_cross(1)
    kv_ally(0)
    grid.final(2)
    project(2)
    kv_ally(1)
    grid.last(3)
    kv_cross(2)
    grid.final(3)
    project(3)
    kv_ally(2)
    kv_cross(3)
    kv_ally(3)
    for r in range(CHUNKS):
        kv_mate(r)
    for d in range(1, 2 * SIDE):
        arrived(segall_ref.at[lax.rem(sp + d, 2 * SIDE)], sr.at[lax.rem(sp + d, 2 * SIDE)], tp, sp)
    segq_ref[0] = seg_ref[...]
    segq_ref[1] = segall_ref[cross]
    for r in range(CHUNKS):
        grid.drain(r)
    for copy in w_sends + seg_copies + kv_sends:
        copy.wait_send()


def qkv_exchange(x_block, wqkv_block, seg_block):
    rows, width = x_block.shape
    depth, cols = wqkv_block.shape
    sps, tps = 2 * SIDE, SIDE * SIDE
    seg_tile = seg_block.reshape(rows // HEAD_DIM, HEAD_DIM)
    vmem = pl.BlockSpec(memory_space=pltpu.VMEM)
    dma = pltpu.SemaphoreType.DMA
    return pl.pallas_call(
        qkv_kernel,
        out_shape=(
            jax.ShapeDtypeStruct((2 * rows, HEAD_DIM), jnp.bfloat16),
            jax.ShapeDtypeStruct((sps * rows, 2 * HEAD_DIM), jnp.bfloat16),
            jax.ShapeDtypeStruct((sps,) + seg_tile.shape, jnp.int32),
            jax.ShapeDtypeStruct((2,) + seg_tile.shape, jnp.int32),
        ),
        in_specs=[vmem] * 3,
        out_specs=(vmem,) * 4,
        scratch_shapes=[
            pltpu.VMEM((rows, tps * width), jnp.bfloat16),
            pltpu.VMEM((sps * depth, cols), jnp.bfloat16),
            pltpu.VMEM((2, rows, 3 * HEAD_DIM), jnp.bfloat16),
            dma((CHUNKS, 2, 15)), dma((CHUNKS, 2, tps)),
            dma((14,)), dma((sps, 2)),
            dma((sps,)), dma((sps,)),
            dma((8 * CHUNKS,)), dma((sps + 1, CHUNKS)),
        ],
        compiler_params=pltpu.CompilerParams(collective_id=0, has_side_effects=True, vmem_limit_bytes=26 * 1024 * 1024),
        name="qkv_exchange",
    )(x_block, wqkv_block, seg_tile)


def output_kernel(ctx_ref, w_ref, y_ref, o_all, w_all, part, os, orr, ws, wr, ms, mr, ys, yr):
    tp, sp = lax.axis_index("tp"), lax.axis_index("sp")
    z, y = tp // SIDE, lax.rem(tp, SIDE)
    x, core = sp // 2, lax.rem(sp, 2)
    rows = ctx_ref.shape[0] // 2
    quarter = rows // SIDE
    depth, width = w_ref.shape
    group = x // 2
    cross = (SIDE - 1 - x) * 2 + core
    mate = x * 2 + 1 - core

    def x_at(d):
        return lax.rem(x + d, SIDE) * 2 + core

    def z_at(d):
        return lax.rem(z + d, SIDE)

    def y_at(d):
        return lax.rem(y + d, SIDE)

    peers = [(z_at(d) * SIDE + y, sp) for d in (1, 2, 3)]
    peers += [(z_at(d) * SIDE + y, cross) for d in range(SIDE)]
    peers += [(z * SIDE + y_at(d), sp) for d in (1, 2, 3)]
    peers += [(tp, x_at(1)), (tp, x_at(3)), (tp, mate)]
    barrier_with(peers)

    o_sends = []

    def o_slot(j, yo, b):
        return (z_at(j) * SIDE + yo) * 2 + (group if b == 0 else 1 - group)

    def o_col(slot):
        return o_all.at[:, pl.ds(pl.multiple_of(slot * HEAD_DIM, HEAD_DIM), HEAD_DIM)]

    def o_send(src, slot, to_tp, to_sp):
        copy = remote(src, o_col(slot), os.at[len(o_sends)], orr.at[slot], to_tp, to_sp)
        copy.start()
        o_sends.append(copy)

    def o_wait(slot):
        arrived(o_col(slot), orr.at[slot], tp, sp)

    def ctx_rows(j, b):
        return ctx_ref.at[pl.ds(pl.multiple_of(b * rows + z_at(j) * quarter, quarter), quarter), :]

    def o_along_y(j, b, src):
        slot = o_slot(j, y, b)
        for d in (1, 3):
            o_send(src, slot, z * SIDE + y_at(d), sp)

    mine = (z * SIDE + y) * 2 + group
    order = [(0, 1), (1, 0), (3, 0), (1, 1), (3, 1), (2, 0), (2, 1)]
    for j, b in order:
        o_send(ctx_rows(j, b), mine, z_at(j) * SIDE + y, sp if b == 0 else cross)
    o_along_y(0, 0, ctx_rows(0, 0))
    o_all[:, pl.ds(pl.multiple_of(mine * HEAD_DIM, HEAD_DIM), HEAD_DIM)] = ctx_ref[pl.ds(pl.multiple_of(z * quarter, quarter), quarter), :]

    steps = 2
    chunk = depth // steps
    half = width // 2
    grid = Gather2D(
        (x, z), lambda u, v: (v * SIDE + y, u * 2 + core),
        lambda r, h: w_ref.at[pl.ds(r * chunk, chunk), pl.ds(h * half, half)],
        lambda r, h, u, v: w_all.at[pl.ds(pl.multiple_of((u * 2 + core) * depth + r * chunk, chunk), chunk),
                                    pl.ds(pl.multiple_of(v * width + h * half, half), half)],
        ws, wr)
    w_all[pl.ds(pl.multiple_of(sp * depth, depth), depth), pl.ds(pl.multiple_of(z * width, width), width)] = w_ref[...]

    def o_near(j, b):
        for d in (3, 1):
            slot = o_slot(j, y_at(d), b)
            o_wait(slot)
            if d == (3 if (j + b) % 2 == 0 else 1):
                o_send(o_col(slot), slot, z * SIDE + y_at(4 - d), sp)

    def o_first(j, b):
        o_wait(o_slot(j, y, b))
        o_along_y(j, b, o_col(o_slot(j, y, b)))

    m_sends = []

    def m_at(sx, other, dz, r):
        owner = lax.rem(x + sx, SIDE) * 2 + (1 - core if other else core)
        return w_all.at[pl.ds(pl.multiple_of(owner * depth + r * chunk, chunk), chunk),
                        pl.ds(pl.multiple_of(z_at(dz) * width, width), width)]

    def m_slot(sx, dz):
        return lax.rem(x + sx, SIDE) * SIDE + z_at(dz)

    def w_mate(r):
        for sx in range(SIDE):
            for dz in range(SIDE):
                src = w_ref.at[pl.ds(r * chunk, chunk), :] if (sx, dz) == (0, 0) else m_at(sx, False, dz, r)
                copy = remote(src, m_at(sx, False, dz, r), ms.at[len(m_sends)], mr.at[m_slot(sx, dz), r], tp, mate)
                copy.start()
                m_sends.append(copy)

    grid.start(0)
    for j, b in order[:3]:
        o_first(j, b)
    o_near(0, 0)
    grid.near(0)
    grid.start(1)
    for j, b in order[3:]:
        o_first(j, b)
    for j, b in order[:2]:
        o_near(j, b)
    grid.far(0)
    for j, b in order[2:4]:
        o_near(j, b)
    grid.last(0)
    grid.final(0)
    w_mate(0)
    for j, b in order[4:]:
        o_near(j, b)
    grid.near(1)
    grid.far(1)
    grid.last(1)
    grid.final(1)
    w_mate(1)
    for j, b in [(0, 0)] + order:
        o_wait(o_slot(j, y_at(2), b))
    for r in range(steps):
        for sx in range(SIDE):
            for dz in range(SIDE):
                arrived(m_at(sx, True, dz, r), mr.at[m_slot(sx, dz), r], tp, sp)

    y_sends = []
    strip = quarter // SIDE
    for zz in range(SIDE):
        out = jnp.dot(o_all[...], w_all[:, zz * width:(zz + 1) * width], preferred_element_type=jnp.float32)
        part[zz] = out.astype(jnp.bfloat16)
        cols = pl.ds(pl.multiple_of((zz * SIDE + y) * width, width), width)
        for d in (2, 1, 3):
            copy = remote(part.at[zz, pl.ds(pl.multiple_of(y_at(d) * strip, strip), strip), :], y_ref.at[:, cols],
                          ys.at[len(y_sends)], yr.at[zz, y], z * SIDE + y_at(d), sp)
            copy.start()
            y_sends.append(copy)
        y_ref[:, cols] = part[zz, pl.ds(pl.multiple_of(y * strip, strip), strip), :]
    for zz in range(SIDE):
        for d in (1, 3, 2):
            cols = pl.ds(pl.multiple_of((zz * SIDE + y_at(d)) * width, width), width)
            arrived(y_ref.at[:, cols], yr.at[zz, y_at(d)], tp, sp)
    for r in range(steps):
        grid.drain(r)
    for copy in o_sends + m_sends + y_sends:
        copy.wait_send()


def output_exchange(context, wout_block):
    rows = context.shape[0] // 2
    depth, width = wout_block.shape
    sps, tps = 2 * SIDE, SIDE * SIDE
    quarter = rows // SIDE
    vmem = pl.BlockSpec(memory_space=pltpu.VMEM)
    dma = pltpu.SemaphoreType.DMA
    return pl.pallas_call(
        output_kernel,
        out_shape=jax.ShapeDtypeStruct((quarter // SIDE, tps * width), jnp.bfloat16),
        in_specs=[vmem] * 2,
        out_specs=vmem,
        scratch_shapes=[
            pltpu.VMEM((quarter, tps * 2 * HEAD_DIM), jnp.bfloat16),
            pltpu.VMEM((sps * depth, SIDE * width), jnp.bfloat16),
            pltpu.VMEM((SIDE, quarter, width), jnp.bfloat16),
            dma((31,)), dma((2 * tps,)),
            dma((2, 2, 15)), dma((2, 2, tps)),
            dma((2 * tps,)), dma((tps, 2)),
            dma((3 * SIDE,)), dma((SIDE, SIDE)),
        ],
        compiler_params=pltpu.CompilerParams(collective_id=1, has_side_effects=True, vmem_limit_bytes=16 * 1024 * 1024),
        name="output_exchange",
    )(context, wout_block)


def solution(mesh):
    def device_block(x_block, doc_block, wqkv_block, wout_block):
        q, kv, seg_all, seg_q = qkv_exchange(x_block, wqkv_block, doc_block)
        context = attention(q, kv, seg_q.reshape(-1, HEAD_DIM), seg_all.reshape(-1, HEAD_DIM))
        return output_exchange(context, wout_block)

    return jax.shard_map(
        device_block,
        mesh=mesh,
        in_specs=(P(("dp", "sp"), "tp"), P(("dp", "sp")), P("sp", "tp"), P("sp", "tp")),
        out_specs=P(("dp", "sp", "tp"), None),
        check_vma=False,
    )
```

```python
import functools

import jax
import jax.numpy as jnp
from jax import lax
from jax.experimental import pallas as pl
from jax.experimental.pallas import tpu as pltpu
from jax.sharding import PartitionSpec as P

HEAD_DIM = 128
EXP2_SCALE = HEAD_DIM ** -0.5 * 1.4426950408889634
FLOOR = -3.0e38
SMALL = 2.0 ** -77
LARGE = 2.0 ** 15


def seg_column(segq_ref, base, rows):
    tiles = [jnp.broadcast_to(segq_ref[pl.ds(base + i, 1), :], (HEAD_DIM, HEAD_DIM)).T for i in range(rows // HEAD_DIM)]
    return jnp.concatenate(tiles, axis=0)


def attention_kernel(qb, kb, sub, q_ref, kv_ref, segq_ref, segall_ref, o_ref, q2_ref, acc_ref, m_ref, l_ref, kmax_ref, segc_ref):
    step_id = pl.program_id(0)
    keys = kv_ref.shape[0]
    qrow = step_id * (qb // HEAD_DIM)

    @pl.when(step_id == 0)
    def _():
        def norms(j, best):
            k = kv_ref[pl.ds(pl.multiple_of(j * 2048, 2048), 2048), :HEAD_DIM].astype(jnp.float32)
            total = jnp.dot((k * k).astype(jnp.bfloat16), jnp.ones((HEAD_DIM, HEAD_DIM), jnp.bfloat16), preferred_element_type=jnp.float32)
            return jnp.maximum(best, jnp.max(total.reshape(-1, 8, HEAD_DIM), axis=0))

        kmax_ref[...] = jnp.sqrt(lax.fori_loop(0, keys // 2048, norms, jnp.zeros(kmax_ref.shape, jnp.float32)))

    segq = segq_ref[pl.ds(qrow, qb // HEAD_DIM), :]
    lo = jnp.min(segq)
    hi = jnp.max(segq)
    seg_all = segall_ref[...]
    first = jnp.sum(jnp.where(seg_all < lo, 1.0, 0.0)).astype(jnp.int32)
    last = jnp.sum(jnp.where(seg_all <= hi, 1.0, 0.0)).astype(jnp.int32)
    one_doc = lo == hi
    whole_rows = first // HEAD_DIM * HEAD_DIM
    units = (last - whole_rows + 256 - 1) // 256
    base = jnp.minimum(whole_rows, keys - units * 256)
    count = units * 256 // kb
    rest = units - count * (kb // 256)

    q = q_ref[...]
    qf = q.astype(jnp.float32)
    bound = jnp.sqrt(jnp.sum(qf * qf, axis=1, keepdims=True)) * jnp.max(kmax_ref[...], axis=0, keepdims=True) * (-1.01 / HEAD_DIM)
    q2_ref[:, :HEAD_DIM] = q
    q2_ref[:, HEAD_DIM:] = bound.astype(jnp.bfloat16)
    acc_ref[...] = jnp.zeros_like(acc_ref)
    segc_ref[...] = seg_column(segq_ref, qrow, qb)

    def same_doc(start, size, rows):
        row = jnp.concatenate([segall_ref[pl.ds(start // HEAD_DIM + i, 1), :] for i in range(size // HEAD_DIM)], axis=1)
        return segc_ref[rows, :1] == row

    def pieces(start, size):
        rows = pl.ds(pl.multiple_of(start, HEAD_DIM), size)
        return kv_ref[rows, :HEAD_DIM], kv_ref[rows, HEAD_DIM:]

    def block(start, size, masked):
        k, v = pieces(start, size)
        ones = jnp.ones((size, HEAD_DIM), jnp.bfloat16)
        k2 = jnp.concatenate([k, ones], axis=1)
        v2 = jnp.concatenate([v, ones], axis=1)
        for i in range(qb // sub):
            rows = slice(i * sub, (i + 1) * sub)
            s = lax.dot_general(q2_ref[rows, :], k2, (((1,), (1,)), ((), ())), preferred_element_type=jnp.float32)
            p = jnp.exp2(s * EXP2_SCALE)
            if masked:
                p = jnp.where(same_doc(start, size, rows), p, 0.0)
            acc_ref[rows, :] += jnp.dot(p.astype(jnp.bfloat16), v2, preferred_element_type=jnp.float32)

    def online(start, size):
        k, v = pieces(start, size)
        for i in range(qb // sub):
            rows = slice(i * sub, (i + 1) * sub)
            s = lax.dot_general(q_ref[rows, :], k, (((1,), (1,)), ((), ())), preferred_element_type=jnp.float32)
            t = jnp.where(same_doc(start, size, rows), s * EXP2_SCALE, -jnp.inf)
            m_prev = m_ref[rows, :1]
            m_new = jnp.maximum(m_prev, jnp.max(t, axis=1, keepdims=True))
            p = jnp.exp2(t - m_new)
            alpha = jnp.exp2(m_prev - m_new)
            l_new = l_ref[rows, :1] * alpha + jnp.sum(p, axis=1, keepdims=True)
            pv = jnp.dot(p.astype(jnp.bfloat16), v, preferred_element_type=jnp.float32)
            acc_ref[rows, :HEAD_DIM] = acc_ref[rows, :HEAD_DIM] * alpha + pv
            m_ref[rows, :] = jnp.broadcast_to(m_new, (sub, HEAD_DIM))
            l_ref[rows, :] = jnp.broadcast_to(l_new, (sub, HEAD_DIM))

    def step(j, carry):
        whole = one_doc & (base + j * kb >= first) & (base + (j + 1) * kb <= last)

        @pl.when(whole)
        def _():
            block(base + j * kb, kb, False)

        @pl.when(jnp.logical_not(whole))
        def _():
            block(base + j * kb, kb, True)

        return carry

    lax.fori_loop(0, count, step, 0)

    size = kb // 2
    while size >= 256:
        @pl.when(rest // (size // 256) % 2 == 1)
        def _(size=size):
            block(base + count * kb + rest // (2 * size // 256) * (2 * size), size, True)

        size //= 2

    total = acc_ref[:, HEAD_DIM:]
    o_ref[...] = (acc_ref[:, :HEAD_DIM] / total).astype(o_ref.dtype)

    @pl.when(jnp.logical_not((jnp.min(total) >= SMALL) & (jnp.max(total) <= LARGE)))
    def _():
        acc_ref[...] = jnp.zeros_like(acc_ref)
        l_ref[...] = jnp.zeros_like(l_ref)
        m_ref[...] = jnp.full_like(m_ref, FLOOR)

        def again(j, carry):
            online(base + j * 256, 256)
            return carry

        lax.fori_loop(0, units, again, 0)
        o_ref[...] = (acc_ref[:, :HEAD_DIM] / l_ref[...]).astype(o_ref.dtype)


def attention(q, kv, seg_q, seg_all, qb=1024, kb=1024, sub=256):
    rows, keys = q.shape[0], kv.shape[0]
    whole = lambda a: pl.BlockSpec(a, lambda i: (0, 0))
    f32 = lambda *shape: pltpu.VMEM(shape, jnp.float32)
    return pl.pallas_call(
        functools.partial(attention_kernel, qb, kb, sub),
        grid=(rows // qb,),
        out_shape=jax.ShapeDtypeStruct(q.shape, jnp.bfloat16),
        in_specs=[
            pl.BlockSpec((qb, HEAD_DIM), lambda i: (i, 0)),
            whole(kv.shape), whole(seg_q.shape), whole(seg_all.shape),
        ],
        out_specs=pl.BlockSpec((qb, HEAD_DIM), lambda i: (i, 0)),
        scratch_shapes=[
            pltpu.VMEM((qb, 2 * HEAD_DIM), jnp.bfloat16),
            f32(qb, 2 * HEAD_DIM), f32(qb, HEAD_DIM), f32(qb, HEAD_DIM), f32(8, HEAD_DIM),
            pltpu.VMEM((qb, HEAD_DIM), jnp.int32),
        ],
        compiler_params=pltpu.CompilerParams(vmem_limit_bytes=24 * 1024 * 1024),
        name="attention",
    )(q, kv, seg_q, seg_all)

SIDE = 4
CUTS = (0, 8, 16, 24, 32)
CHUNKS = len(CUTS) - 1
MESH = pl.DeviceIdType.MESH


def remote(src, dst, send_sem, recv_sem, tp, sp):
    return pltpu.make_async_remote_copy(
        src_ref=src, dst_ref=dst, send_sem=send_sem, recv_sem=recv_sem,
        device_id={"tp": tp, "sp": sp}, device_id_type=MESH)


def arrived(ref, sem, tp, sp):
    remote(ref, ref, sem, sem, tp, sp).wait_recv()


def barrier_with(peers):
    barrier = pltpu.get_barrier_semaphore()
    for tp, sp in peers:
        pl.semaphore_signal(barrier, inc=1, device_id={"tp": tp, "sp": sp}, device_id_type=MESH)
    pl.semaphore_wait(barrier, len(peers))


class Gather2D:
    def __init__(self, coords, place, own, held, send_sem, recv_sem, on_arrival=None):
        self.coords, self.place, self.own, self.held = coords, place, own, held
        self.send_sem, self.recv_sem, self.on_arrival = send_sem, recv_sem, on_arrival
        self.sent = {}

    def at(self, h, j1, j2):
        u, v = self.coords
        j1, j2 = (j1, j2) if h == 0 else (j2, j1)
        return lax.rem(u + j1, SIDE), lax.rem(v + j2, SIDE)

    def send(self, r, h, piece, to):
        src_at, dst_at = self.at(h, *piece), self.at(h, *to)
        src = self.own(r, h) if piece == (0, 0) else self.held(r, h, *src_at)
        k = self.sent.get((r, h), 0)
        self.sent[r, h] = k + 1
        copy = remote(src, self.held(r, h, *src_at), self.send_sem.at[r, h, k],
                      self.recv_sem.at[r, h, src_at[0] * SIDE + src_at[1]], *self.place(*dst_at))
        copy.start()

    def wait(self, r, h, piece):
        src_at = self.at(h, *piece)
        arrived(self.held(r, h, *src_at), self.recv_sem.at[r, h, src_at[0] * SIDE + src_at[1]], *self.place(*self.coords))
        if self.on_arrival is not None:
            self.on_arrival(r, h, *src_at)

    def start(self, r):
        for h in (0, 1):
            for to in ((1, 0), (3, 0), (0, 1), (0, 3)):
                self.send(r, h, (0, 0), to)

    def spread(self, r, h, j1):
        for j2 in (1, 3):
            self.send(r, h, (j1, 0), (0, j2))

    def near(self, r):
        for j1 in (3, 1):
            for h in (0, 1):
                self.wait(r, h, (j1, 0))
                if j1 == (3 if (r + h) % 2 == 0 else 1):
                    self.send(r, h, (j1, 0), (4 - j1, 0))
                self.spread(r, h, j1)

    def pass_on(self, r, j1):
        for h in (0, 1):
            for j2 in (3, 1):
                self.wait(r, h, (j1, j2))
                if j2 == (3 if (r + h + (j1 + 1) // 2) % 2 == 0 else 1):
                    self.send(r, h, (j1, j2), (0, 4 - j2))

    def far(self, r):
        self.pass_on(r, 0)
        for h in (0, 1):
            self.wait(r, h, (2, 0))
            self.spread(r, h, 2)

    def last(self, r):
        for j1 in (3, 1, 2):
            self.pass_on(r, j1)

    def final(self, r):
        for j1 in (0, 3, 1, 2):
            for h in (0, 1):
                self.wait(r, h, (j1, 2))

    def drain(self, r):
        for h in (0, 1):
            for k in range(self.sent[r, h]):
                ref = self.own(r, h)
                remote(ref, ref, self.send_sem.at[r, h, k], self.recv_sem.at[r, h, 0], *self.place(*self.coords)).wait_send()


def qkv_kernel(x_ref, w_ref, seg_ref, q_ref, kv_ref, segall_ref, segq_ref,
               x_all, w_all, qkv, ls, xs, xr, ws, wr, ss, sr, ks, kr):
    tp, sp = lax.axis_index("tp"), lax.axis_index("sp")
    z, y = tp // SIDE, lax.rem(tp, SIDE)
    x, core = sp // 2, lax.rem(sp, 2)
    rows, width = x_ref.shape
    depth = w_ref.shape[0]
    cuts = [rows * c // CUTS[-1] for c in CUTS]
    size = [b - a for a, b in zip(cuts, cuts[1:])]
    half = width // 2

    def sp_at(dx, other=0):
        return lax.rem(x + dx, SIDE) * 2 + lax.rem(core + other, 2)

    mate = sp_at(0, 1)
    group = x // 2
    ally = (x + 1 - 2 * lax.rem(x, 2)) * 2 + core
    cross = (SIDE - 1 - x) * 2 + core

    peers = [(lax.rem(z + d, SIDE) * SIDE + y, sp) for d in (1, 3)]
    peers += [(z * SIDE + lax.rem(y + d, SIDE), sp) for d in (1, 3)]
    peers += [(tp, lax.rem(sp + d, 2 * SIDE)) for d in range(1, 2 * SIDE)]
    x_own = x_all.at[:, pl.ds(pl.multiple_of(tp * width, width), width)]
    w_own_rows = w_all.at[pl.ds(pl.multiple_of(sp * depth, depth), depth), :]
    loads = [pltpu.make_async_copy(x_ref, x_own, ls.at[0]), pltpu.make_async_copy(w_ref, w_own_rows, ls.at[1])]
    for load in loads:
        load.start()
    barrier_with(peers)
    for load in loads:
        load.wait()

    grid = Gather2D(
        (z, y), lambda u, v: (u * SIDE + v, sp),
        lambda r, h: x_own.at[pl.ds(cuts[r], size[r]), pl.ds(h * half, half)],
        lambda r, h, u, v: x_all.at[pl.ds(cuts[r], size[r]), pl.ds(pl.multiple_of((u * SIDE + v) * width + h * half, half), half)],
        xs, xr)

    def w_at(owner, p):
        return w_all.at[pl.ds(pl.multiple_of(owner * depth + p * (depth // 2), depth // 2), depth // 2), :]

    w_sends = []

    def w_send(owner, p, to):
        k = len(w_sends)
        copy = remote(w_at(owner, p), w_at(owner, p), ws.at[k], wr.at[owner, p], tp, to)
        copy.start()
        w_sends.append(copy)

    def w_wait(owner, p):
        arrived(w_at(owner, p), wr.at[owner, p], tp, sp)

    def w_own(p):
        for to in (sp_at(1), sp_at(3), mate):
            w_send(sp, p, to)

    def w_near(p):
        for d in (3, 1):
            w_wait(sp_at(d), p)
            if d == (3 if p == 0 else 1):
                w_send(sp_at(d), p, sp_at(4 - d))
            w_send(sp_at(d), p, mate)

    def w_far():
        for p in (0, 1):
            w_wait(sp_at(2), p)
            w_send(sp_at(2), p, mate)

    def w_mate():
        for p in (0, 1):
            for d in (0, 1, 3, 2):
                w_wait(sp_at(d, 1), p)

    grid.start(0)
    w_own(0)
    seg_copies = []
    for d in range(1, 2 * SIDE):
        copy = remote(seg_ref, segall_ref.at[sp], ss.at[d], sr.at[sp], tp, lax.rem(sp + d, 2 * SIDE))
        copy.start()
        seg_copies.append(copy)
    segall_ref[sp] = seg_ref[...]

    def kv_at(owner, r):
        return kv_ref.at[pl.ds(pl.multiple_of(owner * rows + cuts[r], 64), size[r]), :]

    kv_sends = []

    def kv_send(src, dst, recv, to):
        k = len(kv_sends)
        copy = remote(src, dst, ks.at[k], recv, tp, to)
        copy.start()
        kv_sends.append(copy)

    def project(r):
        here = slice(cuts[r], cuts[r + 1])
        for n in range(3):
            part = slice(n * 256, (n + 1) * 256)
            out = jnp.dot(x_all[here, :], w_all[:, part], preferred_element_type=jnp.float32).astype(jnp.bfloat16)
            for m in range(2):
                col = n * 2 + m
                qkv[col // 3, here, (col % 3) * HEAD_DIM:(col % 3 + 1) * HEAD_DIM] = out[:, m * HEAD_DIM:(m + 1) * HEAD_DIM]
        q_ref[here, :] = qkv[group, here, :HEAD_DIM]
        kv_ref[pl.ds(pl.multiple_of(sp * rows + cuts[r], 64), size[r]), :] = qkv[group, here, HEAD_DIM:]
        span = pl.ds(cuts[r], size[r])
        kv_send(qkv.at[1 - group, span, pl.ds(HEAD_DIM, 2 * HEAD_DIM)], kv_at(sp, r), kr.at[sp, r], cross)
        kv_send(qkv.at[1 - group, span, pl.ds(0, HEAD_DIM)], q_ref.at[pl.ds(rows + cuts[r], size[r]), :], kr.at[2 * SIDE, r], cross)
        kv_send(qkv.at[group, span, pl.ds(HEAD_DIM, 2 * HEAD_DIM)], kv_at(sp, r), kr.at[sp, r], ally)
        kv_send(qkv.at[group, span, pl.ds(HEAD_DIM, 2 * HEAD_DIM)], kv_at(sp, r), kr.at[sp, r], mate)

    ally_cross = lax.rem(x + 2, SIDE) * 2 + core

    def kv_wait(owner, r):
        arrived(kv_at(owner, r), kr.at[owner, r], tp, sp)

    def kv_cross(r):
        kv_wait(cross, r)
        kv_send(kv_at(cross, r), kv_at(cross, r), kr.at[cross, r], ally)
        kv_send(kv_at(cross, r), kv_at(cross, r), kr.at[cross, r], mate)

    def kv_ally(r):
        for owner in (ally, ally_cross):
            kv_wait(owner, r)
            kv_send(kv_at(owner, r), kv_at(owner, r), kr.at[owner, r], mate)

    def kv_mate(r):
        arrived(q_ref.at[pl.ds(rows + cuts[r], size[r]), :], kr.at[2 * SIDE, r], tp, sp)
        for d in range(SIDE):
            kv_wait(sp_at(d, 1), r)

    grid.near(0)
    w_own(1)
    grid.start(1)
    grid.far(0)
    grid.near(1)
    grid.last(0)
    w_near(0)
    grid.start(2)
    grid.far(1)
    grid.near(2)
    w_near(1)
    grid.last(1)
    grid.start(3)
    grid.far(2)
    w_far()
    w_mate()
    grid.final(0)
    project(0)
    grid.near(3)
    grid.final(1)
    project(1)
    grid.last(2)
    grid.far(3)
    kv_cross(0)
    grid.last(3)
    kv_cross(1)
    grid.final(2)
    project(2)
    grid.final(3)
    project(3)
    kv_ally(0)
    kv_ally(1)
    kv_cross(2)
    kv_cross(3)
    kv_ally(2)
    kv_ally(3)
    for r in range(CHUNKS):
        kv_mate(r)
    for d in range(1, 2 * SIDE):
        arrived(segall_ref.at[lax.rem(sp + d, 2 * SIDE)], sr.at[lax.rem(sp + d, 2 * SIDE)], tp, sp)
    segq_ref[0] = seg_ref[...]
    segq_ref[1] = segall_ref[cross]
    for r in range(CHUNKS):
        grid.drain(r)
    for copy in w_sends + seg_copies + kv_sends:
        copy.wait_send()


def qkv_exchange(x_block, wqkv_block, seg_block):
    rows, width = x_block.shape
    depth, cols = wqkv_block.shape
    sps, tps = 2 * SIDE, SIDE * SIDE
    seg_tile = seg_block.reshape(rows // HEAD_DIM, HEAD_DIM)
    vmem = pl.BlockSpec(memory_space=pltpu.VMEM)
    hbm = pl.BlockSpec(memory_space=pltpu.HBM)
    dma = pltpu.SemaphoreType.DMA
    return pl.pallas_call(
        qkv_kernel,
        out_shape=(
            jax.ShapeDtypeStruct((2 * rows, HEAD_DIM), jnp.bfloat16),
            jax.ShapeDtypeStruct((sps * rows, 2 * HEAD_DIM), jnp.bfloat16),
            jax.ShapeDtypeStruct((sps,) + seg_tile.shape, jnp.int32),
            jax.ShapeDtypeStruct((2,) + seg_tile.shape, jnp.int32),
        ),
        in_specs=[hbm, hbm, vmem],
        out_specs=(vmem,) * 4,
        scratch_shapes=[
            pltpu.VMEM((rows, tps * width), jnp.bfloat16),
            pltpu.VMEM((sps * depth, cols), jnp.bfloat16),
            pltpu.VMEM((2, rows, 3 * HEAD_DIM), jnp.bfloat16),
            dma((2,)),
            dma((CHUNKS, 2, 15)), dma((CHUNKS, 2, tps)),
            dma((14,)), dma((sps, 2)),
            dma((sps,)), dma((sps,)),
            dma((8 * CHUNKS,)), dma((sps + 1, CHUNKS)),
        ],
        compiler_params=pltpu.CompilerParams(collective_id=0, has_side_effects=True, vmem_limit_bytes=26 * 1024 * 1024),
        name="qkv_exchange",
    )(x_block, wqkv_block, seg_tile)


def output_kernel(ctx_ref, w_ref, y_ref, o_all, w_all, part, os, orr, ws, wr, ms, mr, ys, yr):
    tp, sp = lax.axis_index("tp"), lax.axis_index("sp")
    z, y = tp // SIDE, lax.rem(tp, SIDE)
    x, core = sp // 2, lax.rem(sp, 2)
    rows = ctx_ref.shape[0] // 2
    quarter = rows // SIDE
    depth, width = w_ref.shape
    group = x // 2
    cross = (SIDE - 1 - x) * 2 + core
    mate = x * 2 + 1 - core

    def x_at(d):
        return lax.rem(x + d, SIDE) * 2 + core

    def z_at(d):
        return lax.rem(z + d, SIDE)

    def y_at(d):
        return lax.rem(y + d, SIDE)

    peers = [(z_at(d) * SIDE + y, sp) for d in (1, 2, 3)]
    peers += [(z_at(d) * SIDE + y, cross) for d in range(SIDE)]
    peers += [(z * SIDE + y_at(d), sp) for d in (1, 2, 3)]
    peers += [(tp, x_at(1)), (tp, x_at(3)), (tp, mate)]
    barrier_with(peers)

    o_sends = []

    def o_slot(j, yo, b):
        return (z_at(j) * SIDE + yo) * 2 + (group if b == 0 else 1 - group)

    def o_col(slot):
        return o_all.at[:, pl.ds(pl.multiple_of(slot * HEAD_DIM, HEAD_DIM), HEAD_DIM)]

    def o_send(src, slot, to_tp, to_sp):
        copy = remote(src, o_col(slot), os.at[len(o_sends)], orr.at[slot], to_tp, to_sp)
        copy.start()
        o_sends.append(copy)

    def o_wait(slot):
        arrived(o_col(slot), orr.at[slot], tp, sp)

    def ctx_rows(j, b):
        return ctx_ref.at[pl.ds(pl.multiple_of(b * rows + z_at(j) * quarter, quarter), quarter), :]

    def o_along_y(j, b, src):
        slot = o_slot(j, y, b)
        for d in (1, 3):
            o_send(src, slot, z * SIDE + y_at(d), sp)

    mine = (z * SIDE + y) * 2 + group
    order = [(0, 1), (1, 0), (3, 0), (1, 1), (3, 1), (2, 0), (2, 1)]
    for j, b in order:
        o_send(ctx_rows(j, b), mine, z_at(j) * SIDE + y, sp if b == 0 else cross)
    o_along_y(0, 0, ctx_rows(0, 0))
    o_all[:, pl.ds(pl.multiple_of(mine * HEAD_DIM, HEAD_DIM), HEAD_DIM)] = ctx_ref[pl.ds(pl.multiple_of(z * quarter, quarter), quarter), :]

    steps = 1
    chunk = depth // steps
    half = width // 2
    m_sends = []

    def panel(r, h, u, v, c):
        return w_all.at[pl.ds(pl.multiple_of((u * 2 + c) * depth + r * chunk, chunk), chunk),
                        pl.ds(pl.multiple_of(v * width + h * half, half), half)]

    def own_panel(r, h):
        return w_ref.at[pl.ds(r * chunk, chunk), pl.ds(h * half, half)]

    def to_mate(r, h, u, v, src=None):
        held = panel(r, h, u, v, core)
        copy = remote(held if src is None else src, held, ms.at[len(m_sends)], mr.at[r, h, u * SIDE + v], tp, mate)
        copy.start()
        m_sends.append(copy)

    grid = Gather2D(
        (x, z), lambda u, v: (v * SIDE + y, u * 2 + core),
        own_panel, lambda r, h, u, v: panel(r, h, u, v, core), ws, wr, to_mate)
    w_all[pl.ds(pl.multiple_of(sp * depth, depth), depth), pl.ds(pl.multiple_of(z * width, width), width)] = w_ref[...]

    def o_near(j, b):
        for d in (3, 1):
            slot = o_slot(j, y_at(d), b)
            o_wait(slot)
            if d == (3 if (j + b) % 2 == 0 else 1):
                o_send(o_col(slot), slot, z * SIDE + y_at(4 - d), sp)

    def o_first(j, b):
        o_wait(o_slot(j, y, b))
        o_along_y(j, b, o_col(o_slot(j, y, b)))

    grid.start(0)
    for r in range(steps):
        for h in (0, 1):
            to_mate(r, h, x, z, own_panel(r, h))
    for j, b in order[0:3]:
        o_first(j, b)
    for j, b in ([(0, 0)] + order)[0:1]:
        o_near(j, b)
    grid.near(0)
    for j, b in order[3:7]:
        o_first(j, b)
    for j, b in ([(0, 0)] + order)[1:3]:
        o_near(j, b)
    grid.far(0)
    for j, b in ([(0, 0)] + order)[3:8]:
        o_near(j, b)
    grid.last(0)
    grid.final(0)
    for j, b in [(0, 0)] + order:
        o_wait(o_slot(j, y_at(2), b))
    for r in range(steps):
        for h in (0, 1):
            for d in range(SIDE * SIDE):
                u, v = lax.rem(x + d // SIDE, SIDE), z_at(d % SIDE)
                arrived(panel(r, h, u, v, 1 - core), mr.at[r, h, u * SIDE + v], tp, sp)

    y_sends = []
    strip = quarter // SIDE
    for zz in range(SIDE):
        out = jnp.dot(o_all[...], w_all[:, zz * width:(zz + 1) * width], preferred_element_type=jnp.float32)
        part[zz] = out.astype(jnp.bfloat16)
        cols = pl.ds(pl.multiple_of((zz * SIDE + y) * width, width), width)
        for d in (2, 1, 3):
            copy = remote(part.at[zz, pl.ds(pl.multiple_of(y_at(d) * strip, strip), strip), :], y_ref.at[:, cols],
                          ys.at[len(y_sends)], yr.at[zz, y], z * SIDE + y_at(d), sp)
            copy.start()
            y_sends.append(copy)
        y_ref[:, cols] = part[zz, pl.ds(pl.multiple_of(y * strip, strip), strip), :]
    for zz in range(SIDE):
        for d in (1, 3, 2):
            cols = pl.ds(pl.multiple_of((zz * SIDE + y_at(d)) * width, width), width)
            arrived(y_ref.at[:, cols], yr.at[zz, y_at(d)], tp, sp)
    for r in range(steps):
        grid.drain(r)
    for copy in o_sends + m_sends + y_sends:
        copy.wait_send()


def output_exchange(context, wout_block):
    rows = context.shape[0] // 2
    depth, width = wout_block.shape
    sps, tps = 2 * SIDE, SIDE * SIDE
    quarter = rows // SIDE
    vmem = pl.BlockSpec(memory_space=pltpu.VMEM)
    dma = pltpu.SemaphoreType.DMA
    return pl.pallas_call(
        output_kernel,
        out_shape=jax.ShapeDtypeStruct((quarter // SIDE, tps * width), jnp.bfloat16),
        in_specs=[vmem] * 2,
        out_specs=vmem,
        scratch_shapes=[
            pltpu.VMEM((quarter, tps * 2 * HEAD_DIM), jnp.bfloat16),
            pltpu.VMEM((sps * depth, SIDE * width), jnp.bfloat16),
            pltpu.VMEM((SIDE, quarter, width), jnp.bfloat16),
            dma((31,)), dma((2 * tps,)),
            dma((1, 2, 15)), dma((1, 2, tps)),
            dma((2 * tps,)), dma((1, 2, tps)),
            dma((3 * SIDE,)), dma((SIDE, SIDE)),
        ],
        compiler_params=pltpu.CompilerParams(collective_id=1, has_side_effects=True, vmem_limit_bytes=16 * 1024 * 1024),
        name="output_exchange",
    )(context, wout_block)


def solution(mesh):
    def device_block(x_block, doc_block, wqkv_block, wout_block):
        q, kv, seg_all, seg_q = qkv_exchange(x_block, wqkv_block, doc_block)
        context = attention(q, kv, seg_q.reshape(-1, HEAD_DIM), seg_all.reshape(-1, HEAD_DIM))
        return output_exchange(context, wout_block)

    return jax.shard_map(
        device_block,
        mesh=mesh,
        in_specs=(P(("dp", "sp"), "tp"), P(("dp", "sp")), P("sp", "tp"), P("sp", "tp")),
        out_specs=P(("dp", "sp", "tp"), None),
        check_vma=False,
    )
```

```python
import functools

import jax
import jax.numpy as jnp
from jax import lax
from jax.experimental import pallas as pl
from jax.experimental.pallas import tpu as pltpu
from jax.sharding import PartitionSpec as P

HEAD_DIM = 128
EXP2_SCALE = HEAD_DIM ** -0.5 * 1.4426950408889634
FLOOR = -3.0e38
SMALL = 2.0 ** -77
LARGE = 2.0 ** 15


def seg_column(segq_ref, base, rows):
    tiles = [jnp.broadcast_to(segq_ref[pl.ds(base + i, 1), :], (HEAD_DIM, HEAD_DIM)).T for i in range(rows // HEAD_DIM)]
    return jnp.concatenate(tiles, axis=0)


def attention_kernel(qb, kb, sub, q_ref, kv_ref, segq_ref, segall_ref, o_ref, q2_ref, acc_ref, m_ref, l_ref, kmax_ref, segc_ref):
    step_id = pl.program_id(0)
    keys = kv_ref.shape[0]
    qrow = step_id * (qb // HEAD_DIM)

    @pl.when(step_id == 0)
    def _():
        def norms(j, best):
            k = kv_ref[pl.ds(pl.multiple_of(j * 2048, 2048), 2048), :HEAD_DIM].astype(jnp.float32)
            total = jnp.dot((k * k).astype(jnp.bfloat16), jnp.ones((HEAD_DIM, HEAD_DIM), jnp.bfloat16), preferred_element_type=jnp.float32)
            return jnp.maximum(best, jnp.max(total.reshape(-1, 8, HEAD_DIM), axis=0))

        kmax_ref[...] = jnp.sqrt(lax.fori_loop(0, keys // 2048, norms, jnp.zeros(kmax_ref.shape, jnp.float32)))

    segq = segq_ref[pl.ds(qrow, qb // HEAD_DIM), :]
    lo = jnp.min(segq)
    hi = jnp.max(segq)
    seg_all = segall_ref[...]
    first = jnp.sum(jnp.where(seg_all < lo, 1.0, 0.0)).astype(jnp.int32)
    last = jnp.sum(jnp.where(seg_all <= hi, 1.0, 0.0)).astype(jnp.int32)
    one_doc = lo == hi
    whole_rows = first // HEAD_DIM * HEAD_DIM
    units = (last - whole_rows + 256 - 1) // 256
    base = jnp.minimum(whole_rows, keys - units * 256)
    count = units * 256 // kb
    rest = units - count * (kb // 256)

    q = q_ref[...]
    qf = q.astype(jnp.float32)
    bound = jnp.sqrt(jnp.sum(qf * qf, axis=1, keepdims=True)) * jnp.max(kmax_ref[...], axis=0, keepdims=True) * (-1.01 / HEAD_DIM)
    q2_ref[:, :HEAD_DIM] = q
    q2_ref[:, HEAD_DIM:] = bound.astype(jnp.bfloat16)
    acc_ref[...] = jnp.zeros_like(acc_ref)
    segc_ref[...] = seg_column(segq_ref, qrow, qb)

    def same_doc(start, size, rows):
        row = jnp.concatenate([segall_ref[pl.ds(start // HEAD_DIM + i, 1), :] for i in range(size // HEAD_DIM)], axis=1)
        return segc_ref[rows, :1] == row

    def pieces(start, size):
        rows = pl.ds(pl.multiple_of(start, HEAD_DIM), size)
        return kv_ref[rows, :HEAD_DIM], kv_ref[rows, HEAD_DIM:]

    def block(start, size, masked):
        k, v = pieces(start, size)
        ones = jnp.ones((size, HEAD_DIM), jnp.bfloat16)
        k2 = jnp.concatenate([k, ones], axis=1)
        v2 = jnp.concatenate([v, ones], axis=1)
        for i in range(qb // sub):
            rows = slice(i * sub, (i + 1) * sub)
            s = lax.dot_general(q2_ref[rows, :], k2, (((1,), (1,)), ((), ())), preferred_element_type=jnp.float32)
            p = jnp.exp2(s * EXP2_SCALE)
            if masked:
                p = jnp.where(same_doc(start, size, rows), p, 0.0)
            acc_ref[rows, :] += jnp.dot(p.astype(jnp.bfloat16), v2, preferred_element_type=jnp.float32)

    def online(start, size):
        k, v = pieces(start, size)
        for i in range(qb // sub):
            rows = slice(i * sub, (i + 1) * sub)
            s = lax.dot_general(q_ref[rows, :], k, (((1,), (1,)), ((), ())), preferred_element_type=jnp.float32)
            t = jnp.where(same_doc(start, size, rows), s * EXP2_SCALE, -jnp.inf)
            m_prev = m_ref[rows, :1]
            m_new = jnp.maximum(m_prev, jnp.max(t, axis=1, keepdims=True))
            p = jnp.exp2(t - m_new)
            alpha = jnp.exp2(m_prev - m_new)
            l_new = l_ref[rows, :1] * alpha + jnp.sum(p, axis=1, keepdims=True)
            pv = jnp.dot(p.astype(jnp.bfloat16), v, preferred_element_type=jnp.float32)
            acc_ref[rows, :HEAD_DIM] = acc_ref[rows, :HEAD_DIM] * alpha + pv
            m_ref[rows, :] = jnp.broadcast_to(m_new, (sub, HEAD_DIM))
            l_ref[rows, :] = jnp.broadcast_to(l_new, (sub, HEAD_DIM))

    def step(j, carry):
        whole = one_doc & (base + j * kb >= first) & (base + (j + 1) * kb <= last)

        @pl.when(whole)
        def _():
            block(base + j * kb, kb, False)

        @pl.when(jnp.logical_not(whole))
        def _():
            block(base + j * kb, kb, True)

        return carry

    lax.fori_loop(0, count, step, 0)

    size = kb // 2
    while size >= 256:
        @pl.when(rest // (size // 256) % 2 == 1)
        def _(size=size):
            block(base + count * kb + rest // (2 * size // 256) * (2 * size), size, True)

        size //= 2

    total = acc_ref[:, HEAD_DIM:]
    o_ref[...] = (acc_ref[:, :HEAD_DIM] / total).astype(o_ref.dtype)

    @pl.when(jnp.logical_not((jnp.min(total) >= SMALL) & (jnp.max(total) <= LARGE)))
    def _():
        acc_ref[...] = jnp.zeros_like(acc_ref)
        l_ref[...] = jnp.zeros_like(l_ref)
        m_ref[...] = jnp.full_like(m_ref, FLOOR)

        def again(j, carry):
            online(base + j * 256, 256)
            return carry

        lax.fori_loop(0, units, again, 0)
        o_ref[...] = (acc_ref[:, :HEAD_DIM] / l_ref[...]).astype(o_ref.dtype)


def attention(q, kv, seg_q, seg_all, qb=1024, kb=1024, sub=256):
    rows, keys = q.shape[0], kv.shape[0]
    whole = lambda a: pl.BlockSpec(a, lambda i: (0, 0))
    f32 = lambda *shape: pltpu.VMEM(shape, jnp.float32)
    return pl.pallas_call(
        functools.partial(attention_kernel, qb, kb, sub),
        grid=(rows // qb,),
        out_shape=jax.ShapeDtypeStruct(q.shape, jnp.bfloat16),
        in_specs=[
            pl.BlockSpec((qb, HEAD_DIM), lambda i: (i, 0)),
            whole(kv.shape), whole(seg_q.shape), whole(seg_all.shape),
        ],
        out_specs=pl.BlockSpec((qb, HEAD_DIM), lambda i: (i, 0)),
        scratch_shapes=[
            pltpu.VMEM((qb, 2 * HEAD_DIM), jnp.bfloat16),
            f32(qb, 2 * HEAD_DIM), f32(qb, HEAD_DIM), f32(qb, HEAD_DIM), f32(8, HEAD_DIM),
            pltpu.VMEM((qb, HEAD_DIM), jnp.int32),
        ],
        compiler_params=pltpu.CompilerParams(vmem_limit_bytes=24 * 1024 * 1024),
        name="attention",
    )(q, kv, seg_q, seg_all)

SIDE = 4
CUTS = (0, 8, 16, 24, 32)
CHUNKS = len(CUTS) - 1
MESH = pl.DeviceIdType.MESH


def remote(src, dst, send_sem, recv_sem, tp, sp):
    return pltpu.make_async_remote_copy(
        src_ref=src, dst_ref=dst, send_sem=send_sem, recv_sem=recv_sem,
        device_id={"tp": tp, "sp": sp}, device_id_type=MESH)


def arrived(ref, sem, tp, sp):
    remote(ref, ref, sem, sem, tp, sp).wait_recv()


def barrier_with(peers):
    barrier = pltpu.get_barrier_semaphore()
    for tp, sp in peers:
        pl.semaphore_signal(barrier, inc=1, device_id={"tp": tp, "sp": sp}, device_id_type=MESH)
    pl.semaphore_wait(barrier, len(peers))


class Gather2D:
    def __init__(self, coords, place, own, held, send_sem, recv_sem, on_arrival=None, first_done=False):
        self.coords, self.place, self.own, self.held = coords, place, own, held
        self.send_sem, self.recv_sem, self.on_arrival = send_sem, recv_sem, on_arrival
        self.first_done = first_done
        self.sent = {}

    def at(self, h, j1, j2):
        u, v = self.coords
        j1, j2 = (j1, j2) if h == 0 else (j2, j1)
        return lax.rem(u + j1, SIDE), lax.rem(v + j2, SIDE)

    def send(self, r, h, piece, to):
        src_at, dst_at = self.at(h, *piece), self.at(h, *to)
        local = piece == (0, 0) or (self.first_done and piece[1] == 0)
        src = self.own(r, h, *src_at) if local else self.held(r, h, *src_at)
        k = self.sent.get((r, h), 0)
        self.sent[r, h] = k + 1
        copy = remote(src, self.held(r, h, *src_at), self.send_sem.at[r, h, k],
                      self.recv_sem.at[r, h, src_at[0] * SIDE + src_at[1]], *self.place(*dst_at))
        copy.start()

    def wait(self, r, h, piece):
        src_at = self.at(h, *piece)
        arrived(self.held(r, h, *src_at), self.recv_sem.at[r, h, src_at[0] * SIDE + src_at[1]], *self.place(*self.coords))
        if self.on_arrival is not None:
            self.on_arrival(r, h, *src_at)

    def start(self, r):
        for h in (0, 1):
            for to in ((1, 0), (3, 0), (0, 1), (0, 3)):
                self.send(r, h, (0, 0), to)

    def spread(self, r, h, j1):
        for j2 in (1, 3):
            self.send(r, h, (j1, 0), (0, j2))

    def near(self, r):
        for j1 in (3, 1):
            for h in (0, 1):
                self.wait(r, h, (j1, 0))
                if j1 == (3 if (r + h) % 2 == 0 else 1):
                    self.send(r, h, (j1, 0), (4 - j1, 0))
                self.spread(r, h, j1)

    def pass_on(self, r, j1):
        for h in (0, 1):
            for j2 in (3, 1):
                self.wait(r, h, (j1, j2))
                if j2 == (3 if (r + h + (j1 + 1) // 2) % 2 == 0 else 1):
                    self.send(r, h, (j1, j2), (0, 4 - j2))

    def far(self, r):
        self.pass_on(r, 0)
        for h in (0, 1):
            self.wait(r, h, (2, 0))
            self.spread(r, h, 2)

    def last(self, r):
        for j1 in (3, 1, 2):
            self.pass_on(r, j1)

    def final(self, r):
        for j1 in (0, 3, 1, 2):
            for h in (0, 1):
                self.wait(r, h, (j1, 2))

    def drain(self, r):
        for h in (0, 1):
            for k in range(self.sent[r, h]):
                ref = self.held(r, h, *self.coords)
                remote(ref, ref, self.send_sem.at[r, h, k], self.recv_sem.at[r, h, 0], *self.place(*self.coords)).wait_send()


def qkv_kernel(x_ref, w_ref, wo_ref, seg_ref, q_ref, kv_ref, segall_ref, segq_ref, oa_ref, ob_ref,
               x_all, w_all, qkv, ls, xs, xr, ws, wr, ss, sr, ks, kr, rs, rr):
    tp, sp = lax.axis_index("tp"), lax.axis_index("sp")
    z, y = tp // SIDE, lax.rem(tp, SIDE)
    x, core = sp // 2, lax.rem(sp, 2)
    rows, width = x_ref.shape
    depth = w_ref.shape[0]
    cuts = [rows * c // CUTS[-1] for c in CUTS]
    size = [b - a for a, b in zip(cuts, cuts[1:])]
    half = width // 2

    def sp_at(dx, other=0):
        return lax.rem(x + dx, SIDE) * 2 + lax.rem(core + other, 2)

    mate = sp_at(0, 1)
    group = x // 2
    ally = (x + 1 - 2 * lax.rem(x, 2)) * 2 + core
    cross = (SIDE - 1 - x) * 2 + core

    peers = [(lax.rem(z + d, SIDE) * SIDE + y, sp) for d in (1, 3)]
    peers += [(z * SIDE + lax.rem(y + d, SIDE), sp) for d in (1, 3)]
    peers += [(tp, lax.rem(sp + d, 2 * SIDE)) for d in range(1, 2 * SIDE)]
    x_own = x_all.at[:, pl.ds(pl.multiple_of(tp * width, width), width)]
    w_own_rows = w_all.at[pl.ds(pl.multiple_of(sp * depth, depth), depth), :]
    loads = [pltpu.make_async_copy(x_ref, x_own, ls.at[0]), pltpu.make_async_copy(w_ref, w_own_rows, ls.at[1]),
             pltpu.make_async_copy(seg_ref, segq_ref.at[0], ls.at[2]),
             pltpu.make_async_copy(wo_ref.at[:, pl.ds(0, HEAD_DIM)], oa_ref.at[x], ls.at[3]),
             pltpu.make_async_copy(wo_ref.at[:, pl.ds(HEAD_DIM, HEAD_DIM)], ob_ref.at[z], ls.at[4])]
    for load in loads:
        load.start()
    barrier_with(peers)
    for load in loads:
        load.wait()

    grid = Gather2D(
        (z, y), lambda u, v: (u * SIDE + v, sp),
        lambda r, h, u, v: x_own.at[pl.ds(cuts[r], size[r]), pl.ds(h * half, half)],
        lambda r, h, u, v: x_all.at[pl.ds(cuts[r], size[r]), pl.ds(pl.multiple_of((u * SIDE + v) * width + h * half, half), half)],
        xs, xr)

    def w_at(owner, p):
        return w_all.at[pl.ds(pl.multiple_of(owner * depth + p * (depth // 2), depth // 2), depth // 2), :]

    w_sends = []

    def w_send(owner, p, to):
        k = len(w_sends)
        copy = remote(w_at(owner, p), w_at(owner, p), ws.at[k], wr.at[owner, p], tp, to)
        copy.start()
        w_sends.append(copy)

    def w_wait(owner, p):
        arrived(w_at(owner, p), wr.at[owner, p], tp, sp)

    def w_own(p):
        for to in (sp_at(1), sp_at(3), mate):
            w_send(sp, p, to)

    def w_near(p):
        for d in (3, 1):
            w_wait(sp_at(d), p)
            if d == (3 if p == 0 else 1):
                w_send(sp_at(d), p, sp_at(4 - d))
            w_send(sp_at(d), p, mate)

    def w_far():
        for p in (0, 1):
            w_wait(sp_at(2), p)
            w_send(sp_at(2), p, mate)

    def w_mate():
        for p in (0, 1):
            for d in (0, 1, 3, 2):
                w_wait(sp_at(d, 1), p)

    class Ring:
        def __init__(self, axis):
            self.axis, self.ref, self.me = axis, (oa_ref, ob_ref)[axis], (x, z)[axis]
            self.sends = []

        def at(self, d, p):
            return self.ref.at[lax.rem(self.me + d, SIDE), pl.ds(p * (depth // 2), depth // 2), :]

        def sem(self, d, p):
            return rr.at[self.axis, lax.rem(self.me + d, SIDE), p]

        def send(self, d, p, to):
            device = (tp, sp_at(to)) if self.axis == 0 else (lax.rem(z + to, SIDE) * SIDE + y, sp)
            copy = remote(self.at(d, p), self.at(d, p), rs.at[self.axis, len(self.sends)], self.sem(d, p), *device)
            copy.start()
            self.sends.append(copy)

        def own(self):
            for p in (0, 1):
                for to in (1, 3):
                    self.send(0, p, to)

        def near(self):
            for p in (0, 1):
                for d in (3, 1):
                    arrived(self.at(d, p), self.sem(d, p), tp, sp)
                    if d == (3 if p == 0 else 1):
                        self.send(d, p, 4 - d)

        def far(self):
            for p in (0, 1):
                arrived(self.at(2, p), self.sem(2, p), tp, sp)

    rings = Ring(0), Ring(1)

    grid.start(0)
    w_own(0)
    seg_copies = []
    for d in range(1, 2 * SIDE):
        copy = remote(segq_ref.at[0], segall_ref.at[sp], ss.at[d], sr.at[sp], tp, lax.rem(sp + d, 2 * SIDE))
        copy.start()
        seg_copies.append(copy)
    segall_ref[sp] = segq_ref[0]

    def kv_at(owner, r):
        return kv_ref.at[pl.ds(pl.multiple_of(owner * rows + cuts[r], 64), size[r]), :]

    kv_sends = []

    def kv_send(src, dst, recv, to):
        k = len(kv_sends)
        copy = remote(src, dst, ks.at[k], recv, tp, to)
        copy.start()
        kv_sends.append(copy)

    def project(r):
        here = slice(cuts[r], cuts[r + 1])
        for n in range(3):
            part = slice(n * 256, (n + 1) * 256)
            out = jnp.dot(x_all[here, :], w_all[:, part], preferred_element_type=jnp.float32).astype(jnp.bfloat16)
            for m in range(2):
                col = n * 2 + m
                qkv[col // 3, here, (col % 3) * HEAD_DIM:(col % 3 + 1) * HEAD_DIM] = out[:, m * HEAD_DIM:(m + 1) * HEAD_DIM]
        q_ref[here, :] = qkv[group, here, :HEAD_DIM]
        kv_ref[pl.ds(pl.multiple_of(sp * rows + cuts[r], 64), size[r]), :] = qkv[group, here, HEAD_DIM:]
        span = pl.ds(cuts[r], size[r])
        kv_send(qkv.at[1 - group, span, pl.ds(HEAD_DIM, 2 * HEAD_DIM)], kv_at(sp, r), kr.at[sp, r], cross)
        kv_send(qkv.at[1 - group, span, pl.ds(0, HEAD_DIM)], q_ref.at[pl.ds(rows + cuts[r], size[r]), :], kr.at[2 * SIDE, r], cross)
        kv_send(qkv.at[group, span, pl.ds(HEAD_DIM, 2 * HEAD_DIM)], kv_at(sp, r), kr.at[sp, r], ally)
        kv_send(qkv.at[group, span, pl.ds(HEAD_DIM, 2 * HEAD_DIM)], kv_at(sp, r), kr.at[sp, r], mate)

    ally_cross = lax.rem(x + 2, SIDE) * 2 + core

    def kv_wait(owner, r):
        arrived(kv_at(owner, r), kr.at[owner, r], tp, sp)

    def kv_cross(r):
        kv_wait(cross, r)
        kv_send(kv_at(cross, r), kv_at(cross, r), kr.at[cross, r], ally)
        kv_send(kv_at(cross, r), kv_at(cross, r), kr.at[cross, r], mate)

    def kv_ally(r):
        for owner in (ally, ally_cross):
            kv_wait(owner, r)
            kv_send(kv_at(owner, r), kv_at(owner, r), kr.at[owner, r], mate)

    def kv_mate(r):
        arrived(q_ref.at[pl.ds(rows + cuts[r], size[r]), :], kr.at[2 * SIDE, r], tp, sp)
        for d in range(SIDE):
            kv_wait(sp_at(d, 1), r)

    grid.near(0)
    w_own(1)
    grid.start(1)
    grid.far(0)
    grid.near(1)
    grid.last(0)
    w_near(0)
    grid.start(2)
    grid.far(1)
    grid.near(2)
    w_near(1)
    rings[0].own()
    grid.last(1)
    grid.start(3)
    rings[1].own()
    grid.far(2)
    w_far()
    w_mate()
    grid.final(0)
    project(0)
    grid.near(3)
    grid.final(1)
    project(1)
    rings[0].near()
    grid.last(2)
    grid.far(3)
    kv_cross(0)
    rings[1].near()
    grid.last(3)
    kv_cross(1)
    grid.final(2)
    project(2)
    grid.final(3)
    project(3)
    kv_ally(0)
    kv_ally(1)
    kv_cross(2)
    kv_cross(3)
    kv_ally(2)
    kv_ally(3)
    rings[0].far()
    rings[1].far()
    for r in range(CHUNKS):
        kv_mate(r)
    for d in range(1, 2 * SIDE):
        arrived(segall_ref.at[lax.rem(sp + d, 2 * SIDE)], sr.at[lax.rem(sp + d, 2 * SIDE)], tp, sp)
    segq_ref[1] = segall_ref[cross]
    for r in range(CHUNKS):
        grid.drain(r)
    for copy in w_sends + seg_copies + kv_sends + rings[0].sends + rings[1].sends:
        copy.wait_send()


def qkv_exchange(x_block, wqkv_block, wout_block, seg_block):
    rows, width = x_block.shape
    depth, cols = wqkv_block.shape
    sps, tps = 2 * SIDE, SIDE * SIDE
    seg_tile = seg_block.reshape(rows // HEAD_DIM, HEAD_DIM)
    vmem = pl.BlockSpec(memory_space=pltpu.VMEM)
    hbm = pl.BlockSpec(memory_space=pltpu.HBM)
    dma = pltpu.SemaphoreType.DMA
    return pl.pallas_call(
        qkv_kernel,
        out_shape=(
            jax.ShapeDtypeStruct((2 * rows, HEAD_DIM), jnp.bfloat16),
            jax.ShapeDtypeStruct((sps * rows, 2 * HEAD_DIM), jnp.bfloat16),
            jax.ShapeDtypeStruct((sps,) + seg_tile.shape, jnp.int32),
            jax.ShapeDtypeStruct((2,) + seg_tile.shape, jnp.int32),
            jax.ShapeDtypeStruct((SIDE, depth, HEAD_DIM), jnp.bfloat16),
            jax.ShapeDtypeStruct((SIDE, depth, HEAD_DIM), jnp.bfloat16),
        ),
        in_specs=[hbm] * 4,
        out_specs=(vmem,) * 6,
        scratch_shapes=[
            pltpu.VMEM((rows, tps * width), jnp.bfloat16),
            pltpu.VMEM((sps * depth, cols), jnp.bfloat16),
            pltpu.VMEM((2, rows, 3 * HEAD_DIM), jnp.bfloat16),
            dma((5,)),
            dma((CHUNKS, 2, 15)), dma((CHUNKS, 2, tps)),
            dma((14,)), dma((sps, 2)),
            dma((sps,)), dma((sps,)),
            dma((8 * CHUNKS,)), dma((sps + 1, CHUNKS)),
            dma((2, 6)), dma((2, SIDE, 2)),
        ],
        compiler_params=pltpu.CompilerParams(collective_id=0, has_side_effects=True, vmem_limit_bytes=26 * 1024 * 1024),
        name="qkv_exchange",
    )(*(pltpu.with_memory_space_constraint(a, pltpu.HBM) for a in (x_block, wqkv_block, wout_block, seg_tile)))


def output_kernel(ctx_ref, oa_ref, ob_ref, y_ref, o_all, w_all, part, os, orr, ws, wr, ms, mr, ys, yr):
    tp, sp = lax.axis_index("tp"), lax.axis_index("sp")
    z, y = tp // SIDE, lax.rem(tp, SIDE)
    x, core = sp // 2, lax.rem(sp, 2)
    rows = ctx_ref.shape[0] // 2
    quarter = rows // SIDE
    depth, width = oa_ref.shape[1], 2 * oa_ref.shape[2]
    group = x // 2
    cross = (SIDE - 1 - x) * 2 + core
    mate = x * 2 + 1 - core

    def x_at(d):
        return lax.rem(x + d, SIDE) * 2 + core

    def z_at(d):
        return lax.rem(z + d, SIDE)

    def y_at(d):
        return lax.rem(y + d, SIDE)

    peers = [(z_at(d) * SIDE + y, sp) for d in (1, 2, 3)]
    peers += [(z_at(d) * SIDE + y, cross) for d in range(SIDE)]
    peers += [(z * SIDE + y_at(d), sp) for d in (1, 2, 3)]
    peers += [(tp, x_at(1)), (tp, x_at(3)), (tp, mate)]
    barrier_with(peers)

    o_sends = []

    def o_slot(j, yo, b):
        return (z_at(j) * SIDE + yo) * 2 + (group if b == 0 else 1 - group)

    def o_col(slot):
        return o_all.at[:, pl.ds(pl.multiple_of(slot * HEAD_DIM, HEAD_DIM), HEAD_DIM)]

    def o_send(src, slot, to_tp, to_sp):
        copy = remote(src, o_col(slot), os.at[len(o_sends)], orr.at[slot], to_tp, to_sp)
        copy.start()
        o_sends.append(copy)

    def o_wait(slot):
        arrived(o_col(slot), orr.at[slot], tp, sp)

    def ctx_rows(j, b):
        return ctx_ref.at[pl.ds(pl.multiple_of(b * rows + z_at(j) * quarter, quarter), quarter), :]

    def o_along_y(j, b, src):
        slot = o_slot(j, y, b)
        for d in (1, 3):
            o_send(src, slot, z * SIDE + y_at(d), sp)

    mine = (z * SIDE + y) * 2 + group
    order = [(0, 1), (1, 0), (3, 0), (1, 1), (3, 1), (2, 0), (2, 1)]
    for j, b in order:
        o_send(ctx_rows(j, b), mine, z_at(j) * SIDE + y, sp if b == 0 else cross)
    o_along_y(0, 0, ctx_rows(0, 0))
    o_all[:, pl.ds(pl.multiple_of(mine * HEAD_DIM, HEAD_DIM), HEAD_DIM)] = ctx_ref[pl.ds(pl.multiple_of(z * quarter, quarter), quarter), :]

    half = width // 2
    m_sends = []

    def panel(r, h, u, v, c):
        return w_all.at[pl.ds(pl.multiple_of((u * 2 + c) * depth, depth), depth),
                        pl.ds(pl.multiple_of(v * width + h * half, half), half)]

    def held_already(r, h, u, v):
        return oa_ref.at[u] if h == 0 else ob_ref.at[v]

    def to_mate(r, h, u, v, src=None):
        held = panel(r, h, u, v, core)
        copy = remote(held if src is None else src, held, ms.at[len(m_sends)], mr.at[r, h, u * SIDE + v], tp, mate)
        copy.start()
        m_sends.append(copy)

    grid = Gather2D(
        (x, z), lambda u, v: (v * SIDE + y, u * 2 + core),
        held_already, lambda r, h, u, v: panel(r, h, u, v, core), ws, wr, to_mate, first_done=True)

    def o_near(j, b):
        for d in (3, 1):
            slot = o_slot(j, y_at(d), b)
            o_wait(slot)
            if d == (3 if (j + b) % 2 == 0 else 1):
                o_send(o_col(slot), slot, z * SIDE + y_at(4 - d), sp)

    def o_first(j, b):
        o_wait(o_slot(j, y, b))
        o_along_y(j, b, o_col(o_slot(j, y, b)))

    for j1 in range(SIDE):
        for h in (0, 1):
            grid.spread(0, h, j1)
    for j1 in range(SIDE):
        for h in (0, 1):
            u, v = grid.at(h, j1, 0)
            to_mate(0, h, u, v, held_already(0, h, u, v))
            rows_at = pl.ds(pl.multiple_of((u * 2 + core) * depth, depth), depth)
            w_all[rows_at, pl.ds(pl.multiple_of(v * width + h * half, half), half)] = oa_ref[u] if h == 0 else ob_ref[v]
    for j, b in order[0:3]:
        o_first(j, b)
    for j, b in ([(0, 0)] + order)[0:1]:
        o_near(j, b)
    grid.pass_on(0, 0)
    for j, b in order[3:7]:
        o_first(j, b)
    for j, b in ([(0, 0)] + order)[1:3]:
        o_near(j, b)
    grid.pass_on(0, 1)
    for j, b in ([(0, 0)] + order)[3:5]:
        o_near(j, b)
    grid.pass_on(0, 2)
    for j, b in ([(0, 0)] + order)[5:8]:
        o_near(j, b)
    grid.pass_on(0, 3)
    grid.final(0)
    for j, b in [(0, 0)] + order:
        o_wait(o_slot(j, y_at(2), b))
    for h in (0, 1):
        for d in range(SIDE * SIDE):
            u, v = lax.rem(x + d // SIDE, SIDE), z_at(d % SIDE)
            arrived(panel(0, h, u, v, 1 - core), mr.at[0, h, u * SIDE + v], tp, sp)

    y_sends = []
    strip = quarter // SIDE
    for zz in range(SIDE):
        out = jnp.dot(o_all[...], w_all[:, zz * width:(zz + 1) * width], preferred_element_type=jnp.float32)
        part[zz] = out.astype(jnp.bfloat16)
        cols = pl.ds(pl.multiple_of((zz * SIDE + y) * width, width), width)
        for d in (2, 1, 3):
            copy = remote(part.at[zz, pl.ds(pl.multiple_of(y_at(d) * strip, strip), strip), :], y_ref.at[:, cols],
                          ys.at[len(y_sends)], yr.at[zz, y], z * SIDE + y_at(d), sp)
            copy.start()
            y_sends.append(copy)
        y_ref[:, cols] = part[zz, pl.ds(pl.multiple_of(y * strip, strip), strip), :]
    for zz in range(SIDE):
        for d in (1, 3, 2):
            cols = pl.ds(pl.multiple_of((zz * SIDE + y_at(d)) * width, width), width)
            arrived(y_ref.at[:, cols], yr.at[zz, y_at(d)], tp, sp)
    grid.drain(0)
    for copy in o_sends + m_sends + y_sends:
        copy.wait_send()


def output_exchange(context, oa, ob):
    rows = context.shape[0] // 2
    depth, width = oa.shape[1], 2 * oa.shape[2]
    sps, tps = 2 * SIDE, SIDE * SIDE
    quarter = rows // SIDE
    vmem = pl.BlockSpec(memory_space=pltpu.VMEM)
    dma = pltpu.SemaphoreType.DMA
    return pl.pallas_call(
        output_kernel,
        out_shape=jax.ShapeDtypeStruct((quarter // SIDE, tps * width), jnp.bfloat16),
        in_specs=[vmem] * 3,
        out_specs=vmem,
        scratch_shapes=[
            pltpu.VMEM((quarter, tps * 2 * HEAD_DIM), jnp.bfloat16),
            pltpu.VMEM((sps * depth, SIDE * width), jnp.bfloat16),
            pltpu.VMEM((SIDE, quarter, width), jnp.bfloat16),
            dma((31,)), dma((2 * tps,)),
            dma((1, 2, 15)), dma((1, 2, tps)),
            dma((2 * tps,)), dma((1, 2, tps)),
            dma((3 * SIDE,)), dma((SIDE, SIDE)),
        ],
        compiler_params=pltpu.CompilerParams(collective_id=1, has_side_effects=True, vmem_limit_bytes=16 * 1024 * 1024),
        name="output_exchange",
    )(context, oa, ob)


def solution(mesh):
    def device_block(x_block, doc_block, wqkv_block, wout_block):
        q, kv, seg_all, seg_q, oa, ob = qkv_exchange(x_block, wqkv_block, wout_block, doc_block)
        context = attention(q, kv, seg_q.reshape(-1, HEAD_DIM), seg_all.reshape(-1, HEAD_DIM))
        return output_exchange(context, oa, ob)

    return jax.shard_map(
        device_block,
        mesh=mesh,
        in_specs=(P(("dp", "sp"), "tp"), P(("dp", "sp")), P("sp", "tp"), P("sp", "tp")),
        out_specs=P(("dp", "sp", "tp"), None),
        check_vma=False,
    )
```

```python
import functools

import jax
import jax.numpy as jnp
from jax import lax
from jax.experimental import pallas as pl
from jax.experimental.pallas import tpu as pltpu
from jax.sharding import PartitionSpec as P

HEAD_DIM = 128
EXP2_SCALE = HEAD_DIM ** -0.5 * 1.4426950408889634
FLOOR = -3.0e38
SMALL = 2.0 ** -77
LARGE = 2.0 ** 15


def seg_column(segq_ref, base, rows):
    tiles = [jnp.broadcast_to(segq_ref[pl.ds(base + i, 1), :], (HEAD_DIM, HEAD_DIM)).T for i in range(rows // HEAD_DIM)]
    return jnp.concatenate(tiles, axis=0)


def attention_kernel(qb, kb, sub, q_ref, kv_ref, segq_ref, segall_ref, o_ref, q2_ref, acc_ref, m_ref, l_ref, kmax_ref, segc_ref):
    step_id = pl.program_id(0)
    keys = kv_ref.shape[0]
    qrow = step_id * (qb // HEAD_DIM)

    @pl.when(step_id == 0)
    def _():
        def norms(j, best):
            k = kv_ref[pl.ds(pl.multiple_of(j * 2048, 2048), 2048), :HEAD_DIM].astype(jnp.float32)
            total = jnp.dot((k * k).astype(jnp.bfloat16), jnp.ones((HEAD_DIM, HEAD_DIM), jnp.bfloat16), preferred_element_type=jnp.float32)
            return jnp.maximum(best, jnp.max(total.reshape(-1, 8, HEAD_DIM), axis=0))

        kmax_ref[...] = jnp.sqrt(lax.fori_loop(0, keys // 2048, norms, jnp.zeros(kmax_ref.shape, jnp.float32)))

    segq = segq_ref[pl.ds(qrow, qb // HEAD_DIM), :]
    lo = jnp.min(segq)
    hi = jnp.max(segq)
    seg_all = segall_ref[...]
    first = jnp.sum(jnp.where(seg_all < lo, 1.0, 0.0)).astype(jnp.int32)
    last = jnp.sum(jnp.where(seg_all <= hi, 1.0, 0.0)).astype(jnp.int32)
    one_doc = lo == hi
    whole_rows = first // HEAD_DIM * HEAD_DIM
    units = (last - whole_rows + 256 - 1) // 256
    base = jnp.minimum(whole_rows, keys - units * 256)
    count = units * 256 // kb
    rest = units - count * (kb // 256)

    q = q_ref[...]
    qf = q.astype(jnp.float32)
    bound = jnp.sqrt(jnp.sum(qf * qf, axis=1, keepdims=True)) * jnp.max(kmax_ref[...], axis=0, keepdims=True) * (-1.01 / HEAD_DIM)
    q2_ref[:, :HEAD_DIM] = q
    q2_ref[:, HEAD_DIM:] = bound.astype(jnp.bfloat16)
    acc_ref[...] = jnp.zeros_like(acc_ref)
    segc_ref[...] = seg_column(segq_ref, qrow, qb)

    def same_doc(start, size, rows):
        row = jnp.concatenate([segall_ref[pl.ds(start // HEAD_DIM + i, 1), :] for i in range(size // HEAD_DIM)], axis=1)
        return segc_ref[rows, :1] == row

    def pieces(start, size):
        rows = pl.ds(pl.multiple_of(start, HEAD_DIM), size)
        return kv_ref[rows, :HEAD_DIM], kv_ref[rows, HEAD_DIM:]

    def block(start, size, masked):
        k, v = pieces(start, size)
        ones = jnp.ones((size, HEAD_DIM), jnp.bfloat16)
        k2 = jnp.concatenate([k, ones], axis=1)
        v2 = jnp.concatenate([v, ones], axis=1)
        for i in range(qb // sub):
            rows = slice(i * sub, (i + 1) * sub)
            s = lax.dot_general(q2_ref[rows, :], k2, (((1,), (1,)), ((), ())), preferred_element_type=jnp.float32)
            p = jnp.exp2(s * EXP2_SCALE)
            if masked:
                p = jnp.where(same_doc(start, size, rows), p, 0.0)
            acc_ref[rows, :] += jnp.dot(p.astype(jnp.bfloat16), v2, preferred_element_type=jnp.float32)

    def online(start, size):
        k, v = pieces(start, size)
        for i in range(qb // sub):
            rows = slice(i * sub, (i + 1) * sub)
            s = lax.dot_general(q_ref[rows, :], k, (((1,), (1,)), ((), ())), preferred_element_type=jnp.float32)
            t = jnp.where(same_doc(start, size, rows), s * EXP2_SCALE, -jnp.inf)
            m_prev = m_ref[rows, :1]
            m_new = jnp.maximum(m_prev, jnp.max(t, axis=1, keepdims=True))
            p = jnp.exp2(t - m_new)
            alpha = jnp.exp2(m_prev - m_new)
            l_new = l_ref[rows, :1] * alpha + jnp.sum(p, axis=1, keepdims=True)
            pv = jnp.dot(p.astype(jnp.bfloat16), v, preferred_element_type=jnp.float32)
            acc_ref[rows, :HEAD_DIM] = acc_ref[rows, :HEAD_DIM] * alpha + pv
            m_ref[rows, :] = jnp.broadcast_to(m_new, (sub, HEAD_DIM))
            l_ref[rows, :] = jnp.broadcast_to(l_new, (sub, HEAD_DIM))

    def step(j, carry):
        whole = one_doc & (base + j * kb >= first) & (base + (j + 1) * kb <= last)

        @pl.when(whole)
        def _():
            block(base + j * kb, kb, False)

        @pl.when(jnp.logical_not(whole))
        def _():
            block(base + j * kb, kb, True)

        return carry

    lax.fori_loop(0, count, step, 0)

    size = kb // 2
    while size >= 256:
        @pl.when(rest // (size // 256) % 2 == 1)
        def _(size=size):
            block(base + count * kb + rest // (2 * size // 256) * (2 * size), size, True)

        size //= 2

    total = acc_ref[:, HEAD_DIM:]
    o_ref[...] = (acc_ref[:, :HEAD_DIM] / total).astype(o_ref.dtype)

    @pl.when(jnp.logical_not((jnp.min(total) >= SMALL) & (jnp.max(total) <= LARGE)))
    def _():
        acc_ref[...] = jnp.zeros_like(acc_ref)
        l_ref[...] = jnp.zeros_like(l_ref)
        m_ref[...] = jnp.full_like(m_ref, FLOOR)

        def again(j, carry):
            online(base + j * 256, 256)
            return carry

        lax.fori_loop(0, units, again, 0)
        o_ref[...] = (acc_ref[:, :HEAD_DIM] / l_ref[...]).astype(o_ref.dtype)


def attention(q, kv, seg_q, seg_all, qb=1024, kb=1024, sub=256):
    rows, keys = q.shape[0], kv.shape[0]
    whole = lambda a: pl.BlockSpec(a, lambda i: (0, 0))
    f32 = lambda *shape: pltpu.VMEM(shape, jnp.float32)
    return pl.pallas_call(
        functools.partial(attention_kernel, qb, kb, sub),
        grid=(rows // qb,),
        out_shape=jax.ShapeDtypeStruct(q.shape, jnp.bfloat16),
        in_specs=[
            pl.BlockSpec((qb, HEAD_DIM), lambda i: (i, 0)),
            whole(kv.shape), whole(seg_q.shape), whole(seg_all.shape),
        ],
        out_specs=pl.BlockSpec((qb, HEAD_DIM), lambda i: (i, 0)),
        scratch_shapes=[
            pltpu.VMEM((qb, 2 * HEAD_DIM), jnp.bfloat16),
            f32(qb, 2 * HEAD_DIM), f32(qb, HEAD_DIM), f32(qb, HEAD_DIM), f32(8, HEAD_DIM),
            pltpu.VMEM((qb, HEAD_DIM), jnp.int32),
        ],
        compiler_params=pltpu.CompilerParams(vmem_limit_bytes=24 * 1024 * 1024),
        name="attention",
    )(q, kv, seg_q, seg_all)

SIDE = 4
CUTS = (0, 8, 16, 24, 32)
CHUNKS = len(CUTS) - 1
MESH = pl.DeviceIdType.MESH


def remote(src, dst, send_sem, recv_sem, tp, sp):
    return pltpu.make_async_remote_copy(
        src_ref=src, dst_ref=dst, send_sem=send_sem, recv_sem=recv_sem,
        device_id={"tp": tp, "sp": sp}, device_id_type=MESH)


def arrived(ref, sem, tp, sp):
    remote(ref, ref, sem, sem, tp, sp).wait_recv()


def barrier_with(peers):
    barrier = pltpu.get_barrier_semaphore()
    for tp, sp in peers:
        pl.semaphore_signal(barrier, inc=1, device_id={"tp": tp, "sp": sp}, device_id_type=MESH)
    pl.semaphore_wait(barrier, len(peers))


class Gather2D:
    def __init__(self, coords, place, own, held, send_sem, recv_sem, on_arrival=None, first_done=False):
        self.coords, self.place, self.own, self.held = coords, place, own, held
        self.send_sem, self.recv_sem, self.on_arrival = send_sem, recv_sem, on_arrival
        self.first_done = first_done
        self.sent = {}

    def at(self, h, j1, j2):
        u, v = self.coords
        j1, j2 = (j1, j2) if h == 0 else (j2, j1)
        return lax.rem(u + j1, SIDE), lax.rem(v + j2, SIDE)

    def send(self, r, h, piece, to):
        src_at, dst_at = self.at(h, *piece), self.at(h, *to)
        local = piece == (0, 0) or (self.first_done and piece[1] == 0)
        src = self.own(r, h, *src_at) if local else self.held(r, h, *src_at)
        k = self.sent.get((r, h), 0)
        self.sent[r, h] = k + 1
        copy = remote(src, self.held(r, h, *src_at), self.send_sem.at[r, h, k],
                      self.recv_sem.at[r, h, src_at[0] * SIDE + src_at[1]], *self.place(*dst_at))
        copy.start()

    def wait(self, r, h, piece):
        src_at = self.at(h, *piece)
        arrived(self.held(r, h, *src_at), self.recv_sem.at[r, h, src_at[0] * SIDE + src_at[1]], *self.place(*self.coords))
        if self.on_arrival is not None:
            self.on_arrival(r, h, *src_at)

    def start(self, r):
        for to in ((1, 0), (3, 0), (0, 1), (0, 3)):
            for h in (0, 1):
                self.send(r, h, (0, 0), to)

    def spread(self, r, h, j1):
        for j2 in (1, 3):
            self.send(r, h, (j1, 0), (0, j2))

    def near(self, r):
        for j1 in (3, 1):
            for h in (0, 1):
                self.wait(r, h, (j1, 0))
                if j1 == (3 if (r + h) % 2 == 0 else 1):
                    self.send(r, h, (j1, 0), (4 - j1, 0))
                self.spread(r, h, j1)

    def pass_on(self, r, j1):
        for h in (0, 1):
            for j2 in (3, 1):
                self.wait(r, h, (j1, j2))
                if j2 == (3 if (r + h + (j1 + 1) // 2) % 2 == 0 else 1):
                    self.send(r, h, (j1, j2), (0, 4 - j2))

    def far(self, r):
        self.pass_on(r, 0)
        for h in (0, 1):
            self.wait(r, h, (2, 0))
            self.spread(r, h, 2)

    def last(self, r):
        for j1 in (3, 1, 2):
            self.pass_on(r, j1)

    def final(self, r):
        for j1 in (0, 3, 1, 2):
            for h in (0, 1):
                self.wait(r, h, (j1, 2))

    def drain(self, r):
        for h in (0, 1):
            for k in range(self.sent[r, h]):
                ref = self.held(r, h, *self.coords)
                remote(ref, ref, self.send_sem.at[r, h, k], self.recv_sem.at[r, h, 0], *self.place(*self.coords)).wait_send()


def qkv_kernel(x_ref, w_ref, wo_ref, seg_ref, q_ref, kv_ref, segall_ref, segq_ref, oa_ref, ob_ref,
               x_all, w_all, qkv, ls, xs, xr, ws, wr, ss, sr, ks, kr, rs, rr):
    tp, sp = lax.axis_index("tp"), lax.axis_index("sp")
    z, y = tp // SIDE, lax.rem(tp, SIDE)
    x, core = sp // 2, lax.rem(sp, 2)
    rows, width = x_ref.shape
    depth = w_ref.shape[0]
    cuts = [rows * c // CUTS[-1] for c in CUTS]
    size = [b - a for a, b in zip(cuts, cuts[1:])]
    half = width // 2

    def sp_at(dx, other=0):
        return lax.rem(x + dx, SIDE) * 2 + lax.rem(core + other, 2)

    mate = sp_at(0, 1)
    group = x // 2
    ally = (x + 1 - 2 * lax.rem(x, 2)) * 2 + core
    cross = (SIDE - 1 - x) * 2 + core

    peers = [(lax.rem(z + d, SIDE) * SIDE + y, sp) for d in (1, 3)]
    peers += [(z * SIDE + lax.rem(y + d, SIDE), sp) for d in (1, 3)]
    peers += [(tp, lax.rem(sp + d, 2 * SIDE)) for d in range(1, 2 * SIDE)]
    x_own = x_all.at[:, pl.ds(pl.multiple_of(tp * width, width), width)]
    w_own_rows = w_all.at[pl.ds(pl.multiple_of(sp * depth, depth), depth), :]
    loads = [pltpu.make_async_copy(x_ref, x_own, ls.at[0]), pltpu.make_async_copy(w_ref, w_own_rows, ls.at[1]),
             pltpu.make_async_copy(seg_ref, segq_ref.at[0], ls.at[2]),
             pltpu.make_async_copy(wo_ref.at[:, pl.ds(0, HEAD_DIM)], oa_ref.at[x], ls.at[3]),
             pltpu.make_async_copy(wo_ref.at[:, pl.ds(HEAD_DIM, HEAD_DIM)], ob_ref.at[z], ls.at[4])]
    for load in loads:
        load.start()
    barrier_with(peers)
    for load in loads:
        load.wait()

    grid = Gather2D(
        (z, y), lambda u, v: (u * SIDE + v, sp),
        lambda r, h, u, v: x_own.at[pl.ds(cuts[r], size[r]), pl.ds(h * half, half)],
        lambda r, h, u, v: x_all.at[pl.ds(cuts[r], size[r]), pl.ds(pl.multiple_of((u * SIDE + v) * width + h * half, half), half)],
        xs, xr)

    def w_at(owner, p):
        return w_all.at[pl.ds(pl.multiple_of(owner * depth + p * (depth // 2), depth // 2), depth // 2), :]

    w_sends = []

    def w_send(owner, p, to):
        k = len(w_sends)
        copy = remote(w_at(owner, p), w_at(owner, p), ws.at[k], wr.at[owner, p], tp, to)
        copy.start()
        w_sends.append(copy)

    def w_wait(owner, p):
        arrived(w_at(owner, p), wr.at[owner, p], tp, sp)

    def w_own(p):
        for to in (sp_at(1), sp_at(3), mate):
            w_send(sp, p, to)

    def w_near(p):
        for d in (3, 1):
            w_wait(sp_at(d), p)
            if d == (3 if p == 0 else 1):
                w_send(sp_at(d), p, sp_at(4 - d))
            w_send(sp_at(d), p, mate)

    def w_far():
        for p in (0, 1):
            w_wait(sp_at(2), p)
            w_send(sp_at(2), p, mate)

    def w_mate():
        for p in (0, 1):
            for d in (0, 1, 3, 2):
                w_wait(sp_at(d, 1), p)

    class Ring:
        def __init__(self, axis):
            self.axis, self.ref, self.me = axis, (oa_ref, ob_ref)[axis], (x, z)[axis]
            self.sends = []

        def at(self, d, p):
            return self.ref.at[lax.rem(self.me + d, SIDE), pl.ds(p * (depth // 2), depth // 2), :]

        def sem(self, d, p):
            return rr.at[self.axis, lax.rem(self.me + d, SIDE), p]

        def send(self, d, p, to):
            device = (tp, sp_at(to)) if self.axis == 0 else (lax.rem(z + to, SIDE) * SIDE + y, sp)
            copy = remote(self.at(d, p), self.at(d, p), rs.at[self.axis, len(self.sends)], self.sem(d, p), *device)
            copy.start()
            self.sends.append(copy)

        def own(self):
            for p in (0, 1):
                for to in (1, 3):
                    self.send(0, p, to)

        def near(self):
            for p in (0, 1):
                for d in (3, 1):
                    arrived(self.at(d, p), self.sem(d, p), tp, sp)
                    if d == (3 if p == 0 else 1):
                        self.send(d, p, 4 - d)

        def far(self):
            for p in (0, 1):
                arrived(self.at(2, p), self.sem(2, p), tp, sp)

    rings = Ring(0), Ring(1)

    grid.start(0)
    w_own(0)
    seg_copies = []
    for d in range(1, 2 * SIDE):
        copy = remote(segq_ref.at[0], segall_ref.at[sp], ss.at[d], sr.at[sp], tp, lax.rem(sp + d, 2 * SIDE))
        copy.start()
        seg_copies.append(copy)
    segall_ref[sp] = segq_ref[0]

    def kv_at(owner, r):
        return kv_ref.at[pl.ds(pl.multiple_of(owner * rows + cuts[r], 64), size[r]), :]

    kv_sends = []

    def kv_send(src, dst, recv, to):
        k = len(kv_sends)
        copy = remote(src, dst, ks.at[k], recv, tp, to)
        copy.start()
        kv_sends.append(copy)

    def project(r):
        here = slice(cuts[r], cuts[r + 1])
        for n in range(3):
            part = slice(n * 256, (n + 1) * 256)
            out = jnp.dot(x_all[here, :], w_all[:, part], preferred_element_type=jnp.float32).astype(jnp.bfloat16)
            for m in range(2):
                col = n * 2 + m
                qkv[col // 3, here, (col % 3) * HEAD_DIM:(col % 3 + 1) * HEAD_DIM] = out[:, m * HEAD_DIM:(m + 1) * HEAD_DIM]
        q_ref[here, :] = qkv[group, here, :HEAD_DIM]
        kv_ref[pl.ds(pl.multiple_of(sp * rows + cuts[r], 64), size[r]), :] = qkv[group, here, HEAD_DIM:]
        span = pl.ds(cuts[r], size[r])
        kv_send(qkv.at[1 - group, span, pl.ds(HEAD_DIM, 2 * HEAD_DIM)], kv_at(sp, r), kr.at[sp, r], cross)
        kv_send(qkv.at[1 - group, span, pl.ds(0, HEAD_DIM)], q_ref.at[pl.ds(rows + cuts[r], size[r]), :], kr.at[2 * SIDE, r], cross)
        kv_send(qkv.at[group, span, pl.ds(HEAD_DIM, 2 * HEAD_DIM)], kv_at(sp, r), kr.at[sp, r], ally)
        kv_send(qkv.at[group, span, pl.ds(HEAD_DIM, 2 * HEAD_DIM)], kv_at(sp, r), kr.at[sp, r], mate)

    ally_cross = lax.rem(x + 2, SIDE) * 2 + core

    def kv_wait(owner, r):
        arrived(kv_at(owner, r), kr.at[owner, r], tp, sp)

    def kv_cross(r):
        kv_wait(cross, r)
        kv_send(kv_at(cross, r), kv_at(cross, r), kr.at[cross, r], ally)
        kv_send(kv_at(cross, r), kv_at(cross, r), kr.at[cross, r], mate)

    def kv_ally(r):
        for owner in (ally, ally_cross):
            kv_wait(owner, r)
            kv_send(kv_at(owner, r), kv_at(owner, r), kr.at[owner, r], mate)

    def kv_mate(r):
        arrived(q_ref.at[pl.ds(rows + cuts[r], size[r]), :], kr.at[2 * SIDE, r], tp, sp)
        for d in range(SIDE):
            kv_wait(sp_at(d, 1), r)

    grid.near(0)
    w_own(1)
    grid.start(1)
    grid.far(0)
    grid.near(1)
    grid.last(0)
    w_near(0)
    grid.start(2)
    grid.far(1)
    grid.near(2)
    w_near(1)
    rings[0].own()
    grid.last(1)
    grid.start(3)
    rings[1].own()
    grid.far(2)
    w_far()
    w_mate()
    grid.final(0)
    project(0)
    grid.near(3)
    grid.final(1)
    project(1)
    rings[0].near()
    grid.last(2)
    grid.far(3)
    kv_cross(0)
    rings[1].near()
    grid.last(3)
    kv_cross(1)
    grid.final(2)
    project(2)
    grid.final(3)
    project(3)
    kv_ally(0)
    kv_ally(1)
    kv_cross(2)
    kv_cross(3)
    kv_ally(2)
    kv_ally(3)
    rings[0].far()
    rings[1].far()
    for r in range(CHUNKS):
        kv_mate(r)
    for d in range(1, 2 * SIDE):
        arrived(segall_ref.at[lax.rem(sp + d, 2 * SIDE)], sr.at[lax.rem(sp + d, 2 * SIDE)], tp, sp)
    segq_ref[1] = segall_ref[cross]
    for r in range(CHUNKS):
        grid.drain(r)
    for copy in w_sends + seg_copies + kv_sends + rings[0].sends + rings[1].sends:
        copy.wait_send()


def qkv_exchange(x_block, wqkv_block, wout_block, seg_block):
    rows, width = x_block.shape
    depth, cols = wqkv_block.shape
    sps, tps = 2 * SIDE, SIDE * SIDE
    seg_tile = seg_block.reshape(rows // HEAD_DIM, HEAD_DIM)
    vmem = pl.BlockSpec(memory_space=pltpu.VMEM)
    hbm = pl.BlockSpec(memory_space=pltpu.HBM)
    dma = pltpu.SemaphoreType.DMA
    return pl.pallas_call(
        qkv_kernel,
        out_shape=(
            jax.ShapeDtypeStruct((2 * rows, HEAD_DIM), jnp.bfloat16),
            jax.ShapeDtypeStruct((sps * rows, 2 * HEAD_DIM), jnp.bfloat16),
            jax.ShapeDtypeStruct((sps,) + seg_tile.shape, jnp.int32),
            jax.ShapeDtypeStruct((2,) + seg_tile.shape, jnp.int32),
            jax.ShapeDtypeStruct((SIDE, depth, HEAD_DIM), jnp.bfloat16),
            jax.ShapeDtypeStruct((SIDE, depth, HEAD_DIM), jnp.bfloat16),
        ),
        in_specs=[hbm] * 4,
        out_specs=(vmem,) * 6,
        scratch_shapes=[
            pltpu.VMEM((rows, tps * width), jnp.bfloat16),
            pltpu.VMEM((sps * depth, cols), jnp.bfloat16),
            pltpu.VMEM((2, rows, 3 * HEAD_DIM), jnp.bfloat16),
            dma((5,)),
            dma((CHUNKS, 2, 15)), dma((CHUNKS, 2, tps)),
            dma((14,)), dma((sps, 2)),
            dma((sps,)), dma((sps,)),
            dma((8 * CHUNKS,)), dma((sps + 1, CHUNKS)),
            dma((2, 6)), dma((2, SIDE, 2)),
        ],
        compiler_params=pltpu.CompilerParams(collective_id=0, has_side_effects=True, vmem_limit_bytes=26 * 1024 * 1024),
        name="qkv_exchange",
    )(*(pltpu.with_memory_space_constraint(a, pltpu.HBM) for a in (x_block, wqkv_block, wout_block, seg_tile)))


def output_kernel(ctx_ref, oa_ref, ob_ref, y_ref, o_all, w_all, part, os, orr, ws, wr, ms, mr, ys, yr):
    tp, sp = lax.axis_index("tp"), lax.axis_index("sp")
    z, y = tp // SIDE, lax.rem(tp, SIDE)
    x, core = sp // 2, lax.rem(sp, 2)
    rows = ctx_ref.shape[0] // 2
    quarter = rows // SIDE
    depth, width = oa_ref.shape[1], 2 * oa_ref.shape[2]
    group = x // 2
    cross = (SIDE - 1 - x) * 2 + core
    mate = x * 2 + 1 - core

    def x_at(d):
        return lax.rem(x + d, SIDE) * 2 + core

    def z_at(d):
        return lax.rem(z + d, SIDE)

    def y_at(d):
        return lax.rem(y + d, SIDE)

    peers = [(z_at(d) * SIDE + y, sp) for d in (1, 2, 3)]
    peers += [(z_at(d) * SIDE + y, cross) for d in range(SIDE)]
    peers += [(z * SIDE + y_at(d), sp) for d in (1, 2, 3)]
    peers += [(tp, x_at(1)), (tp, x_at(3)), (tp, mate)]
    barrier_with(peers)

    o_sends = []

    def o_slot(j, yo, b):
        return (z_at(j) * SIDE + yo) * 2 + (group if b == 0 else 1 - group)

    def o_col(slot):
        return o_all.at[:, pl.ds(pl.multiple_of(slot * HEAD_DIM, HEAD_DIM), HEAD_DIM)]

    def o_send(src, slot, to_tp, to_sp):
        copy = remote(src, o_col(slot), os.at[len(o_sends)], orr.at[slot], to_tp, to_sp)
        copy.start()
        o_sends.append(copy)

    def o_wait(slot):
        arrived(o_col(slot), orr.at[slot], tp, sp)

    def ctx_rows(j, b):
        return ctx_ref.at[pl.ds(pl.multiple_of(b * rows + z_at(j) * quarter, quarter), quarter), :]

    def o_along_y(j, b, src):
        slot = o_slot(j, y, b)
        for d in (1, 3):
            o_send(src, slot, z * SIDE + y_at(d), sp)

    mine = (z * SIDE + y) * 2 + group
    order = [(0, 1), (1, 0), (3, 0), (1, 1), (3, 1), (2, 0), (2, 1)]
    for j, b in order:
        o_send(ctx_rows(j, b), mine, z_at(j) * SIDE + y, sp if b == 0 else cross)
    o_along_y(0, 0, ctx_rows(0, 0))
    o_all[:, pl.ds(pl.multiple_of(mine * HEAD_DIM, HEAD_DIM), HEAD_DIM)] = ctx_ref[pl.ds(pl.multiple_of(z * quarter, quarter), quarter), :]

    half = width // 2
    m_sends = []

    def panel(r, h, u, v, c):
        return w_all.at[pl.ds(pl.multiple_of((u * 2 + c) * depth, depth), depth),
                        pl.ds(pl.multiple_of(v * width + h * half, half), half)]

    def held_already(r, h, u, v):
        return oa_ref.at[u] if h == 0 else ob_ref.at[v]

    def to_mate(r, h, u, v, src=None):
        held = panel(r, h, u, v, core)
        copy = remote(held if src is None else src, held, ms.at[len(m_sends)], mr.at[r, h, u * SIDE + v], tp, mate)
        copy.start()
        m_sends.append(copy)

    grid = Gather2D(
        (x, z), lambda u, v: (v * SIDE + y, u * 2 + core),
        held_already, lambda r, h, u, v: panel(r, h, u, v, core), ws, wr, to_mate, first_done=True)

    def o_near(j, b):
        for d in (3, 1):
            slot = o_slot(j, y_at(d), b)
            o_wait(slot)
            if d == (3 if (j + b) % 2 == 0 else 1):
                o_send(o_col(slot), slot, z * SIDE + y_at(4 - d), sp)

    def o_first(j, b):
        o_wait(o_slot(j, y, b))
        o_along_y(j, b, o_col(o_slot(j, y, b)))

    for j1 in range(SIDE):
        for h in (0, 1):
            grid.spread(0, h, j1)
    for j1 in range(SIDE):
        for h in (0, 1):
            u, v = grid.at(h, j1, 0)
            to_mate(0, h, u, v, held_already(0, h, u, v))
            rows_at = pl.ds(pl.multiple_of((u * 2 + core) * depth, depth), depth)
            w_all[rows_at, pl.ds(pl.multiple_of(v * width + h * half, half), half)] = oa_ref[u] if h == 0 else ob_ref[v]
    for j, b in order[0:3]:
        o_first(j, b)
    for j, b in ([(0, 0)] + order)[0:1]:
        o_near(j, b)
    grid.pass_on(0, 0)
    for j, b in order[3:7]:
        o_first(j, b)
    for j, b in ([(0, 0)] + order)[1:3]:
        o_near(j, b)
    grid.pass_on(0, 1)
    for j, b in ([(0, 0)] + order)[3:5]:
        o_near(j, b)
    grid.pass_on(0, 2)
    for j, b in ([(0, 0)] + order)[5:8]:
        o_near(j, b)
    grid.pass_on(0, 3)
    grid.final(0)
    for j, b in [(0, 0)] + order:
        o_wait(o_slot(j, y_at(2), b))
    for h in (0, 1):
        for d in range(SIDE * SIDE):
            u, v = lax.rem(x + d // SIDE, SIDE), z_at(d % SIDE)
            arrived(panel(0, h, u, v, 1 - core), mr.at[0, h, u * SIDE + v], tp, sp)

    y_sends = []
    strip = quarter // SIDE
    for zz in range(SIDE):
        out = jnp.dot(o_all[...], w_all[:, zz * width:(zz + 1) * width], preferred_element_type=jnp.float32)
        part[zz] = out.astype(jnp.bfloat16)
        cols = pl.ds(pl.multiple_of((zz * SIDE + y) * width, width), width)
        for d in (2, 1, 3):
            copy = remote(part.at[zz, pl.ds(pl.multiple_of(y_at(d) * strip, strip), strip), :], y_ref.at[:, cols],
                          ys.at[len(y_sends)], yr.at[zz, y], z * SIDE + y_at(d), sp)
            copy.start()
            y_sends.append(copy)
        y_ref[:, cols] = part[zz, pl.ds(pl.multiple_of(y * strip, strip), strip), :]
    for zz in range(SIDE):
        for d in (1, 3, 2):
            cols = pl.ds(pl.multiple_of((zz * SIDE + y_at(d)) * width, width), width)
            arrived(y_ref.at[:, cols], yr.at[zz, y_at(d)], tp, sp)
    grid.drain(0)
    for copy in o_sends + m_sends + y_sends:
        copy.wait_send()


def output_exchange(context, oa, ob):
    rows = context.shape[0] // 2
    depth, width = oa.shape[1], 2 * oa.shape[2]
    sps, tps = 2 * SIDE, SIDE * SIDE
    quarter = rows // SIDE
    vmem = pl.BlockSpec(memory_space=pltpu.VMEM)
    dma = pltpu.SemaphoreType.DMA
    return pl.pallas_call(
        output_kernel,
        out_shape=jax.ShapeDtypeStruct((quarter // SIDE, tps * width), jnp.bfloat16),
        in_specs=[vmem] * 3,
        out_specs=vmem,
        scratch_shapes=[
            pltpu.VMEM((quarter, tps * 2 * HEAD_DIM), jnp.bfloat16),
            pltpu.VMEM((sps * depth, SIDE * width), jnp.bfloat16),
            pltpu.VMEM((SIDE, quarter, width), jnp.bfloat16),
            dma((31,)), dma((2 * tps,)),
            dma((1, 2, 15)), dma((1, 2, tps)),
            dma((2 * tps,)), dma((1, 2, tps)),
            dma((3 * SIDE,)), dma((SIDE, SIDE)),
        ],
        compiler_params=pltpu.CompilerParams(collective_id=1, has_side_effects=True, vmem_limit_bytes=16 * 1024 * 1024),
        name="output_exchange",
    )(context, oa, ob)


def solution(mesh):
    def device_block(x_block, doc_block, wqkv_block, wout_block):
        q, kv, seg_all, seg_q, oa, ob = qkv_exchange(x_block, wqkv_block, wout_block, doc_block)
        context = attention(q, kv, seg_q.reshape(-1, HEAD_DIM), seg_all.reshape(-1, HEAD_DIM))
        return output_exchange(context, oa, ob)

    return jax.shard_map(
        device_block,
        mesh=mesh,
        in_specs=(P(("dp", "sp"), "tp"), P(("dp", "sp")), P("sp", "tp"), P("sp", "tp")),
        out_specs=P(("dp", "sp", "tp"), None),
        check_vma=False,
    )
```

```python
import functools

import jax
import jax.numpy as jnp
from jax import lax
from jax.experimental import pallas as pl
from jax.experimental.pallas import tpu as pltpu
from jax.sharding import PartitionSpec as P

HEAD_DIM = 128
EXP2_SCALE = HEAD_DIM ** -0.5 * 1.4426950408889634
FLOOR = -3.0e38
SMALL = 2.0 ** -77
LARGE = 2.0 ** 15


def seg_column(segq_ref, base, rows):
    tiles = [jnp.broadcast_to(segq_ref[pl.ds(base + i, 1), :], (HEAD_DIM, HEAD_DIM)).T for i in range(rows // HEAD_DIM)]
    return jnp.concatenate(tiles, axis=0)


def attention_kernel(qb, kb, sub, q_ref, kv_ref, segq_ref, segall_ref, o_ref, q2_ref, acc_ref, m_ref, l_ref, kmax_ref, segc_ref):
    step_id = pl.program_id(0)
    keys = kv_ref.shape[0]
    qrow = step_id * (qb // HEAD_DIM)

    @pl.when(step_id == 0)
    def _():
        def norms(j, best):
            k = kv_ref[pl.ds(pl.multiple_of(j * 2048, 2048), 2048), :HEAD_DIM].astype(jnp.float32)
            total = jnp.dot((k * k).astype(jnp.bfloat16), jnp.ones((HEAD_DIM, HEAD_DIM), jnp.bfloat16), preferred_element_type=jnp.float32)
            return jnp.maximum(best, jnp.max(total.reshape(-1, 8, HEAD_DIM), axis=0))

        kmax_ref[...] = jnp.sqrt(lax.fori_loop(0, keys // 2048, norms, jnp.zeros(kmax_ref.shape, jnp.float32)))

    segq = segq_ref[pl.ds(qrow, qb // HEAD_DIM), :]
    lo = jnp.min(segq)
    hi = jnp.max(segq)
    seg_all = segall_ref[...]
    first = jnp.sum(jnp.where(seg_all < lo, 1.0, 0.0)).astype(jnp.int32)
    last = jnp.sum(jnp.where(seg_all <= hi, 1.0, 0.0)).astype(jnp.int32)
    one_doc = lo == hi
    whole_rows = first // HEAD_DIM * HEAD_DIM
    units = (last - whole_rows + 256 - 1) // 256
    base = jnp.minimum(whole_rows, keys - units * 256)
    count = units * 256 // kb
    rest = units - count * (kb // 256)

    q = q_ref[...]
    qf = q.astype(jnp.float32)
    bound = jnp.sqrt(jnp.sum(qf * qf, axis=1, keepdims=True)) * jnp.max(kmax_ref[...], axis=0, keepdims=True) * (-1.01 / HEAD_DIM)
    q2_ref[:, :HEAD_DIM] = q
    q2_ref[:, HEAD_DIM:] = bound.astype(jnp.bfloat16)
    acc_ref[...] = jnp.zeros_like(acc_ref)
    segc_ref[...] = seg_column(segq_ref, qrow, qb)

    def same_doc(start, size, rows):
        row = jnp.concatenate([segall_ref[pl.ds(start // HEAD_DIM + i, 1), :] for i in range(size // HEAD_DIM)], axis=1)
        return segc_ref[rows, :1] == row

    def pieces(start, size):
        rows = pl.ds(pl.multiple_of(start, HEAD_DIM), size)
        return kv_ref[rows, :HEAD_DIM], kv_ref[rows, HEAD_DIM:]

    def block(start, size, masked):
        k, v = pieces(start, size)
        ones = jnp.ones((size, HEAD_DIM), jnp.bfloat16)
        k2 = jnp.concatenate([k, ones], axis=1)
        v2 = jnp.concatenate([v, ones], axis=1)
        for i in range(qb // sub):
            rows = slice(i * sub, (i + 1) * sub)
            s = lax.dot_general(q2_ref[rows, :], k2, (((1,), (1,)), ((), ())), preferred_element_type=jnp.float32)
            p = jnp.exp2(s * EXP2_SCALE)
            if masked:
                p = jnp.where(same_doc(start, size, rows), p, 0.0)
            acc_ref[rows, :] += jnp.dot(p.astype(jnp.bfloat16), v2, preferred_element_type=jnp.float32)

    def online(start, size):
        k, v = pieces(start, size)
        for i in range(qb // sub):
            rows = slice(i * sub, (i + 1) * sub)
            s = lax.dot_general(q_ref[rows, :], k, (((1,), (1,)), ((), ())), preferred_element_type=jnp.float32)
            t = jnp.where(same_doc(start, size, rows), s * EXP2_SCALE, -jnp.inf)
            m_prev = m_ref[rows, :1]
            m_new = jnp.maximum(m_prev, jnp.max(t, axis=1, keepdims=True))
            p = jnp.exp2(t - m_new)
            alpha = jnp.exp2(m_prev - m_new)
            l_new = l_ref[rows, :1] * alpha + jnp.sum(p, axis=1, keepdims=True)
            pv = jnp.dot(p.astype(jnp.bfloat16), v, preferred_element_type=jnp.float32)
            acc_ref[rows, :HEAD_DIM] = acc_ref[rows, :HEAD_DIM] * alpha + pv
            m_ref[rows, :] = jnp.broadcast_to(m_new, (sub, HEAD_DIM))
            l_ref[rows, :] = jnp.broadcast_to(l_new, (sub, HEAD_DIM))

    def step(j, carry):
        whole = one_doc & (base + j * kb >= first) & (base + (j + 1) * kb <= last)

        @pl.when(whole)
        def _():
            block(base + j * kb, kb, False)

        @pl.when(jnp.logical_not(whole))
        def _():
            block(base + j * kb, kb, True)

        return carry

    lax.fori_loop(0, count, step, 0)

    size = kb // 2
    while size >= 256:
        @pl.when(rest // (size // 256) % 2 == 1)
        def _(size=size):
            block(base + count * kb + rest // (2 * size // 256) * (2 * size), size, True)

        size //= 2

    total = acc_ref[:, HEAD_DIM:]
    o_ref[...] = (acc_ref[:, :HEAD_DIM] / total).astype(o_ref.dtype)

    @pl.when(jnp.logical_not((jnp.min(total) >= SMALL) & (jnp.max(total) <= LARGE)))
    def _():
        acc_ref[...] = jnp.zeros_like(acc_ref)
        l_ref[...] = jnp.zeros_like(l_ref)
        m_ref[...] = jnp.full_like(m_ref, FLOOR)

        def again(j, carry):
            online(base + j * 256, 256)
            return carry

        lax.fori_loop(0, units, again, 0)
        o_ref[...] = (acc_ref[:, :HEAD_DIM] / l_ref[...]).astype(o_ref.dtype)


def attention(q, kv, seg_q, seg_all, qb=1024, kb=2048, sub=256):
    rows, keys = q.shape[0], kv.shape[0]
    whole = lambda a: pl.BlockSpec(a, lambda i: (0, 0))
    f32 = lambda *shape: pltpu.VMEM(shape, jnp.float32)
    return pl.pallas_call(
        functools.partial(attention_kernel, qb, kb, sub),
        grid=(rows // qb,),
        out_shape=jax.ShapeDtypeStruct(q.shape, jnp.bfloat16),
        in_specs=[
            pl.BlockSpec((qb, HEAD_DIM), lambda i: (i, 0)),
            whole(kv.shape), whole(seg_q.shape), whole(seg_all.shape),
        ],
        out_specs=pl.BlockSpec((qb, HEAD_DIM), lambda i: (i, 0)),
        scratch_shapes=[
            pltpu.VMEM((qb, 2 * HEAD_DIM), jnp.bfloat16),
            f32(qb, 2 * HEAD_DIM), f32(qb, HEAD_DIM), f32(qb, HEAD_DIM), f32(8, HEAD_DIM),
            pltpu.VMEM((qb, HEAD_DIM), jnp.int32),
        ],
        compiler_params=pltpu.CompilerParams(vmem_limit_bytes=24 * 1024 * 1024),
        name="attention",
    )(q, kv, seg_q, seg_all)

SIDE = 4
CUTS = (0, 8, 16, 24, 32)
CHUNKS = len(CUTS) - 1
MESH = pl.DeviceIdType.MESH


def remote(src, dst, send_sem, recv_sem, tp, sp):
    return pltpu.make_async_remote_copy(
        src_ref=src, dst_ref=dst, send_sem=send_sem, recv_sem=recv_sem,
        device_id={"tp": tp, "sp": sp}, device_id_type=MESH)


def arrived(ref, sem, tp, sp):
    remote(ref, ref, sem, sem, tp, sp).wait_recv()


def barrier_with(peers):
    barrier = pltpu.get_barrier_semaphore()
    for tp, sp in peers:
        pl.semaphore_signal(barrier, inc=1, device_id={"tp": tp, "sp": sp}, device_id_type=MESH)
    pl.semaphore_wait(barrier, len(peers))


class Gather2D:
    def __init__(self, coords, place, own, held, send_sem, recv_sem, on_arrival=None, first_done=False):
        self.coords, self.place, self.own, self.held = coords, place, own, held
        self.send_sem, self.recv_sem, self.on_arrival = send_sem, recv_sem, on_arrival
        self.first_done = first_done
        self.sent = {}

    def at(self, h, j1, j2):
        u, v = self.coords
        j1, j2 = (j1, j2) if h == 0 else (j2, j1)
        return lax.rem(u + j1, SIDE), lax.rem(v + j2, SIDE)

    def send(self, r, h, piece, to):
        src_at, dst_at = self.at(h, *piece), self.at(h, *to)
        local = piece == (0, 0) or (self.first_done and piece[1] == 0)
        src = self.own(r, h, *src_at) if local else self.held(r, h, *src_at)
        k = self.sent.get((r, h), 0)
        self.sent[r, h] = k + 1
        copy = remote(src, self.held(r, h, *src_at), self.send_sem.at[r, h, k],
                      self.recv_sem.at[r, h, src_at[0] * SIDE + src_at[1]], *self.place(*dst_at))
        copy.start()

    def wait(self, r, h, piece):
        src_at = self.at(h, *piece)
        arrived(self.held(r, h, *src_at), self.recv_sem.at[r, h, src_at[0] * SIDE + src_at[1]], *self.place(*self.coords))
        if self.on_arrival is not None:
            self.on_arrival(r, h, *src_at)

    def start(self, r):
        for to in ((1, 0), (3, 0), (0, 1), (0, 3)):
            for h in (0, 1):
                self.send(r, h, (0, 0), to)

    def spread(self, r, h, j1):
        for j2 in (1, 3):
            self.send(r, h, (j1, 0), (0, j2))

    def near(self, r):
        for j1 in (3, 1):
            for h in (0, 1):
                self.wait(r, h, (j1, 0))
                if j1 == (3 if (r + h) % 2 == 0 else 1):
                    self.send(r, h, (j1, 0), (4 - j1, 0))
                self.spread(r, h, j1)

    def pass_on(self, r, j1):
        for h in (0, 1):
            for j2 in (3, 1):
                self.wait(r, h, (j1, j2))
                if j2 == (3 if (r + h + (j1 + 1) // 2) % 2 == 0 else 1):
                    self.send(r, h, (j1, j2), (0, 4 - j2))

    def far(self, r):
        self.pass_on(r, 0)
        for h in (0, 1):
            self.wait(r, h, (2, 0))
            self.spread(r, h, 2)

    def last(self, r):
        for j1 in (3, 1, 2):
            self.pass_on(r, j1)

    def final(self, r):
        for j1 in (0, 3, 1, 2):
            for h in (0, 1):
                self.wait(r, h, (j1, 2))

    def drain(self, r):
        for h in (0, 1):
            for k in range(self.sent[r, h]):
                ref = self.held(r, h, *self.coords)
                remote(ref, ref, self.send_sem.at[r, h, k], self.recv_sem.at[r, h, 0], *self.place(*self.coords)).wait_send()


def qkv_kernel(x_ref, w_ref, wo_ref, seg_ref, q_ref, kv_ref, segall_ref, segq_ref, oa_ref, ob_ref,
               x_all, w_all, qkv, ls, xs, xr, ws, wr, ss, sr, ks, kr, rs, rr):
    tp, sp = lax.axis_index("tp"), lax.axis_index("sp")
    z, y = tp // SIDE, lax.rem(tp, SIDE)
    x, core = sp // 2, lax.rem(sp, 2)
    rows, width = x_ref.shape
    depth = w_ref.shape[0]
    cuts = [rows * c // CUTS[-1] for c in CUTS]
    size = [b - a for a, b in zip(cuts, cuts[1:])]
    half = width // 2

    def sp_at(dx, other=0):
        return lax.rem(x + dx, SIDE) * 2 + lax.rem(core + other, 2)

    mate = sp_at(0, 1)
    group = x // 2
    ally = (x + 1 - 2 * lax.rem(x, 2)) * 2 + core
    cross = (SIDE - 1 - x) * 2 + core

    peers = [(lax.rem(z + d, SIDE) * SIDE + y, sp) for d in (1, 3)]
    peers += [(z * SIDE + lax.rem(y + d, SIDE), sp) for d in (1, 3)]
    peers += [(tp, lax.rem(sp + d, 2 * SIDE)) for d in range(1, 2 * SIDE)]
    x_own = x_all.at[:, pl.ds(pl.multiple_of(tp * width, width), width)]
    w_own_rows = w_all.at[pl.ds(pl.multiple_of(sp * depth, depth), depth), :]
    loads = [pltpu.make_async_copy(x_ref, x_own, ls.at[0]), pltpu.make_async_copy(w_ref, w_own_rows, ls.at[1]),
             pltpu.make_async_copy(seg_ref, segq_ref.at[0], ls.at[2]),
             pltpu.make_async_copy(wo_ref.at[:, pl.ds(0, HEAD_DIM)], oa_ref.at[x], ls.at[3]),
             pltpu.make_async_copy(wo_ref.at[:, pl.ds(HEAD_DIM, HEAD_DIM)], ob_ref.at[z], ls.at[4])]
    for load in loads:
        load.start()
    barrier_with(peers)
    for load in loads:
        load.wait()

    grid = Gather2D(
        (z, y), lambda u, v: (u * SIDE + v, sp),
        lambda r, h, u, v: x_own.at[pl.ds(cuts[r], size[r]), pl.ds(h * half, half)],
        lambda r, h, u, v: x_all.at[pl.ds(cuts[r], size[r]), pl.ds(pl.multiple_of((u * SIDE + v) * width + h * half, half), half)],
        xs, xr)

    def w_at(owner, p):
        return w_all.at[pl.ds(pl.multiple_of(owner * depth + p * (depth // 2), depth // 2), depth // 2), :]

    w_sends = []

    def w_send(owner, p, to):
        k = len(w_sends)
        copy = remote(w_at(owner, p), w_at(owner, p), ws.at[k], wr.at[owner, p], tp, to)
        copy.start()
        w_sends.append(copy)

    def w_wait(owner, p):
        arrived(w_at(owner, p), wr.at[owner, p], tp, sp)

    def w_own(p):
        for to in (sp_at(1), sp_at(3), mate):
            w_send(sp, p, to)

    def w_near(p):
        for d in (3, 1):
            w_wait(sp_at(d), p)
            if d == (3 if p == 0 else 1):
                w_send(sp_at(d), p, sp_at(4 - d))
            w_send(sp_at(d), p, mate)

    def w_far():
        for p in (0, 1):
            w_wait(sp_at(2), p)
            w_send(sp_at(2), p, mate)

    def w_mate():
        for p in (0, 1):
            for d in (0, 1, 3, 2):
                w_wait(sp_at(d, 1), p)

    class Ring:
        def __init__(self, axis):
            self.axis, self.ref, self.me = axis, (oa_ref, ob_ref)[axis], (x, z)[axis]
            self.sends = []

        def at(self, d, p):
            return self.ref.at[lax.rem(self.me + d, SIDE), pl.ds(p * (depth // 2), depth // 2), :]

        def sem(self, d, p):
            return rr.at[self.axis, lax.rem(self.me + d, SIDE), p]

        def send(self, d, p, to):
            device = (tp, sp_at(to)) if self.axis == 0 else (lax.rem(z + to, SIDE) * SIDE + y, sp)
            copy = remote(self.at(d, p), self.at(d, p), rs.at[self.axis, len(self.sends)], self.sem(d, p), *device)
            copy.start()
            self.sends.append(copy)

        def own(self):
            for p in (0, 1):
                for to in (1, 3):
                    self.send(0, p, to)

        def near(self):
            for p in (0, 1):
                for d in (3, 1):
                    arrived(self.at(d, p), self.sem(d, p), tp, sp)
                    if d == (3 if p == 0 else 1):
                        self.send(d, p, 4 - d)

        def far(self):
            for p in (0, 1):
                arrived(self.at(2, p), self.sem(2, p), tp, sp)

    rings = Ring(0), Ring(1)

    grid.start(0)
    w_own(0)
    seg_copies = []
    for d in range(1, 2 * SIDE):
        copy = remote(segq_ref.at[0], segall_ref.at[sp], ss.at[d], sr.at[sp], tp, lax.rem(sp + d, 2 * SIDE))
        copy.start()
        seg_copies.append(copy)
    segall_ref[sp] = segq_ref[0]

    def kv_at(owner, r):
        return kv_ref.at[pl.ds(pl.multiple_of(owner * rows + cuts[r], 64), size[r]), :]

    kv_sends = []

    def kv_send(src, dst, recv, to):
        k = len(kv_sends)
        copy = remote(src, dst, ks.at[k], recv, tp, to)
        copy.start()
        kv_sends.append(copy)

    def project(r):
        here = slice(cuts[r], cuts[r + 1])
        for n in range(3):
            part = slice(n * 256, (n + 1) * 256)
            out = jnp.dot(x_all[here, :], w_all[:, part], preferred_element_type=jnp.float32).astype(jnp.bfloat16)
            for m in range(2):
                col = n * 2 + m
                qkv[col // 3, here, (col % 3) * HEAD_DIM:(col % 3 + 1) * HEAD_DIM] = out[:, m * HEAD_DIM:(m + 1) * HEAD_DIM]
        q_ref[here, :] = qkv[group, here, :HEAD_DIM]
        kv_ref[pl.ds(pl.multiple_of(sp * rows + cuts[r], 64), size[r]), :] = qkv[group, here, HEAD_DIM:]
        span = pl.ds(cuts[r], size[r])
        kv_send(qkv.at[1 - group, span, pl.ds(HEAD_DIM, 2 * HEAD_DIM)], kv_at(sp, r), kr.at[sp, r], cross)
        kv_send(qkv.at[1 - group, span, pl.ds(0, HEAD_DIM)], q_ref.at[pl.ds(rows + cuts[r], size[r]), :], kr.at[2 * SIDE, r], cross)
        kv_send(qkv.at[group, span, pl.ds(HEAD_DIM, 2 * HEAD_DIM)], kv_at(sp, r), kr.at[sp, r], ally)
        kv_send(qkv.at[group, span, pl.ds(HEAD_DIM, 2 * HEAD_DIM)], kv_at(sp, r), kr.at[sp, r], mate)

    ally_cross = lax.rem(x + 2, SIDE) * 2 + core

    def kv_wait(owner, r):
        arrived(kv_at(owner, r), kr.at[owner, r], tp, sp)

    def kv_cross(r):
        kv_wait(cross, r)
        kv_send(kv_at(cross, r), kv_at(cross, r), kr.at[cross, r], ally)
        kv_send(kv_at(cross, r), kv_at(cross, r), kr.at[cross, r], mate)

    def kv_ally(r):
        for owner in (ally, ally_cross):
            kv_wait(owner, r)
            kv_send(kv_at(owner, r), kv_at(owner, r), kr.at[owner, r], mate)

    def kv_mate(r):
        arrived(q_ref.at[pl.ds(rows + cuts[r], size[r]), :], kr.at[2 * SIDE, r], tp, sp)
        for d in range(SIDE):
            kv_wait(sp_at(d, 1), r)

    grid.near(0)
    w_own(1)
    grid.start(1)
    grid.far(0)
    grid.near(1)
    grid.last(0)
    w_near(0)
    grid.start(2)
    grid.far(1)
    grid.near(2)
    w_near(1)
    rings[0].own()
    grid.last(1)
    grid.start(3)
    rings[1].own()
    grid.far(2)
    w_far()
    w_mate()
    grid.final(0)
    project(0)
    grid.near(3)
    grid.final(1)
    project(1)
    rings[0].near()
    grid.last(2)
    grid.far(3)
    kv_cross(0)
    rings[1].near()
    grid.last(3)
    kv_cross(1)
    grid.final(2)
    project(2)
    grid.final(3)
    project(3)
    kv_ally(0)
    kv_ally(1)
    kv_cross(2)
    kv_cross(3)
    kv_ally(2)
    kv_ally(3)
    rings[0].far()
    rings[1].far()
    for r in range(CHUNKS):
        kv_mate(r)
    for d in range(1, 2 * SIDE):
        arrived(segall_ref.at[lax.rem(sp + d, 2 * SIDE)], sr.at[lax.rem(sp + d, 2 * SIDE)], tp, sp)
    segq_ref[1] = segall_ref[cross]
    for r in range(CHUNKS):
        grid.drain(r)
    for copy in w_sends + seg_copies + kv_sends + rings[0].sends + rings[1].sends:
        copy.wait_send()


def qkv_exchange(x_block, wqkv_block, wout_block, seg_block):
    rows, width = x_block.shape
    depth, cols = wqkv_block.shape
    sps, tps = 2 * SIDE, SIDE * SIDE
    seg_tile = seg_block.reshape(rows // HEAD_DIM, HEAD_DIM)
    vmem = pl.BlockSpec(memory_space=pltpu.VMEM)
    hbm = pl.BlockSpec(memory_space=pltpu.HBM)
    dma = pltpu.SemaphoreType.DMA
    return pl.pallas_call(
        qkv_kernel,
        out_shape=(
            jax.ShapeDtypeStruct((2 * rows, HEAD_DIM), jnp.bfloat16),
            jax.ShapeDtypeStruct((sps * rows, 2 * HEAD_DIM), jnp.bfloat16),
            jax.ShapeDtypeStruct((sps,) + seg_tile.shape, jnp.int32),
            jax.ShapeDtypeStruct((2,) + seg_tile.shape, jnp.int32),
            jax.ShapeDtypeStruct((SIDE, depth, HEAD_DIM), jnp.bfloat16),
            jax.ShapeDtypeStruct((SIDE, depth, HEAD_DIM), jnp.bfloat16),
        ),
        in_specs=[hbm] * 4,
        out_specs=(vmem,) * 6,
        scratch_shapes=[
            pltpu.VMEM((rows, tps * width), jnp.bfloat16),
            pltpu.VMEM((sps * depth, cols), jnp.bfloat16),
            pltpu.VMEM((2, rows, 3 * HEAD_DIM), jnp.bfloat16),
            dma((5,)),
            dma((CHUNKS, 2, 15)), dma((CHUNKS, 2, tps)),
            dma((14,)), dma((sps, 2)),
            dma((sps,)), dma((sps,)),
            dma((8 * CHUNKS,)), dma((sps + 1, CHUNKS)),
            dma((2, 6)), dma((2, SIDE, 2)),
        ],
        compiler_params=pltpu.CompilerParams(collective_id=0, has_side_effects=True, vmem_limit_bytes=26 * 1024 * 1024),
        name="qkv_exchange",
    )(*(pltpu.with_memory_space_constraint(a, pltpu.HBM) for a in (x_block, wqkv_block, wout_block, seg_tile)))


def output_kernel(ctx_ref, oa_ref, ob_ref, y_ref, o_all, w_all, part, os, orr, ws, wr, ms, mr, ys, yr):
    tp, sp = lax.axis_index("tp"), lax.axis_index("sp")
    z, y = tp // SIDE, lax.rem(tp, SIDE)
    x, core = sp // 2, lax.rem(sp, 2)
    rows = ctx_ref.shape[0] // 2
    quarter = rows // SIDE
    depth, width = oa_ref.shape[1], 2 * oa_ref.shape[2]
    group = x // 2
    cross = (SIDE - 1 - x) * 2 + core
    mate = x * 2 + 1 - core

    def x_at(d):
        return lax.rem(x + d, SIDE) * 2 + core

    def z_at(d):
        return lax.rem(z + d, SIDE)

    def y_at(d):
        return lax.rem(y + d, SIDE)

    peers = [(z_at(d) * SIDE + y, sp) for d in (1, 2, 3)]
    peers += [(z_at(d) * SIDE + y, cross) for d in range(SIDE)]
    peers += [(z * SIDE + y_at(d), sp) for d in (1, 2, 3)]
    peers += [(tp, x_at(1)), (tp, x_at(3)), (tp, mate)]
    barrier_with(peers)

    o_sends = []

    def o_slot(j, yo, b):
        return (z_at(j) * SIDE + yo) * 2 + (group if b == 0 else 1 - group)

    def o_col(slot):
        return o_all.at[:, pl.ds(pl.multiple_of(slot * HEAD_DIM, HEAD_DIM), HEAD_DIM)]

    def o_send(src, slot, to_tp, to_sp):
        copy = remote(src, o_col(slot), os.at[len(o_sends)], orr.at[slot], to_tp, to_sp)
        copy.start()
        o_sends.append(copy)

    def o_wait(slot):
        arrived(o_col(slot), orr.at[slot], tp, sp)

    def ctx_rows(j, b):
        return ctx_ref.at[pl.ds(pl.multiple_of(b * rows + z_at(j) * quarter, quarter), quarter), :]

    def o_along_y(j, b, src):
        slot = o_slot(j, y, b)
        for d in (1, 3):
            o_send(src, slot, z * SIDE + y_at(d), sp)

    mine = (z * SIDE + y) * 2 + group
    order = [(0, 1), (1, 0), (3, 0), (1, 1), (3, 1), (2, 0), (2, 1)]
    for j, b in order:
        o_send(ctx_rows(j, b), mine, z_at(j) * SIDE + y, sp if b == 0 else cross)
    o_along_y(0, 0, ctx_rows(0, 0))
    o_all[:, pl.ds(pl.multiple_of(mine * HEAD_DIM, HEAD_DIM), HEAD_DIM)] = ctx_ref[pl.ds(pl.multiple_of(z * quarter, quarter), quarter), :]

    half = width // 2
    m_sends = []

    def panel(r, h, u, v, c):
        return w_all.at[pl.ds(pl.multiple_of((u * 2 + c) * depth, depth), depth),
                        pl.ds(pl.multiple_of(v * width + h * half, half), half)]

    def held_already(r, h, u, v):
        return oa_ref.at[u] if h == 0 else ob_ref.at[v]

    def to_mate(r, h, u, v, src=None):
        held = panel(r, h, u, v, core)
        copy = remote(held if src is None else src, held, ms.at[len(m_sends)], mr.at[r, h, u * SIDE + v], tp, mate)
        copy.start()
        m_sends.append(copy)

    grid = Gather2D(
        (x, z), lambda u, v: (v * SIDE + y, u * 2 + core),
        held_already, lambda r, h, u, v: panel(r, h, u, v, core), ws, wr, to_mate, first_done=True)

    def o_near(j, b):
        for d in (3, 1):
            slot = o_slot(j, y_at(d), b)
            o_wait(slot)
            if d == (3 if (j + b) % 2 == 0 else 1):
                o_send(o_col(slot), slot, z * SIDE + y_at(4 - d), sp)

    def o_first(j, b):
        o_wait(o_slot(j, y, b))
        o_along_y(j, b, o_col(o_slot(j, y, b)))

    for j1 in range(SIDE):
        for h in (0, 1):
            grid.spread(0, h, j1)
    for j1 in range(SIDE):
        for h in (0, 1):
            u, v = grid.at(h, j1, 0)
            to_mate(0, h, u, v, held_already(0, h, u, v))
            rows_at = pl.ds(pl.multiple_of((u * 2 + core) * depth, depth), depth)
            w_all[rows_at, pl.ds(pl.multiple_of(v * width + h * half, half), half)] = oa_ref[u] if h == 0 else ob_ref[v]
    for j, b in order[0:3]:
        o_first(j, b)
    for j, b in ([(0, 0)] + order)[0:1]:
        o_near(j, b)
    for j, b in order[3:5]:
        o_first(j, b)
    for j, b in ([(0, 0)] + order)[1:3]:
        o_near(j, b)
    for j, b in order[5:7]:
        o_first(j, b)
    grid.pass_on(0, 0)
    for j, b in ([(0, 0)] + order)[3:5]:
        o_near(j, b)
    grid.pass_on(0, 1)
    for j, b in ([(0, 0)] + order)[5:8]:
        o_near(j, b)
    grid.pass_on(0, 2)
    grid.pass_on(0, 3)
    grid.final(0)
    for j, b in [(0, 0)] + order:
        o_wait(o_slot(j, y_at(2), b))
    for h in (0, 1):
        for d in range(SIDE * SIDE):
            u, v = lax.rem(x + d // SIDE, SIDE), z_at(d % SIDE)
            arrived(panel(0, h, u, v, 1 - core), mr.at[0, h, u * SIDE + v], tp, sp)

    y_sends = []
    strip = quarter // SIDE
    for zz in range(SIDE):
        out = jnp.dot(o_all[...], w_all[:, zz * width:(zz + 1) * width], preferred_element_type=jnp.float32)
        part[zz] = out.astype(jnp.bfloat16)
        cols = pl.ds(pl.multiple_of((zz * SIDE + y) * width, width), width)
        for d in (2, 1, 3):
            copy = remote(part.at[zz, pl.ds(pl.multiple_of(y_at(d) * strip, strip), strip), :], y_ref.at[:, cols],
                          ys.at[len(y_sends)], yr.at[zz, y], z * SIDE + y_at(d), sp)
            copy.start()
            y_sends.append(copy)
        y_ref[:, cols] = part[zz, pl.ds(pl.multiple_of(y * strip, strip), strip), :]
    for zz in range(SIDE):
        for d in (1, 3, 2):
            cols = pl.ds(pl.multiple_of((zz * SIDE + y_at(d)) * width, width), width)
            arrived(y_ref.at[:, cols], yr.at[zz, y_at(d)], tp, sp)
    grid.drain(0)
    for copy in o_sends + m_sends + y_sends:
        copy.wait_send()


def output_exchange(context, oa, ob):
    rows = context.shape[0] // 2
    depth, width = oa.shape[1], 2 * oa.shape[2]
    sps, tps = 2 * SIDE, SIDE * SIDE
    quarter = rows // SIDE
    vmem = pl.BlockSpec(memory_space=pltpu.VMEM)
    dma = pltpu.SemaphoreType.DMA
    return pl.pallas_call(
        output_kernel,
        out_shape=jax.ShapeDtypeStruct((quarter // SIDE, tps * width), jnp.bfloat16),
        in_specs=[vmem] * 3,
        out_specs=vmem,
        scratch_shapes=[
            pltpu.VMEM((quarter, tps * 2 * HEAD_DIM), jnp.bfloat16),
            pltpu.VMEM((sps * depth, SIDE * width), jnp.bfloat16),
            pltpu.VMEM((SIDE, quarter, width), jnp.bfloat16),
            dma((31,)), dma((2 * tps,)),
            dma((1, 2, 15)), dma((1, 2, tps)),
            dma((2 * tps,)), dma((1, 2, tps)),
            dma((3 * SIDE,)), dma((SIDE, SIDE)),
        ],
        compiler_params=pltpu.CompilerParams(collective_id=1, has_side_effects=True, vmem_limit_bytes=16 * 1024 * 1024),
        name="output_exchange",
    )(context, oa, ob)


def solution(mesh):
    def device_block(x_block, doc_block, wqkv_block, wout_block):
        q, kv, seg_all, seg_q, oa, ob = qkv_exchange(x_block, wqkv_block, wout_block, doc_block)
        context = attention(q, kv, seg_q.reshape(-1, HEAD_DIM), seg_all.reshape(-1, HEAD_DIM))
        return output_exchange(context, oa, ob)

    return jax.shard_map(
        device_block,
        mesh=mesh,
        in_specs=(P(("dp", "sp"), "tp"), P(("dp", "sp")), P("sp", "tp"), P("sp", "tp")),
        out_specs=P(("dp", "sp", "tp"), None),
        check_vma=False,
    )
```

```python
import functools

import jax
import jax.numpy as jnp
from jax import lax
from jax.experimental import pallas as pl
from jax.experimental.pallas import tpu as pltpu
from jax.sharding import PartitionSpec as P

HEAD_DIM = 128
EXP2_SCALE = HEAD_DIM ** -0.5 * 1.4426950408889634
FLOOR = -3.0e38
SMALL = 2.0 ** -77
LARGE = 2.0 ** 15


def seg_column(segq_ref, base, rows):
    tiles = [jnp.broadcast_to(segq_ref[pl.ds(base + i, 1), :], (HEAD_DIM, HEAD_DIM)).T for i in range(rows // HEAD_DIM)]
    return jnp.concatenate(tiles, axis=0)


def attention_kernel(qb, kb, sub, q_ref, kv_ref, segq_ref, segall_ref, o_ref, q2_ref, acc_ref, m_ref, l_ref, kmax_ref, segc_ref):
    step_id = pl.program_id(0)
    keys = kv_ref.shape[0]
    qrow = step_id * (qb // HEAD_DIM)

    @pl.when(step_id == 0)
    def _():
        def norms(j, best):
            k = kv_ref[pl.ds(pl.multiple_of(j * 2048, 2048), 2048), :HEAD_DIM].astype(jnp.float32)
            total = jnp.dot((k * k).astype(jnp.bfloat16), jnp.ones((HEAD_DIM, HEAD_DIM), jnp.bfloat16), preferred_element_type=jnp.float32)
            return jnp.maximum(best, jnp.max(total.reshape(-1, 8, HEAD_DIM), axis=0))

        kmax_ref[...] = jnp.sqrt(lax.fori_loop(0, keys // 2048, norms, jnp.zeros(kmax_ref.shape, jnp.float32)))

    segq = segq_ref[pl.ds(qrow, qb // HEAD_DIM), :]
    lo = jnp.min(segq)
    hi = jnp.max(segq)
    seg_all = segall_ref[...]
    first = jnp.sum(jnp.where(seg_all < lo, 1.0, 0.0)).astype(jnp.int32)
    last = jnp.sum(jnp.where(seg_all <= hi, 1.0, 0.0)).astype(jnp.int32)
    one_doc = lo == hi
    whole_rows = first // HEAD_DIM * HEAD_DIM
    units = (last - whole_rows + 256 - 1) // 256
    base = jnp.minimum(whole_rows, keys - units * 256)
    count = units * 256 // kb
    rest = units - count * (kb // 256)

    q = q_ref[...]
    qf = q.astype(jnp.float32)
    bound = jnp.sqrt(jnp.sum(qf * qf, axis=1, keepdims=True)) * jnp.max(kmax_ref[...], axis=0, keepdims=True) * (-1.01 / HEAD_DIM)
    q2_ref[:, :HEAD_DIM] = q
    q2_ref[:, HEAD_DIM:] = bound.astype(jnp.bfloat16)
    acc_ref[...] = jnp.zeros_like(acc_ref)
    segc_ref[...] = seg_column(segq_ref, qrow, qb)

    def same_doc(start, size, rows):
        row = jnp.concatenate([segall_ref[pl.ds(start // HEAD_DIM + i, 1), :] for i in range(size // HEAD_DIM)], axis=1)
        return segc_ref[rows, :1] == row

    def pieces(start, size):
        rows = pl.ds(pl.multiple_of(start, HEAD_DIM), size)
        return kv_ref[rows, :HEAD_DIM], kv_ref[rows, HEAD_DIM:]

    def block(start, size, masked):
        k, v = pieces(start, size)
        ones = jnp.ones((size, HEAD_DIM), jnp.bfloat16)
        k2 = jnp.concatenate([k, ones], axis=1)
        v2 = jnp.concatenate([v, ones], axis=1)
        for i in range(qb // sub):
            rows = slice(i * sub, (i + 1) * sub)
            s = lax.dot_general(q2_ref[rows, :], k2, (((1,), (1,)), ((), ())), preferred_element_type=jnp.float32)
            p = jnp.exp2(s * EXP2_SCALE)
            if masked:
                p = jnp.where(same_doc(start, size, rows), p, 0.0)
            acc_ref[rows, :] += jnp.dot(p.astype(jnp.bfloat16), v2, preferred_element_type=jnp.float32)

    def online(start, size):
        k, v = pieces(start, size)
        for i in range(qb // sub):
            rows = slice(i * sub, (i + 1) * sub)
            s = lax.dot_general(q_ref[rows, :], k, (((1,), (1,)), ((), ())), preferred_element_type=jnp.float32)
            t = jnp.where(same_doc(start, size, rows), s * EXP2_SCALE, -jnp.inf)
            m_prev = m_ref[rows, :1]
            m_new = jnp.maximum(m_prev, jnp.max(t, axis=1, keepdims=True))
            p = jnp.exp2(t - m_new)
            alpha = jnp.exp2(m_prev - m_new)
            l_new = l_ref[rows, :1] * alpha + jnp.sum(p, axis=1, keepdims=True)
            pv = jnp.dot(p.astype(jnp.bfloat16), v, preferred_element_type=jnp.float32)
            acc_ref[rows, :HEAD_DIM] = acc_ref[rows, :HEAD_DIM] * alpha + pv
            m_ref[rows, :] = jnp.broadcast_to(m_new, (sub, HEAD_DIM))
            l_ref[rows, :] = jnp.broadcast_to(l_new, (sub, HEAD_DIM))

    def step(j, carry):
        whole = one_doc & (base + j * kb >= first) & (base + (j + 1) * kb <= last)

        @pl.when(whole)
        def _():
            block(base + j * kb, kb, False)

        @pl.when(jnp.logical_not(whole))
        def _():
            block(base + j * kb, kb, True)

        return carry

    lax.fori_loop(0, count, step, 0)

    size = kb // 2
    while size >= 256:
        @pl.when(rest // (size // 256) % 2 == 1)
        def _(size=size):
            block(base + count * kb + rest // (2 * size // 256) * (2 * size), size, True)

        size //= 2

    total = acc_ref[:, HEAD_DIM:]
    o_ref[...] = (acc_ref[:, :HEAD_DIM] / total).astype(o_ref.dtype)

    @pl.when(jnp.logical_not((jnp.min(total) >= SMALL) & (jnp.max(total) <= LARGE)))
    def _():
        acc_ref[...] = jnp.zeros_like(acc_ref)
        l_ref[...] = jnp.zeros_like(l_ref)
        m_ref[...] = jnp.full_like(m_ref, FLOOR)

        def again(j, carry):
            online(base + j * 256, 256)
            return carry

        lax.fori_loop(0, units, again, 0)
        o_ref[...] = (acc_ref[:, :HEAD_DIM] / l_ref[...]).astype(o_ref.dtype)


def attention(q, kv, seg_q, seg_all, qb=1024, kb=2048, sub=256):
    rows, keys = q.shape[0], kv.shape[0]
    whole = lambda a: pl.BlockSpec(a, lambda i: (0, 0))
    f32 = lambda *shape: pltpu.VMEM(shape, jnp.float32)
    return pl.pallas_call(
        functools.partial(attention_kernel, qb, kb, sub),
        grid=(rows // qb,),
        out_shape=jax.ShapeDtypeStruct(q.shape, jnp.bfloat16),
        in_specs=[
            pl.BlockSpec((qb, HEAD_DIM), lambda i: (i, 0)),
            whole(kv.shape), whole(seg_q.shape), whole(seg_all.shape),
        ],
        out_specs=pl.BlockSpec((qb, HEAD_DIM), lambda i: (i, 0)),
        scratch_shapes=[
            pltpu.VMEM((qb, 2 * HEAD_DIM), jnp.bfloat16),
            f32(qb, 2 * HEAD_DIM), f32(qb, HEAD_DIM), f32(qb, HEAD_DIM), f32(8, HEAD_DIM),
            pltpu.VMEM((qb, HEAD_DIM), jnp.int32),
        ],
        compiler_params=pltpu.CompilerParams(vmem_limit_bytes=24 * 1024 * 1024),
        name="attention",
    )(q, kv, seg_q, seg_all)

SIDE = 4
CUTS = (0, 8, 16, 24, 32)
CHUNKS = len(CUTS) - 1
MESH = pl.DeviceIdType.MESH


def remote(src, dst, send_sem, recv_sem, tp, sp):
    return pltpu.make_async_remote_copy(
        src_ref=src, dst_ref=dst, send_sem=send_sem, recv_sem=recv_sem,
        device_id={"tp": tp, "sp": sp}, device_id_type=MESH)


def arrived(ref, sem, tp, sp):
    remote(ref, ref, sem, sem, tp, sp).wait_recv()


def barrier_with(peers, meanwhile=None):
    barrier = pltpu.get_barrier_semaphore()
    for tp, sp in peers:
        pl.semaphore_signal(barrier, inc=1, device_id={"tp": tp, "sp": sp}, device_id_type=MESH)
    if meanwhile is not None:
        meanwhile()
    pl.semaphore_wait(barrier, len(peers))


class Gather2D:
    def __init__(self, coords, place, own, held, send_sem, recv_sem, on_arrival=None, first_done=False):
        self.coords, self.place, self.own, self.held = coords, place, own, held
        self.send_sem, self.recv_sem, self.on_arrival = send_sem, recv_sem, on_arrival
        self.first_done = first_done
        self.sent = {}

    def at(self, h, j1, j2):
        u, v = self.coords
        j1, j2 = (j1, j2) if h == 0 else (j2, j1)
        return lax.rem(u + j1, SIDE), lax.rem(v + j2, SIDE)

    def send(self, r, h, piece, to):
        src_at, dst_at = self.at(h, *piece), self.at(h, *to)
        local = piece == (0, 0) or (self.first_done and piece[1] == 0)
        src = self.own(r, h, *src_at) if local else self.held(r, h, *src_at)
        k = self.sent.get((r, h), 0)
        self.sent[r, h] = k + 1
        copy = remote(src, self.held(r, h, *src_at), self.send_sem.at[r, h, k],
                      self.recv_sem.at[r, h, src_at[0] * SIDE + src_at[1]], *self.place(*dst_at))
        copy.start()

    def wait(self, r, h, piece):
        src_at = self.at(h, *piece)
        arrived(self.held(r, h, *src_at), self.recv_sem.at[r, h, src_at[0] * SIDE + src_at[1]], *self.place(*self.coords))
        if self.on_arrival is not None:
            self.on_arrival(r, h, *src_at)

    def start(self, r):
        for to in ((1, 0), (3, 0), (0, 1), (0, 3)):
            for h in (0, 1):
                self.send(r, h, (0, 0), to)

    def spread(self, r, h, j1):
        for j2 in (1, 3):
            self.send(r, h, (j1, 0), (0, j2))

    def near(self, r):
        for j1 in (3, 1):
            for h in (0, 1):
                self.wait(r, h, (j1, 0))
                if j1 == (3 if (r + h) % 2 == 0 else 1):
                    self.send(r, h, (j1, 0), (4 - j1, 0))
                self.spread(r, h, j1)

    def pass_on(self, r, j1):
        for h in (0, 1):
            for j2 in (3, 1):
                self.wait(r, h, (j1, j2))
                if j2 == (3 if (r + h + (j1 + 1) // 2) % 2 == 0 else 1):
                    self.send(r, h, (j1, j2), (0, 4 - j2))

    def far(self, r):
        self.pass_on(r, 0)
        for h in (0, 1):
            self.wait(r, h, (2, 0))
            self.spread(r, h, 2)

    def last(self, r):
        for j1 in (3, 1, 2):
            self.pass_on(r, j1)

    def final(self, r):
        for j1 in (0, 3, 1, 2):
            for h in (0, 1):
                self.wait(r, h, (j1, 2))

    def drain(self, r):
        for h in (0, 1):
            for k in range(self.sent[r, h]):
                ref = self.held(r, h, *self.coords)
                remote(ref, ref, self.send_sem.at[r, h, k], self.recv_sem.at[r, h, 0], *self.place(*self.coords)).wait_send()


def qkv_kernel(x_ref, w_ref, wo_ref, seg_ref, q_ref, kv_ref, segall_ref, segq_ref, oa_ref, ob_ref,
               x_all, w_all, qkv, ls, xs, xr, ws, wr, ss, sr, ks, kr, rs, rr):
    tp, sp = lax.axis_index("tp"), lax.axis_index("sp")
    z, y = tp // SIDE, lax.rem(tp, SIDE)
    x, core = sp // 2, lax.rem(sp, 2)
    rows, width = x_ref.shape
    depth = w_ref.shape[0]
    cuts = [rows * c // CUTS[-1] for c in CUTS]
    size = [b - a for a, b in zip(cuts, cuts[1:])]
    half = width // 2

    def sp_at(dx, other=0):
        return lax.rem(x + dx, SIDE) * 2 + lax.rem(core + other, 2)

    mate = sp_at(0, 1)
    group = x // 2
    ally = (x + 1 - 2 * lax.rem(x, 2)) * 2 + core
    cross = (SIDE - 1 - x) * 2 + core

    peers = [(lax.rem(z + d, SIDE) * SIDE + y, sp) for d in (1, 3)]
    peers += [(z * SIDE + lax.rem(y + d, SIDE), sp) for d in (1, 3)]
    peers += [(tp, lax.rem(sp + d, 2 * SIDE)) for d in range(1, 2 * SIDE)]
    x_own = x_all.at[:, pl.ds(pl.multiple_of(tp * width, width), width)]
    w_own_rows = w_all.at[pl.ds(pl.multiple_of(sp * depth, depth), depth), :]
    loads = [pltpu.make_async_copy(x_ref, x_own, ls.at[0]), pltpu.make_async_copy(w_ref, w_own_rows, ls.at[1]),
             pltpu.make_async_copy(seg_ref, segq_ref.at[0], ls.at[2]),
             pltpu.make_async_copy(wo_ref.at[:, pl.ds(0, HEAD_DIM)], oa_ref.at[x], ls.at[3]),
             pltpu.make_async_copy(wo_ref.at[:, pl.ds(HEAD_DIM, HEAD_DIM)], ob_ref.at[z], ls.at[4])]
    for load in loads:
        load.start()
    barrier_with(peers)
    for load in loads:
        load.wait()

    grid = Gather2D(
        (z, y), lambda u, v: (u * SIDE + v, sp),
        lambda r, h, u, v: x_own.at[pl.ds(cuts[r], size[r]), pl.ds(h * half, half)],
        lambda r, h, u, v: x_all.at[pl.ds(cuts[r], size[r]), pl.ds(pl.multiple_of((u * SIDE + v) * width + h * half, half), half)],
        xs, xr)

    def w_at(owner, p):
        return w_all.at[pl.ds(pl.multiple_of(owner * depth + p * (depth // 2), depth // 2), depth // 2), :]

    w_sends = []

    def w_send(owner, p, to):
        k = len(w_sends)
        copy = remote(w_at(owner, p), w_at(owner, p), ws.at[k], wr.at[owner, p], tp, to)
        copy.start()
        w_sends.append(copy)

    def w_wait(owner, p):
        arrived(w_at(owner, p), wr.at[owner, p], tp, sp)

    def w_own(p):
        for to in (sp_at(1), sp_at(3), mate):
            w_send(sp, p, to)

    def w_near(p):
        for d in (3, 1):
            w_wait(sp_at(d), p)
            if d == (3 if p == 0 else 1):
                w_send(sp_at(d), p, sp_at(4 - d))
            w_send(sp_at(d), p, mate)

    def w_far():
        for p in (0, 1):
            w_wait(sp_at(2), p)
            w_send(sp_at(2), p, mate)

    def w_mate():
        for p in (0, 1):
            for d in (0, 1, 3, 2):
                w_wait(sp_at(d, 1), p)

    class Ring:
        def __init__(self, axis):
            self.axis, self.ref, self.me = axis, (oa_ref, ob_ref)[axis], (x, z)[axis]
            self.sends = []

        def at(self, d, p):
            return self.ref.at[lax.rem(self.me + d, SIDE), pl.ds(p * (depth // 2), depth // 2), :]

        def sem(self, d, p):
            return rr.at[self.axis, lax.rem(self.me + d, SIDE), p]

        def send(self, d, p, to):
            device = (tp, sp_at(to)) if self.axis == 0 else (lax.rem(z + to, SIDE) * SIDE + y, sp)
            copy = remote(self.at(d, p), self.at(d, p), rs.at[self.axis, len(self.sends)], self.sem(d, p), *device)
            copy.start()
            self.sends.append(copy)

        def own(self):
            for p in (0, 1):
                for to in (1, 3):
                    self.send(0, p, to)

        def near(self):
            for p in (0, 1):
                for d in (3, 1):
                    arrived(self.at(d, p), self.sem(d, p), tp, sp)
                    if d == (3 if p == 0 else 1):
                        self.send(d, p, 4 - d)

        def far(self):
            for p in (0, 1):
                arrived(self.at(2, p), self.sem(2, p), tp, sp)

    rings = Ring(0), Ring(1)

    grid.start(0)
    w_own(0)
    seg_copies = []
    for d in range(1, 2 * SIDE):
        copy = remote(segq_ref.at[0], segall_ref.at[sp], ss.at[d], sr.at[sp], tp, lax.rem(sp + d, 2 * SIDE))
        copy.start()
        seg_copies.append(copy)
    segall_ref[sp] = segq_ref[0]

    def kv_at(owner, r):
        return kv_ref.at[pl.ds(pl.multiple_of(owner * rows + cuts[r], 64), size[r]), :]

    kv_sends = []

    def kv_send(src, dst, recv, to):
        k = len(kv_sends)
        copy = remote(src, dst, ks.at[k], recv, tp, to)
        copy.start()
        kv_sends.append(copy)

    def project(r):
        here = slice(cuts[r], cuts[r + 1])
        for n in range(3):
            part = slice(n * 256, (n + 1) * 256)
            out = jnp.dot(x_all[here, :], w_all[:, part], preferred_element_type=jnp.float32).astype(jnp.bfloat16)
            for m in range(2):
                col = n * 2 + m
                qkv[col // 3, here, (col % 3) * HEAD_DIM:(col % 3 + 1) * HEAD_DIM] = out[:, m * HEAD_DIM:(m + 1) * HEAD_DIM]
        q_ref[here, :] = qkv[group, here, :HEAD_DIM]
        kv_ref[pl.ds(pl.multiple_of(sp * rows + cuts[r], 64), size[r]), :] = qkv[group, here, HEAD_DIM:]
        span = pl.ds(cuts[r], size[r])
        kv_send(qkv.at[1 - group, span, pl.ds(HEAD_DIM, 2 * HEAD_DIM)], kv_at(sp, r), kr.at[sp, r], cross)
        kv_send(qkv.at[1 - group, span, pl.ds(0, HEAD_DIM)], q_ref.at[pl.ds(rows + cuts[r], size[r]), :], kr.at[2 * SIDE, r], cross)
        kv_send(qkv.at[group, span, pl.ds(HEAD_DIM, 2 * HEAD_DIM)], kv_at(sp, r), kr.at[sp, r], ally)
        kv_send(qkv.at[group, span, pl.ds(HEAD_DIM, 2 * HEAD_DIM)], kv_at(sp, r), kr.at[sp, r], mate)

    ally_cross = lax.rem(x + 2, SIDE) * 2 + core

    def kv_wait(owner, r):
        arrived(kv_at(owner, r), kr.at[owner, r], tp, sp)

    def kv_cross(r):
        kv_wait(cross, r)
        kv_send(kv_at(cross, r), kv_at(cross, r), kr.at[cross, r], ally)
        kv_send(kv_at(cross, r), kv_at(cross, r), kr.at[cross, r], mate)

    def kv_ally(r):
        for owner in (ally, ally_cross):
            kv_wait(owner, r)
            kv_send(kv_at(owner, r), kv_at(owner, r), kr.at[owner, r], mate)

    def kv_mate(r):
        arrived(q_ref.at[pl.ds(rows + cuts[r], size[r]), :], kr.at[2 * SIDE, r], tp, sp)
        for d in range(SIDE):
            kv_wait(sp_at(d, 1), r)

    grid.near(0)
    w_own(1)
    grid.start(1)
    grid.far(0)
    grid.near(1)
    grid.last(0)
    w_near(0)
    grid.start(2)
    grid.far(1)
    grid.near(2)
    w_near(1)
    rings[0].own()
    grid.last(1)
    grid.start(3)
    rings[1].own()
    grid.far(2)
    w_far()
    w_mate()
    grid.final(0)
    project(0)
    grid.near(3)
    grid.final(1)
    project(1)
    rings[0].near()
    grid.last(2)
    grid.far(3)
    kv_cross(0)
    rings[1].near()
    grid.last(3)
    kv_cross(1)
    grid.final(2)
    project(2)
    grid.final(3)
    project(3)
    kv_ally(0)
    kv_ally(1)
    kv_cross(2)
    kv_cross(3)
    kv_ally(2)
    kv_ally(3)
    rings[0].far()
    rings[1].far()
    for r in range(CHUNKS):
        kv_mate(r)
    for d in range(1, 2 * SIDE):
        arrived(segall_ref.at[lax.rem(sp + d, 2 * SIDE)], sr.at[lax.rem(sp + d, 2 * SIDE)], tp, sp)
    segq_ref[1] = segall_ref[cross]
    for r in range(CHUNKS):
        grid.drain(r)
    for copy in w_sends + seg_copies + kv_sends + rings[0].sends + rings[1].sends:
        copy.wait_send()


def qkv_exchange(x_block, wqkv_block, wout_block, seg_block):
    rows, width = x_block.shape
    depth, cols = wqkv_block.shape
    sps, tps = 2 * SIDE, SIDE * SIDE
    seg_tile = seg_block.reshape(rows // HEAD_DIM, HEAD_DIM)
    vmem = pl.BlockSpec(memory_space=pltpu.VMEM)
    hbm = pl.BlockSpec(memory_space=pltpu.HBM)
    dma = pltpu.SemaphoreType.DMA
    return pl.pallas_call(
        qkv_kernel,
        out_shape=(
            jax.ShapeDtypeStruct((2 * rows, HEAD_DIM), jnp.bfloat16),
            jax.ShapeDtypeStruct((sps * rows, 2 * HEAD_DIM), jnp.bfloat16),
            jax.ShapeDtypeStruct((sps,) + seg_tile.shape, jnp.int32),
            jax.ShapeDtypeStruct((2,) + seg_tile.shape, jnp.int32),
            jax.ShapeDtypeStruct((SIDE, depth, HEAD_DIM), jnp.bfloat16),
            jax.ShapeDtypeStruct((SIDE, depth, HEAD_DIM), jnp.bfloat16),
        ),
        in_specs=[hbm] * 4,
        out_specs=(vmem,) * 6,
        scratch_shapes=[
            pltpu.VMEM((rows, tps * width), jnp.bfloat16),
            pltpu.VMEM((sps * depth, cols), jnp.bfloat16),
            pltpu.VMEM((2, rows, 3 * HEAD_DIM), jnp.bfloat16),
            dma((5,)),
            dma((CHUNKS, 2, 15)), dma((CHUNKS, 2, tps)),
            dma((14,)), dma((sps, 2)),
            dma((sps,)), dma((sps,)),
            dma((8 * CHUNKS,)), dma((sps + 1, CHUNKS)),
            dma((2, 6)), dma((2, SIDE, 2)),
        ],
        compiler_params=pltpu.CompilerParams(collective_id=0, has_side_effects=True, vmem_limit_bytes=26 * 1024 * 1024),
        name="qkv_exchange",
    )(*(pltpu.with_memory_space_constraint(a, pltpu.HBM) for a in (x_block, wqkv_block, wout_block, seg_tile)))


def output_kernel(ctx_ref, oa_ref, ob_ref, y_ref, o_all, w_all, part, os, orr, ws, wr, ms, mr, ys, yr):
    tp, sp = lax.axis_index("tp"), lax.axis_index("sp")
    z, y = tp // SIDE, lax.rem(tp, SIDE)
    x, core = sp // 2, lax.rem(sp, 2)
    rows = ctx_ref.shape[0] // 2
    quarter = rows // SIDE
    depth, width = oa_ref.shape[1], 2 * oa_ref.shape[2]
    group = x // 2
    cross = (SIDE - 1 - x) * 2 + core
    mate = x * 2 + 1 - core

    def x_at(d):
        return lax.rem(x + d, SIDE) * 2 + core

    def z_at(d):
        return lax.rem(z + d, SIDE)

    def y_at(d):
        return lax.rem(y + d, SIDE)

    peers = [(z_at(d) * SIDE + y, sp) for d in (1, 2, 3)]
    peers += [(z_at(d) * SIDE + y, cross) for d in range(SIDE)]
    peers += [(z * SIDE + y_at(d), sp) for d in (1, 2, 3)]
    peers += [(tp, x_at(1)), (tp, x_at(3)), (tp, mate)]
    mine = (z * SIDE + y) * 2 + group

    def keep_own():
        o_all[:, pl.ds(pl.multiple_of(mine * HEAD_DIM, HEAD_DIM), HEAD_DIM)] = ctx_ref[pl.ds(pl.multiple_of(z * quarter, quarter), quarter), :]
        for j in range(SIDE):
            block, left = lax.rem(x + j, SIDE), z_at(j) * width
            w_all[pl.ds(pl.multiple_of((block * 2 + core) * depth, depth), depth), pl.ds(pl.multiple_of(z * width, width), width // 2)] = oa_ref[block]
            w_all[pl.ds(pl.multiple_of(sp * depth, depth), depth), pl.ds(pl.multiple_of(left + width // 2, width // 2), width // 2)] = ob_ref[z_at(j)]

    barrier_with(peers, keep_own)

    o_sends = []

    def o_slot(j, yo, b):
        return (z_at(j) * SIDE + yo) * 2 + (group if b == 0 else 1 - group)

    def o_col(slot):
        return o_all.at[:, pl.ds(pl.multiple_of(slot * HEAD_DIM, HEAD_DIM), HEAD_DIM)]

    def o_send(src, slot, to_tp, to_sp):
        copy = remote(src, o_col(slot), os.at[len(o_sends)], orr.at[slot], to_tp, to_sp)
        copy.start()
        o_sends.append(copy)

    def o_wait(slot):
        arrived(o_col(slot), orr.at[slot], tp, sp)

    def ctx_rows(j, b):
        return ctx_ref.at[pl.ds(pl.multiple_of(b * rows + z_at(j) * quarter, quarter), quarter), :]

    def o_along_y(j, b, src):
        slot = o_slot(j, y, b)
        for d in (1, 3):
            o_send(src, slot, z * SIDE + y_at(d), sp)

    order = [(0, 1), (1, 0), (3, 0), (1, 1), (3, 1), (2, 0), (2, 1)]
    for j, b in order:
        o_send(ctx_rows(j, b), mine, z_at(j) * SIDE + y, sp if b == 0 else cross)
    o_along_y(0, 0, ctx_rows(0, 0))

    half = width // 2
    m_sends = []

    def panel(r, h, u, v, c):
        return w_all.at[pl.ds(pl.multiple_of((u * 2 + c) * depth, depth), depth),
                        pl.ds(pl.multiple_of(v * width + h * half, half), half)]

    def held_already(r, h, u, v):
        return oa_ref.at[u] if h == 0 else ob_ref.at[v]

    def to_mate(r, h, u, v, src=None):
        held = panel(r, h, u, v, core)
        copy = remote(held if src is None else src, held, ms.at[len(m_sends)], mr.at[r, h, u * SIDE + v], tp, mate)
        copy.start()
        m_sends.append(copy)

    grid = Gather2D(
        (x, z), lambda u, v: (v * SIDE + y, u * 2 + core),
        held_already, lambda r, h, u, v: panel(r, h, u, v, core), ws, wr, to_mate, first_done=True)

    def o_near(j, b):
        for d in (3, 1):
            slot = o_slot(j, y_at(d), b)
            o_wait(slot)
            if d == (3 if (j + b) % 2 == 0 else 1):
                o_send(o_col(slot), slot, z * SIDE + y_at(4 - d), sp)

    def o_first(j, b):
        o_wait(o_slot(j, y, b))
        o_along_y(j, b, o_col(o_slot(j, y, b)))

    for j1 in range(SIDE):
        for h in (0, 1):
            grid.spread(0, h, j1)
    for j1 in range(SIDE):
        for h in (0, 1):
            u, v = grid.at(h, j1, 0)
            to_mate(0, h, u, v, held_already(0, h, u, v))
    for j, b in order[0:3]:
        o_first(j, b)
    for j, b in ([(0, 0)] + order)[0:1]:
        o_near(j, b)
    for j, b in order[3:5]:
        o_first(j, b)
    for j, b in ([(0, 0)] + order)[1:3]:
        o_near(j, b)
    for j, b in order[5:7]:
        o_first(j, b)
    grid.pass_on(0, 0)
    for j, b in ([(0, 0)] + order)[3:5]:
        o_near(j, b)
    grid.pass_on(0, 1)
    for j, b in ([(0, 0)] + order)[5:8]:
        o_near(j, b)
    grid.pass_on(0, 2)
    grid.pass_on(0, 3)
    grid.final(0)
    for j, b in [(0, 0)] + order:
        o_wait(o_slot(j, y_at(2), b))
    for h in (0, 1):
        for d in range(SIDE * SIDE):
            u, v = lax.rem(x + d // SIDE, SIDE), z_at(d % SIDE)
            arrived(panel(0, h, u, v, 1 - core), mr.at[0, h, u * SIDE + v], tp, sp)

    y_sends = []
    strip = quarter // SIDE
    for zz in range(SIDE):
        out = jnp.dot(o_all[...], w_all[:, zz * width:(zz + 1) * width], preferred_element_type=jnp.float32)
        part[zz] = out.astype(jnp.bfloat16)
        cols = pl.ds(pl.multiple_of((zz * SIDE + y) * width, width), width)
        for d in (2, 1, 3):
            copy = remote(part.at[zz, pl.ds(pl.multiple_of(y_at(d) * strip, strip), strip), :], y_ref.at[:, cols],
                          ys.at[len(y_sends)], yr.at[zz, y], z * SIDE + y_at(d), sp)
            copy.start()
            y_sends.append(copy)
        y_ref[:, cols] = part[zz, pl.ds(pl.multiple_of(y * strip, strip), strip), :]
    for zz in range(SIDE):
        for d in (1, 3, 2):
            cols = pl.ds(pl.multiple_of((zz * SIDE + y_at(d)) * width, width), width)
            arrived(y_ref.at[:, cols], yr.at[zz, y_at(d)], tp, sp)
    grid.drain(0)
    for copy in o_sends + m_sends + y_sends:
        copy.wait_send()


def output_exchange(context, oa, ob):
    rows = context.shape[0] // 2
    depth, width = oa.shape[1], 2 * oa.shape[2]
    sps, tps = 2 * SIDE, SIDE * SIDE
    quarter = rows // SIDE
    vmem = pl.BlockSpec(memory_space=pltpu.VMEM)
    dma = pltpu.SemaphoreType.DMA
    return pl.pallas_call(
        output_kernel,
        out_shape=jax.ShapeDtypeStruct((quarter // SIDE, tps * width), jnp.bfloat16),
        in_specs=[vmem] * 3,
        out_specs=vmem,
        scratch_shapes=[
            pltpu.VMEM((quarter, tps * 2 * HEAD_DIM), jnp.bfloat16),
            pltpu.VMEM((sps * depth, SIDE * width), jnp.bfloat16),
            pltpu.VMEM((SIDE, quarter, width), jnp.bfloat16),
            dma((31,)), dma((2 * tps,)),
            dma((1, 2, 15)), dma((1, 2, tps)),
            dma((2 * tps,)), dma((1, 2, tps)),
            dma((3 * SIDE,)), dma((SIDE, SIDE)),
        ],
        compiler_params=pltpu.CompilerParams(collective_id=1, has_side_effects=True, vmem_limit_bytes=16 * 1024 * 1024),
        name="output_exchange",
    )(context, oa, ob)


def solution(mesh):
    def device_block(x_block, doc_block, wqkv_block, wout_block):
        q, kv, seg_all, seg_q, oa, ob = qkv_exchange(x_block, wqkv_block, wout_block, doc_block)
        context = attention(q, kv, seg_q.reshape(-1, HEAD_DIM), seg_all.reshape(-1, HEAD_DIM))
        return output_exchange(context, oa, ob)

    return jax.shard_map(
        device_block,
        mesh=mesh,
        in_specs=(P(("dp", "sp"), "tp"), P(("dp", "sp")), P("sp", "tp"), P("sp", "tp")),
        out_specs=P(("dp", "sp", "tp"), None),
        check_vma=False,
    )
```
